32 devices in a mesh: ctx: 8 (over z, x), wsh: 4 (over y, core).
Axes of the slice: x: 2, y: 2, z: 4, core: 2. Of those that a mesh axis runs over, the one named last changes fastest.
Arguments:
- tokens: bfloat16 [4, 1024, 1024], P('wsh', 'ctx'), may hold values from -6 to 6
- output_cotangent: bfloat16 [4, 1024, 1024], P('wsh', 'ctx'), may hold values from -6 to 6
- block_table: int32 [16], replicated, may hold values from 0 to 15, as said below
- weight_project: bfloat16 [1024, 3072], P('wsh'), may hold values from -0.25 to 0.25
- weight_combine: bfloat16 [1024, 1024], P('wsh'), may hold values from -0.75 to 0.75
- weight_expand: bfloat16 [1024, 4096], P('wsh'), may hold values from -0.1875 to 0.1875
- weight_reduce: bfloat16 [4096, 1024], P('wsh'), may hold values from -0.09375 to 0.09375
- vectors: bfloat16 [12, 1024], P(None, 'wsh'), may hold values from -1.1 to 4.5
- moment_project: float32 [1024, 3072], P('wsh'), may hold values from -0.66 to 0.66
- square_project: float32 [1024, 3072], P('wsh'), may hold values from 0.02 to 0.2
- moment_combine: float32 [1024, 1024], P('wsh'), may hold values from -0.66 to 0.66
- square_combine: float32 [1024, 1024], P('wsh'), may hold values from 0.02 to 0.2
- moment_expand: float32 [1024, 4096], P('wsh'), may hold values from -0.66 to 0.66
- square_expand: float32 [1024, 4096], P('wsh'), may hold values from 0.001 to 0.01
- moment_reduce: float32 [4096, 1024], P('wsh'), may hold values from -0.66 to 0.66
- square_reduce: float32 [4096, 1024], P('wsh'), may hold values from 0.02 to 0.2
- moment_vectors: float32 [12, 1024], P(None, 'wsh'), may hold values from -0.66 to 0.66
- square_vectors: float32 [12, 1024], P(None, 'wsh'), may hold values from 0.02 to 0.2
Outputs:
- layer_output: bfloat16 [4, 1024, 1024], P('wsh', 'ctx')
- input_gradient: bfloat16 [4, 1024, 1024], P('wsh', 'ctx')
- gradient_norm: float32 [1], replicated
- gradient_project: float32 [1024, 3072], P('wsh')
- new_moment_project: float32 [1024, 3072], P('wsh')
- new_square_project: float32 [1024, 3072], P('wsh')
- update_project: float32 [1024, 3072], P('wsh')
- gradient_combine: float32 [1024, 1024], P('wsh')
- new_moment_combine: float32 [1024, 1024], P('wsh')
- new_square_combine: float32 [1024, 1024], P('wsh')
- update_combine: float32 [1024, 1024], P('wsh')
- gradient_expand: float32 [1024, 4096], P('wsh')
- new_moment_expand: float32 [1024, 4096], P('wsh')
- new_square_expand: float32 [1024, 4096], P('wsh')
- update_expand: float32 [1024, 4096], P('wsh')
- gradient_reduce: float32 [4096, 1024], P('wsh')
- new_moment_reduce: float32 [4096, 1024], P('wsh')
- new_square_reduce: float32 [4096, 1024], P('wsh')
- update_reduce: float32 [4096, 1024], P('wsh')
- gradient_vectors: float32 [12, 1024], P(None, 'wsh')
- new_moment_vectors: float32 [12, 1024], P(None, 'wsh')
- new_square_vectors: float32 [12, 1024], P(None, 'wsh')
- update_vectors: float32 [12, 1024], P(None, 'wsh')
The draws below stay inside these ranges and needn't reach their ends.
Inputs may be any that keep to these rules, and one draw needn't show every extreme that they name: `block_table`: device p of ctx stores the blocks in slots 2p and 2p+1; these are two blocks j and 15 - j, in either order; every block appears once.
All inputs are finite; a program needn't handle non-finite values.
Results may differ from the reference program's by a relative error of at most 0.03.
Values may be sent and summed in bfloat16 or wider, within the bound.
A program may use at most 256 MiB of HBM per device.

```python
import math
import jax
import jax.numpy as jnp
from jax import lax

D = 1024
HEADS = 16
FF = 4096
BLK = 64
STEP = 4
L = 1024
NBLK = 16
SEQS = 4
VECS = 12
PARAMS = 12595200


def draw_block_table(key, part):
    first_key, second_key = jax.random.split(key)
    half_count = NBLK // 2
    lower = jax.random.permutation(first_key, half_count).astype(jnp.int32)
    upper = NBLK - 1 - lower
    flipped = jax.random.randint(second_key, (half_count,), 0, 2, dtype=jnp.int32)
    slot_first = jnp.where(flipped == 1, upper, lower)
    slot_second = jnp.where(flipped == 1, lower, upper)
    return jnp.stack([slot_first, slot_second], axis=1).reshape(NBLK).astype(jnp.int32)


def draw_vectors(key, part):
    first_key = jax.random.fold_in(key, 0)
    row_index = jnp.arange(VECS)[:, None]
    is_gain = (row_index == 0) | (row_index == 5)
    feature_share = jnp.arange(D, dtype=jnp.float32)[None, :] / D
    spread = jax.random.truncated_normal(first_key, -3.0, 3.0, (VECS, D), jnp.float32)
    ramp = 0.5 + 1.5 * feature_share
    gains = ramp * (1.0 + 0.25 * spread)
    biases = 0.3 * spread
    return jnp.where(is_gain, gains, biases).astype(jnp.bfloat16)


def block_scale(key, extent, pieces, smallest, largest):
    def one(position, shards_of):
        draws = jax.random.uniform(jax.random.fold_in(jax.random.fold_in(key, 6), position), (shards_of,), jnp.float32, smallest / len(pieces), largest / len(pieces))
        return jnp.repeat(jnp.exp(draws), extent[position] // shards_of).reshape((-1,) + (1,) * (len(extent) - position - 1))

    factor_of = one(*pieces[0])
    for cut in pieces[1:]:
        factor_of = factor_of * one(*cut)
    return factor_of


def normal_values(rng, extent, scale, bound, shards=(), kind=jnp.bfloat16):
    result = scale * jax.random.normal(rng, extent, jnp.float32)
    if shards:
        result = result * block_scale(rng, extent, shards, -0.22, 0.18)
    return jnp.clip(result, -bound, bound).astype(kind)


def setup_inputs(seed: int = 0) -> dict:
    seeds = jax.random.split(jax.random.key(seed), 19)
    tokens = normal_values(seeds[0], (SEQS, L, D), 1.0, 6.0, ((0, 4), (1, 8)))
    output_cotangent = normal_values(seeds[1], (SEQS, L, D), 1.0, 6.0, ((0, 4), (1, 8)))
    block_table = draw_block_table(jax.random.fold_in(seeds[18], 71), 0)
    weight_project = normal_values(seeds[3], (D, 3 * D), (D // 2) ** -0.5, 0.25, ((0, 4),))
    weight_combine = normal_values(seeds[4], (D, D), (D // 16) ** -0.5, 0.75, ((0, 4),))
    weight_expand = normal_values(seeds[5], (D, FF), D ** -0.5, 0.1875, ((0, 4),))
    weight_reduce = normal_values(seeds[6], (FF, D), FF ** -0.5, 0.09375, ((0, 4),))
    vectors = draw_vectors(jax.random.fold_in(seeds[18], 71), 0)
    moment_project = normal_values(seeds[8], (D, 3 * D), 0.11, 0.66, ((0, 4),), jnp.float32)
    square_project = jnp.clip(jnp.exp(math.log(0.2) - 2.3025851 * jax.random.uniform(seeds[9], (D, 3 * D), jnp.float32) ** block_scale(seeds[9], (D, 3 * D), ((0, 4),), -0.2, 0.2)), 0.02, 0.2)
    moment_combine = normal_values(seeds[10], (D, D), 0.11, 0.66, ((0, 4),), jnp.float32)
    square_combine = jnp.clip(jnp.exp(math.log(0.2) - 2.3025851 * jax.random.uniform(seeds[11], (D, D), jnp.float32) ** block_scale(seeds[11], (D, D), ((0, 4),), -0.2, 0.2)), 0.02, 0.2)
    moment_expand = normal_values(seeds[12], (D, FF), 0.11, 0.66, ((0, 4),), jnp.float32)
    square_expand = jnp.clip(jnp.exp(math.log(0.01) - 2.30258502 * jax.random.uniform(seeds[13], (D, FF), jnp.float32) ** block_scale(seeds[13], (D, FF), ((0, 4),), -0.2, 0.2)), 0.001, 0.01)
    moment_reduce = normal_values(seeds[14], (FF, D), 0.11, 0.66, ((0, 4),), jnp.float32)
    square_reduce = jnp.clip(jnp.exp(math.log(0.2) - 2.3025851 * jax.random.uniform(seeds[15], (FF, D), jnp.float32) ** block_scale(seeds[15], (FF, D), ((0, 4),), -0.2, 0.2)), 0.02, 0.2)
    moment_vectors = normal_values(seeds[16], (VECS, D), 0.11, 0.66, ((1, 4),), jnp.float32)
    square_vectors = jnp.clip(jnp.exp(math.log(0.2) - 2.3025851 * jax.random.uniform(seeds[17], (VECS, D), jnp.float32) ** block_scale(seeds[17], (VECS, D), ((1, 4),), -0.2, 0.2)), 0.02, 0.2)
    return {"tokens": tokens, "output_cotangent": output_cotangent, "block_table": block_table, "weight_project": weight_project, "weight_combine": weight_combine, "weight_expand": weight_expand, "weight_reduce": weight_reduce, "vectors": vectors, "moment_project": moment_project, "square_project": square_project, "moment_combine": moment_combine, "square_combine": square_combine, "moment_expand": moment_expand, "square_expand": square_expand, "moment_reduce": moment_reduce, "square_reduce": square_reduce, "moment_vectors": moment_vectors, "square_vectors": square_vectors}


@jax.custom_vjp
def low(v):
    return lax.optimization_barrier(v.astype(jnp.bfloat16)).astype(jnp.float32)

@jax.custom_vjp
def low_back(v):
    return v

def low_keep(v):
    return (low(v), None)

def low_pass(kept, grad):
    return (grad,)

def back_keep(v):
    return (v, None)

def back_low(kept, grad):
    return (low(grad),)
low.defvjp(low_keep, low_pass)
low_back.defvjp(back_keep, back_low)
norm_eps = 1e-05
masked_score = -1e+30
beta_one = 0.9
beta_two = 0.95
learn_rate = 0.02
decay_rate = 0.1
adam_eps = 1e-08

def product(left, right):
    return jnp.dot(left, right, precision=lax.Precision.HIGHEST, preferred_element_type=jnp.float32)

def layer_norm(values, norm_gain, norm_bias):
    row_mean = lax.optimization_barrier(jnp.mean(values, axis=-1, keepdims=True))
    centered = values - row_mean
    variance = lax.optimization_barrier(jnp.mean(centered * centered, axis=-1, keepdims=True))
    return centered * lax.rsqrt(variance + norm_eps) * norm_gain + norm_bias

def attention(queries, keys, values, positions):
    query_rows = min(512, L)
    head_size = D // HEADS
    score_scale = head_size ** (-0.5)
    key_heads = keys.reshape(L, HEADS, head_size)
    value_heads = values.reshape(L, HEADS, head_size)

    def one_block(block_entry):
        block_queries, block_pos = block_entry
        query_heads = block_queries.reshape(query_rows, HEADS, head_size)
        scores = jnp.einsum('qhd,khd->hqk', query_heads, key_heads, precision=lax.Precision.HIGHEST) * score_scale
        scores = low_back(scores)
        visible = positions[None, None, :] <= block_pos[None, :, None]
        scores = jnp.where(visible, scores, masked_score)
        soft_weights = low(jax.nn.softmax(scores, axis=-1))
        mixed = jnp.einsum('hqk,khd->qhd', soft_weights, value_heads, precision=lax.Precision.HIGHEST)
        return mixed.reshape(query_rows, D)
    blocked = lax.map(jax.checkpoint(one_block), (queries.reshape(L // query_rows, query_rows, D), positions.reshape(L // query_rows, query_rows)))
    return blocked.reshape(L, D)

def forward(sequence, weight_project, weight_combine, weight_expand, weight_reduce, vectors, positions):
    normed_one = low(layer_norm(sequence, vectors[0], vectors[1]))
    projected = product(normed_one, weight_project)
    queries = low(low_back(projected[:, :D] + vectors[2]))
    keys = low(low_back(projected[:, D:2 * D]))
    values = low(low_back(projected[:, 2 * D:] + vectors[3]))
    attended = low(low_back(attention(queries, keys, values, positions)))
    middle = sequence + low_back(product(attended, weight_combine) + vectors[4])
    normed_two = low(layer_norm(middle, vectors[5], vectors[6]))
    hidden_pre = low_back(product(normed_two, weight_expand) + vectors[8:].reshape(FF))
    hidden = low(jax.nn.gelu(hidden_pre, approximate=False))
    return middle + product(hidden, weight_reduce) + vectors[7]

def adam_step(weight, gradient, first_moment, second_moment, clip_factor, step_value):
    clipped = gradient * clip_factor
    moment = beta_one * first_moment + (1.0 - beta_one) * clipped
    square = beta_two * second_moment + (1.0 - beta_two) * clipped * clipped
    moment_hat = moment / (1.0 - jnp.power(jnp.float32(beta_one), step_value))
    square_hat = square / (1.0 - jnp.power(jnp.float32(beta_two), step_value))
    update = -learn_rate * (moment_hat / (jnp.sqrt(square_hat) + adam_eps) + decay_rate * weight.astype(jnp.float32))
    return (moment, square, update)

def reference(tokens, output_cotangent, block_table, weight_project, weight_combine, weight_expand, weight_reduce, vectors, moment_project, square_project, moment_combine, square_combine, moment_expand, square_expand, moment_reduce, square_reduce, moment_vectors, square_vectors):
    row_index = jnp.arange(L, dtype=jnp.int32)
    positions = (block_table[row_index // BLK] * BLK + row_index % BLK).astype(jnp.int32)
    weights = tuple((member.astype(jnp.float32) for member in (weight_project, weight_combine, weight_expand, weight_reduce, vectors)))

    def run_layer(inputs, project_in, combine_in, expand_in, reduce_in, vectors_in):
        return forward(inputs, project_in, combine_in, expand_in, reduce_in, vectors_in, positions)

    def one_sequence(carried, sequence_pair):
        sequence, cotangent = sequence_pair
        output, pullback = jax.vjp(run_layer, sequence.astype(jnp.float32), *weights)
        grads = pullback(cotangent.astype(jnp.float32))
        carried = tuple((running + member for running, member in zip(carried, grads[1:])))
        return (carried, (output.astype(jnp.bfloat16), grads[0].astype(jnp.bfloat16)))
    zero_grads = tuple((jnp.zeros(member.shape, jnp.float32) for member in weights))
    grads, outputs = lax.scan(one_sequence, zero_grads, (tokens, output_cotangent))
    layer_output, input_gradient = outputs
    grad_project, grad_combine, grad_expand, grad_reduce, grad_vectors = grads
    square_total = jnp.float32(0.0)
    for member in grads:
        square_total = square_total + jnp.sum(member * member)
    norm_value = jnp.sqrt(square_total)
    clip_max = jnp.sqrt(jnp.float32(PARAMS))
    clip_factor = clip_max / jnp.maximum(norm_value, clip_max)
    step_value = jnp.float32(STEP)
    mom_project, sq_project, up_project = adam_step(weight_project, grad_project, moment_project, square_project, clip_factor, step_value)
    mom_combine, sq_combine, up_combine = adam_step(weight_combine, grad_combine, moment_combine, square_combine, clip_factor, step_value)
    mom_expand, sq_expand, up_expand = adam_step(weight_expand, grad_expand, moment_expand, square_expand, clip_factor, step_value)
    mom_reduce, sq_reduce, up_reduce = adam_step(weight_reduce, grad_reduce, moment_reduce, square_reduce, clip_factor, step_value)
    mom_vectors, sq_vectors, up_vectors = adam_step(vectors, grad_vectors, moment_vectors, square_vectors, clip_factor, step_value)
    return (layer_output, input_gradient, norm_value.reshape(1), grad_project, mom_project, sq_project, up_project, grad_combine, mom_combine, sq_combine, up_combine, grad_expand, mom_expand, sq_expand, up_expand, grad_reduce, mom_reduce, sq_reduce, up_reduce, grad_vectors, mom_vectors, sq_vectors, up_vectors)
```

```python
import jax
import jax.numpy as jnp
from jax import lax
from jax.experimental import pallas as pl
from jax.experimental.pallas import tpu as pltpu
from jax.sharding import PartitionSpec as P

HEADS = 16
STEP = 4

norm_eps = 1e-05
masked_score = -1e30
beta_one = 0.9
beta_two = 0.95
learn_rate = 0.02
decay_rate = 0.1
adam_eps = 1e-08

MESH_ID = pl.DeviceIdType.MESH
FAST_CTX, FAST_WSH = 8, 4


def layer_norm(values, norm_gain, norm_bias):
    row_mean = jnp.mean(values, axis=-1, keepdims=True)
    centered = values - row_mean
    variance = jnp.mean(centered * centered, axis=-1, keepdims=True)
    return centered * lax.rsqrt(variance + norm_eps) * norm_gain + norm_bias


def gelu_exact(values):
    return jax.nn.gelu(values, approximate=False)


def matmul(left, right):
    return jnp.dot(left, right, preferred_element_type=jnp.float32)


def matmul_left_t(left, right):
    return lax.dot_general(
        left, right, (((0,), (0,)), ((), ())), preferred_element_type=jnp.float32
    )


def matmul_right_t(left, right):
    return lax.dot_general(
        left, right, (((1,), (1,)), ((), ())), preferred_element_type=jnp.float32
    )


class Place:
    def __init__(self):
        self.c = lax.axis_index("ctx")
        self.s = lax.axis_index("wsh")
        self.z, self.x = self.c // 2, self.c % 2
        self.y, self.k = self.s // 2, self.s % 2

    def ctx_of(self, dz, dx):
        return (self.z + dz + 4) % 4 * 2 + (self.x + dx) % 2

    def wsh_of(self, dy, dk):
        return (self.y + dy) % 2 * 2 + (self.k + dk) % 2


def remote(src, dst, sems, index, device):
    return pltpu.make_async_remote_copy(
        src_ref=src,
        dst_ref=dst,
        send_sem=sems[0].at[index],
        recv_sem=sems[1].at[index],
        device_id=device,
        device_id_type=MESH_ID,
    )


class Flow:
    count = 0
    local = 1

    def __init__(self, place, src, dst, sems, local_sem):
        self.place, self.src, self.dst = place, src, dst
        self.sems, self.local_sem = sems, local_sem
        self.sent = []

    def send(self, index, src, dst, device):
        copy = remote(src, dst, self.sems, index, device)
        copy.start()
        self.sent.append(copy)

    def arrived(self, index, dst, device):
        remote(dst, dst, self.sems, index, device).wait_recv()

    def keep(self, src, dst):
        self.kept = pltpu.make_async_copy(src, dst, self.local_sem)
        self.kept.start()

    def phase(self, number):
        pass

    def finish(self):
        for copy in self.sent:
            copy.wait_send()
        self.kept.wait()


class CtxGather(Flow):
    count = 11
    groups = ("x", "z")

    def half(self, slot, which):
        rows = self.dst.shape[1] // 2
        return self.dst.at[slot, pl.ds(which * rows, rows)]

    def phase(self, number):
        p = self.place
        across = (p.ctx_of(0, 1), p.s)
        above = (p.ctx_of(1, 0), p.s)
        below = (p.ctx_of(-1, 0), p.s)
        own = self.dst.at[p.c]
        slot = p.ctx_of
        if number == 0:
            self.send(0, self.src, own, across)
            self.send(1, self.src, own, below)
            self.send(2, self.src, own, above)
            self.keep(self.src, own)
        if number == 1:
            self.arrived(1, self.dst.at[slot(1, 0)], above)
            self.send(5, self.half(slot(1, 0), 0), self.half(slot(1, 0), 0), below)
            self.send(6, self.half(slot(1, 0), 1), self.half(slot(1, 0), 1), across)
            self.arrived(2, self.dst.at[slot(-1, 0)], below)
            self.send(7, self.half(slot(-1, 0), 1), self.half(slot(-1, 0), 1), above)
            self.send(8, self.half(slot(-1, 0), 1), self.half(slot(-1, 0), 1), across)
            self.arrived(0, self.dst.at[slot(0, 1)], across)
            self.send(3, self.half(slot(0, 1), 0), self.half(slot(0, 1), 0), below)
            self.send(4, self.half(slot(0, 1), 0), self.half(slot(0, 1), 0), above)
        if number == 2:
            self.arrived(3, self.half(slot(1, 1), 0), above)
            self.send(9, self.half(slot(1, 1), 0), self.half(slot(1, 1), 0), below)
            self.arrived(8, self.half(slot(-1, 1), 1), across)
            self.send(10, self.half(slot(-1, 1), 1), self.half(slot(-1, 1), 1), above)
        if number == 3:
            self.arrived(4, self.half(slot(-1, 1), 0), below)
            self.arrived(6, self.half(slot(1, 1), 1), across)
            self.arrived(5, self.half(slot(2, 0), 0), above)
            self.arrived(7, self.half(slot(2, 0), 1), below)
            self.arrived(9, self.half(slot(2, 1), 0), above)
            self.arrived(10, self.half(slot(2, 1), 1), below)
            self.finish()


class CtxSwap(Flow):
    count = 7
    groups = ("x", "z", "ctx")
    steps = ((2, 1), (2, 0), (1, 1), (-1, 1), (1, 0), (-1, 0), (0, 1))

    def phase(self, number):
        p = self.place
        if number == 0:
            for index, (dz, dx) in enumerate(self.steps):
                to = p.ctx_of(dz, dx)
                self.send(index, self.src.at[to], self.dst.at[p.c], (to, p.s))
            self.keep(self.src.at[p.c], self.dst.at[p.c])
        if number == 3:
            for index, (dz, dx) in enumerate(self.steps):
                source = p.ctx_of(-dz, dx)
                self.arrived(index, self.dst.at[source], (source, p.s))
            self.finish()


class WshGather(Flow):
    count = 3
    groups = ("y", "core")

    def phase(self, number):
        p = self.place
        partner, over = p.wsh_of(0, 1), p.wsh_of(1, 0)
        own = self.dst.at[p.s]
        if number == 0:
            self.send(1, self.src, own, (p.c, over))
            self.send(0, self.src, own, (p.c, partner))
            self.keep(self.src, own)
        if number == 2:
            self.arrived(1, self.dst.at[over], (p.c, over))
            self.send(2, self.dst.at[over], self.dst.at[over], (p.c, partner))
        if number == 3:
            self.arrived(0, self.dst.at[partner], (p.c, partner))
            self.arrived(2, self.dst.at[p.wsh_of(1, 1)], (p.c, partner))
            self.finish()


class WshSwap(Flow):
    count = 3
    groups = ("y", "core", "wsh")
    steps = ((1, 1), (1, 0), (0, 1))

    def phase(self, number):
        p = self.place
        if number == 0:
            for index, (dy, dk) in enumerate(self.steps):
                to = p.wsh_of(dy, dk)
                self.send(index, self.src.at[to], self.dst.at[p.s], (p.c, to))
            self.keep(self.src.at[p.s], self.dst.at[p.s])
        if number == 3:
            for index, (dy, dk) in enumerate(self.steps):
                source = p.wsh_of(dy, dk)
                self.arrived(index, self.dst.at[source], (p.c, source))
            self.finish()


def greet(place, groups):
    peers = set()
    if "x" in groups:
        peers.add("x")
    others = []
    if "ctx" in groups:
        for dz, dx in CtxSwap.steps:
            others.append((place.ctx_of(dz, dx), place.s))
    else:
        if "x" in groups:
            others.append((place.ctx_of(0, 1), place.s))
        if "z" in groups:
            others.append((place.ctx_of(1, 0), place.s))
            others.append((place.ctx_of(-1, 0), place.s))
    if "wsh" in groups:
        for dy, dk in WshSwap.steps:
            others.append((place.c, place.wsh_of(dy, dk)))
    else:
        if "y" in groups:
            others.append((place.c, place.wsh_of(1, 0)))
        if "core" in groups:
            others.append((place.c, place.wsh_of(0, 1)))
    barrier = pltpu.get_barrier_semaphore()
    for device in others:
        pl.semaphore_signal(barrier, inc=1, device_id=device, device_id_type=MESH_ID)
    pl.semaphore_wait(barrier, len(others))


def exchange(name, call_id, *pairs):
    kinds = [kind for kind, _ in pairs]
    arrays = [array for _, array in pairs]
    flows = len(pairs)
    groups = set()
    for kind in kinds:
        groups.update(kind.groups)

    def kernel(*refs):
        sources, targets = refs[:flows], refs[flows : 2 * flows]
        scratch = refs[2 * flows :]
        place = Place()
        greet(place, groups)
        running = []
        for index, kind in enumerate(kinds):
            sems = (scratch[3 * index], scratch[3 * index + 1])
            running.append(
                kind(place, sources[index], targets[index], sems, scratch[3 * index + 2])
            )
        for number in range(4):
            for flow in running:
                flow.phase(number)

    out_shape = []
    sem_shapes = []
    sizes = {CtxGather: FAST_CTX, WshGather: FAST_WSH}
    for kind, array in pairs:
        shape = array.shape if kind in (CtxSwap, WshSwap) else (sizes[kind],) + array.shape
        out_shape.append(jax.ShapeDtypeStruct(shape, array.dtype))
        sem_shapes.append(pltpu.SemaphoreType.DMA((kind.count,)))
        sem_shapes.append(pltpu.SemaphoreType.DMA((kind.count,)))
        sem_shapes.append(pltpu.SemaphoreType.DMA)
    return pl.pallas_call(
        kernel,
        out_shape=out_shape,
        in_specs=[pl.BlockSpec(memory_space=pltpu.VMEM)] * flows,
        out_specs=[pl.BlockSpec(memory_space=pl.ANY)] * flows,
        scratch_shapes=sem_shapes,
        compiler_params=pltpu.CompilerParams(
            collective_id=call_id, has_side_effects=True, vmem_limit_bytes=48 * 2**20
        ),
        name=name,
    )(*arrays)


def plain(name, call_id, *pairs):
    outs = []
    for kind, array in pairs:
        if kind is CtxGather:
            outs.append(lax.all_gather(array, "ctx", axis=0))
        elif kind is WshGather:
            outs.append(lax.all_gather(array, "wsh", axis=0))
        elif kind is CtxSwap:
            outs.append(lax.all_to_all(array, "ctx", 0, 0, tiled=True))
        else:
            outs.append(lax.all_to_all(array, "wsh", 0, 0, tiled=True))
    return outs


def adam_step(weight, gradient, first_moment, second_moment, clip_factor, step_value):
    clipped = gradient * clip_factor
    moment = beta_one * first_moment + (1.0 - beta_one) * clipped
    square = beta_two * second_moment + (1.0 - beta_two) * clipped * clipped
    moment_hat = moment / (1.0 - jnp.power(jnp.float32(beta_one), step_value))
    square_hat = square / (1.0 - jnp.power(jnp.float32(beta_two), step_value))
    update = -learn_rate * (
        moment_hat / (jnp.sqrt(square_hat) + adam_eps) + decay_rate * weight.astype(jnp.float32)
    )
    return (moment, square, update)


def body(
    tokens,
    output_cotangent,
    block_table,
    weight_project,
    weight_combine,
    weight_expand,
    weight_reduce,
    vectors,
    moment_project,
    square_project,
    moment_combine,
    square_combine,
    moment_expand,
    square_expand,
    moment_reduce,
    square_reduce,
    moment_vectors,
    square_vectors,
):
    low = jnp.bfloat16
    ctx_count, wsh_count = lax.axis_size("ctx"), lax.axis_size("wsh")
    ctx_index, wsh_index = lax.axis_index("ctx"), lax.axis_index("wsh")
    rows_dev, width = tokens.shape[1], tokens.shape[2]
    block_rows = rows_dev // 2
    total_rows = rows_dev * ctx_count
    group_rows = rows_dev * wsh_count
    head_size = width // HEADS
    score_scale = head_size ** (-0.5)
    head_cols = width // ctx_count
    local_heads = head_cols // head_size
    shard_rows = weight_project.shape[0]
    ff_width = weight_expand.shape[1]
    chunk = ff_width // wsh_count
    vec_rows = vectors.shape[0]
    fast = (ctx_count, wsh_count) == (FAST_CTX, FAST_WSH)
    swap = exchange if fast else plain

    sequence = tokens[0].astype(jnp.float32)
    cotangent_low = output_cotangent[0]
    cotangent = cotangent_low.astype(jnp.float32)

    project_cols = lax.dynamic_slice_in_dim(
        weight_project.reshape(shard_rows, 3, ctx_count, head_cols), ctx_index, 1, axis=2
    ).reshape(shard_rows, 3 * head_cols)

    vec_pad = -vec_rows % 16
    (vec_parts,) = swap("vec", 0, (WshGather, jnp.pad(vectors, ((0, vec_pad), (0, 0)))))
    vec_table = (
        vec_parts[:, :vec_rows].transpose(1, 0, 2).reshape(vec_rows, width).astype(jnp.float32)
    )
    normed_one = layer_norm(sequence, vec_table[0], vec_table[1]).astype(low)
    normed_all, project_parts, cot_parts, combine_parts, expand_parts = swap(
        "front",
        1,
        (CtxGather, normed_one),
        (WshGather, project_cols),
        (WshGather, cotangent_low),
        (WshGather, weight_combine),
        (WshSwap, weight_expand.reshape(shard_rows, wsh_count, chunk).transpose(1, 0, 2)),
    )
    normed_all = normed_all.reshape(total_rows, width)
    project_mine = project_parts.reshape(width, 3 * head_cols)
    full_combine = combine_parts.reshape(width, width)
    expand_mine = expand_parts.reshape(width, chunk)
    cot_group = cot_parts.reshape(group_rows, width)

    qkv = matmul(normed_all, project_mine)
    bias_cols = lax.dynamic_slice_in_dim(
        vec_table[:4].reshape(4, ctx_count, head_cols), ctx_index, 1, axis=1
    ).reshape(4, head_cols)
    queries = (qkv[:, :head_cols] + bias_cols[2]).astype(low)
    keys = qkv[:, head_cols : 2 * head_cols].astype(low)
    values = (qkv[:, 2 * head_cols :] + bias_cols[3]).astype(low)
    positions = (
        block_table[:, None] * block_rows + jnp.arange(block_rows, dtype=jnp.int32)[None, :]
    ).reshape(total_rows)
    visible = positions[None, None, :] <= positions[None, :, None]
    heads = (total_rows, local_heads, head_size)
    query_heads, key_heads, value_heads = (
        queries.reshape(heads),
        keys.reshape(heads),
        values.reshape(heads),
    )
    scores = (
        jnp.einsum("qhd,khd->hqk", query_heads, key_heads, preferred_element_type=jnp.float32)
        * score_scale
    )
    scores = jnp.where(visible, scores, masked_score)
    peak = jnp.max(scores, axis=2, keepdims=True)
    grown = jnp.exp(scores - peak)
    soft = grown / jnp.sum(grown, axis=2, keepdims=True)
    soft_low = soft.astype(low)
    attended_heads = jnp.einsum(
        "hqk,khd->qhd", soft_low, value_heads, preferred_element_type=jnp.float32
    )
    attended = attended_heads.reshape(total_rows, head_cols)
    (att_parts,) = swap(
        "attended", 2, (CtxSwap, attended.astype(low).reshape(ctx_count, rows_dev, head_cols))
    )
    attended_rows = att_parts.transpose(1, 0, 2).reshape(rows_dev, width)

    middle = sequence + matmul(attended_rows, full_combine) + vec_table[4]
    normed_two = layer_norm(middle, vec_table[5], vec_table[6]).astype(low)
    two_parts, att_cols = swap(
        "normed_two",
        3,
        (WshGather, normed_two),
        (WshSwap, attended_rows.reshape(rows_dev, wsh_count, shard_rows).transpose(1, 0, 2)),
    )
    two_group = two_parts.reshape(group_rows, width)

    bias_ff = lax.dynamic_slice_in_dim(vec_table[8:].reshape(-1), wsh_index * chunk, chunk)
    hidden_pre = matmul(two_group, expand_mine) + bias_ff
    hidden, gelu_back = jax.vjp(gelu_exact, hidden_pre)
    hidden = hidden.astype(low)
    out_partial = matmul(hidden, weight_reduce)
    pre_grad = gelu_back(matmul_right_t(cot_group, weight_reduce))[0].astype(low)
    two_partial = matmul_right_t(pre_grad, expand_mine)
    part_shape = (wsh_count, rows_dev, width)
    two_terms, out_terms = swap(
        "ff_sums",
        4,
        (WshSwap, two_partial.astype(low).reshape(part_shape)),
        (WshSwap, out_partial.astype(low).reshape(part_shape)),
    )
    layer_output = middle + jnp.sum(out_terms.astype(jnp.float32), axis=0) + vec_table[7]
    normed_two_grad = jnp.sum(two_terms.astype(jnp.float32), axis=0)
    norm_two_back = jax.vjp(layer_norm, middle, vec_table[5], vec_table[6])[1](normed_two_grad)
    middle_grad = cotangent + norm_two_back[0]
    branch_grad = middle_grad.astype(low)
    attended_grad_rows = matmul_right_t(branch_grad, full_combine).astype(low)
    att_grad_parts, branch_parts = swap(
        "attended_grad",
        5,
        (CtxSwap, attended_grad_rows.reshape(rows_dev, ctx_count, head_cols).transpose(1, 0, 2)),
        (WshGather, branch_grad),
    )
    branch_group = branch_parts.reshape(group_rows, width)
    attended_grad = att_grad_parts.reshape(total_rows, head_cols)

    grad_reduce = matmul_left_t(hidden, cot_group)
    grad_expand = matmul_left_t(two_group, pre_grad)
    grad_combine = matmul_left_t(att_cols.reshape(group_rows, shard_rows), branch_group)

    grad_heads = attended_grad.reshape(heads)
    delta = jnp.sum(
        grad_heads.astype(jnp.float32) * attended_heads, axis=2
    ).transpose(1, 0)[:, :, None]
    soft_grad = jnp.einsum(
        "qhd,khd->hqk", grad_heads, value_heads, preferred_element_type=jnp.float32
    )
    score_grad = (soft * (soft_grad - delta)).astype(low)
    query_grad = (
        jnp.einsum("hqk,khd->qhd", score_grad, key_heads, preferred_element_type=jnp.float32)
        * score_scale
    )
    key_grad = (
        jnp.einsum("hqk,qhd->khd", score_grad, query_heads, preferred_element_type=jnp.float32)
        * score_scale
    )
    value_grad = jnp.einsum(
        "hqk,qhd->khd", soft_low, grad_heads, preferred_element_type=jnp.float32
    )
    flat = (total_rows, head_cols)
    qkv_grad = jnp.concatenate(
        [member.reshape(flat).astype(low) for member in (query_grad, key_grad, value_grad)], axis=1
    )
    grad_project = matmul_left_t(normed_all, qkv_grad)
    one_partial = matmul_right_t(qkv_grad, project_mine)

    cut = shard_rows // ctx_count
    cut_reduce = chunk // ctx_count
    for_ctx = jnp.concatenate(
        [
            grad_reduce.astype(low).reshape(ctx_count, cut_reduce, width),
            grad_combine.astype(low).reshape(ctx_count, cut, width),
        ],
        axis=1,
    )
    expand_ctx = (
        grad_expand.astype(low)
        .reshape(wsh_count, ctx_count, cut, chunk)
        .transpose(1, 0, 2, 3)
        .reshape(ctx_count, wsh_count * cut, chunk)
    )
    ctx_terms, expand_terms, one_terms, project_terms = swap(
        "grad_sums",
        6,
        (CtxSwap, for_ctx),
        (CtxSwap, expand_ctx),
        (CtxSwap, one_partial.astype(low).reshape(ctx_count, rows_dev, width)),
        (WshSwap, grad_project.astype(low).reshape(wsh_count, shard_rows, 3 * head_cols)),
    )
    normed_one_grad = jnp.sum(one_terms.astype(jnp.float32), axis=0)
    norm_one_back = jax.vjp(layer_norm, sequence, vec_table[0], vec_table[1])[1](normed_one_grad)
    input_gradient = (middle_grad + norm_one_back[0]).astype(low)
    ctx_piece = jnp.sum(ctx_terms.astype(jnp.float32), axis=0).astype(low)
    expand_piece = jnp.sum(expand_terms.astype(jnp.float32), axis=0).astype(low)
    project_piece = jnp.sum(project_terms.astype(jnp.float32), axis=0).astype(low)

    def spread(columns, start):
        return lax.dynamic_update_slice(
            jnp.zeros((width,), jnp.float32), columns, (start,)
        )

    ff_terms = lax.dynamic_update_slice(
        jnp.zeros((ff_width,), jnp.float32),
        jnp.sum(pre_grad.astype(jnp.float32), axis=0),
        (wsh_index * chunk,),
    ).reshape(-1, width)
    head_start = ctx_index * head_cols
    query_sum = jnp.sum(qkv_grad[:, :head_cols].astype(jnp.float32), axis=0)
    value_sum = jnp.sum(qkv_grad[:, 2 * head_cols :].astype(jnp.float32), axis=0)
    vec_terms = jnp.concatenate(
        [
            jnp.stack(
                [
                    norm_one_back[1],
                    norm_one_back[2],
                    spread(query_sum, head_start),
                    spread(value_sum, head_start),
                    jnp.sum(branch_grad.astype(jnp.float32), axis=0),
                    norm_two_back[1],
                    norm_two_back[2],
                    jnp.sum(cotangent, axis=0),
                ]
            ),
            ff_terms,
            jnp.zeros((vec_pad, width), jnp.float32),
        ],
        axis=0,
    )
    vec_cols = vectors.shape[1]
    vec_swapped, expand_rows = swap(
        "vec_sums",
        7,
        (WshSwap, vec_terms.reshape(-1, wsh_count, vec_cols).transpose(1, 0, 2)),
        (WshSwap, expand_piece.reshape(wsh_count, cut, chunk)),
    )
    vec_mine = jnp.sum(vec_swapped, axis=0)
    expand_mine_rows = expand_rows.transpose(1, 0, 2).reshape(cut, ff_width)
    square_mine = (
        jnp.sum(jnp.square(ctx_piece.astype(jnp.float32)))
        + jnp.sum(jnp.square(expand_rows.astype(jnp.float32)))
        + jnp.sum(jnp.square(project_piece.astype(jnp.float32)))
    )
    ctx_all, expand_all, project_all, vec_all, square_ctx = swap(
        "grads",
        8,
        (CtxGather, ctx_piece),
        (CtxGather, expand_mine_rows),
        (CtxGather, project_piece),
        (CtxGather, vec_mine),
        (CtxGather, jnp.full((16, 128), square_mine, jnp.float32)),
    )
    sum_reduce = ctx_all[:, :cut_reduce].reshape(chunk, width).astype(jnp.float32)
    sum_combine = ctx_all[:, cut_reduce:].reshape(shard_rows, width).astype(jnp.float32)
    sum_expand = expand_all.reshape(shard_rows, ff_width).astype(jnp.float32)
    sum_project = (
        project_all.reshape(ctx_count, shard_rows, 3, head_cols)
        .transpose(1, 2, 0, 3)
        .reshape(shard_rows, 3 * width)
        .astype(jnp.float32)
    )
    sum_vectors = jnp.sum(vec_all, axis=0)[:vec_rows]
    square_part = jnp.sum(square_ctx[:, 0, 0]) + jnp.sum(jnp.square(sum_vectors))
    (square_all,) = swap(
        "squares", 9, (WshGather, jnp.full((8, 128), square_part, jnp.float32))
    )
    norm_value = jnp.sqrt(jnp.sum(square_all[:, 0, 0]))
    params_total = 4 * width * width + 2 * width * ff_width + vec_rows * width
    clip_max = jnp.sqrt(jnp.float32(params_total))
    clip_factor = clip_max / jnp.maximum(norm_value, clip_max)
    step_value = jnp.float32(STEP)
    results = [layer_output.astype(low)[None], input_gradient[None], norm_value.reshape(1)]
    for weight, total, first, second in (
        (weight_project, sum_project, moment_project, square_project),
        (weight_combine, sum_combine, moment_combine, square_combine),
        (weight_expand, sum_expand, moment_expand, square_expand),
        (weight_reduce, sum_reduce, moment_reduce, square_reduce),
        (vectors, sum_vectors, moment_vectors, square_vectors),
    ):
        results.append(total)
        results.extend(adam_step(weight, total, first, second, clip_factor, step_value))
    return tuple(results)


def solution(mesh):
    rows, cols = P("wsh", None), P(None, "wsh")
    token = P("wsh", "ctx", None)
    return jax.shard_map(
        body,
        mesh=mesh,
        in_specs=(token, token, P(), rows, rows, rows, rows, cols) + (rows,) * 8 + (cols,) * 2,
        out_specs=(token, token, P()) + (rows,) * 16 + (cols,) * 4,
        check_vma=False,
    )
```

```python
import jax
import jax.numpy as jnp
from jax import lax
from jax.experimental import pallas as pl
from jax.experimental.pallas import tpu as pltpu
from jax.sharding import PartitionSpec as P

HEADS = 16
STEP = 4

norm_eps = 1e-05
masked_score = -1e30
beta_one = 0.9
beta_two = 0.95
learn_rate = 0.02
decay_rate = 0.1
adam_eps = 1e-08

MESH_ID = pl.DeviceIdType.MESH
FAST_CTX, FAST_WSH = 8, 4


def layer_norm(values, norm_gain, norm_bias):
    row_mean = jnp.mean(values, axis=-1, keepdims=True)
    centered = values - row_mean
    variance = jnp.mean(centered * centered, axis=-1, keepdims=True)
    return centered * lax.rsqrt(variance + norm_eps) * norm_gain + norm_bias


def gelu_exact(values):
    return jax.nn.gelu(values, approximate=False)


def matmul(left, right):
    return jnp.dot(left, right, preferred_element_type=jnp.float32)


def matmul_left_t(left, right):
    return lax.dot_general(
        left, right, (((0,), (0,)), ((), ())), preferred_element_type=jnp.float32
    )


def matmul_right_t(left, right):
    return lax.dot_general(
        left, right, (((1,), (1,)), ((), ())), preferred_element_type=jnp.float32
    )


class Place:
    def __init__(self):
        self.c = lax.axis_index("ctx")
        self.s = lax.axis_index("wsh")
        self.z, self.x = self.c // 2, self.c % 2
        self.y, self.k = self.s // 2, self.s % 2

    def ctx_of(self, dz, dx):
        return (self.z + dz + 4) % 4 * 2 + (self.x + dx) % 2

    def wsh_of(self, dy, dk):
        return (self.y + dy) % 2 * 2 + (self.k + dk) % 2


def remote(src, dst, sems, index, device):
    return pltpu.make_async_remote_copy(
        src_ref=src,
        dst_ref=dst,
        send_sem=sems[0].at[index],
        recv_sem=sems[1].at[index],
        device_id=device,
        device_id_type=MESH_ID,
    )


class Flow:
    count = 0
    local = 1

    def __init__(self, place, src, dst, sems, local_sem):
        self.place, self.src, self.dst = place, src, dst
        self.sems, self.local_sem = sems, local_sem
        self.sent = []

    def send(self, index, src, dst, device):
        copy = remote(src, dst, self.sems, index, device)
        copy.start()
        self.sent.append(copy)

    def arrived(self, index, dst, device):
        remote(dst, dst, self.sems, index, device).wait_recv()

    def keep(self, src, dst):
        self.kept = pltpu.make_async_copy(src, dst, self.local_sem)
        self.kept.start()

    def phase(self, number):
        pass

    def finish(self):
        for copy in self.sent:
            copy.wait_send()
        self.kept.wait()


class CtxGather(Flow):
    count = 11
    groups = ("x", "z")

    def half(self, slot, which):
        rows = self.dst.shape[1] // 2
        return self.dst.at[slot, pl.ds(which * rows, rows)]

    def phase(self, number):
        p = self.place
        across = (p.ctx_of(0, 1), p.s)
        above = (p.ctx_of(1, 0), p.s)
        below = (p.ctx_of(-1, 0), p.s)
        own = self.dst.at[p.c]
        slot = p.ctx_of
        if number == 0:
            self.send(0, self.src, own, across)
            self.send(1, self.src, own, below)
            self.send(2, self.src, own, above)
            self.keep(self.src, own)
        if number == 1:
            self.arrived(1, self.dst.at[slot(1, 0)], above)
            self.send(5, self.half(slot(1, 0), 0), self.half(slot(1, 0), 0), below)
            self.send(6, self.half(slot(1, 0), 1), self.half(slot(1, 0), 1), across)
            self.arrived(2, self.dst.at[slot(-1, 0)], below)
            self.send(7, self.half(slot(-1, 0), 1), self.half(slot(-1, 0), 1), above)
            self.send(8, self.half(slot(-1, 0), 1), self.half(slot(-1, 0), 1), across)
            self.arrived(0, self.dst.at[slot(0, 1)], across)
            self.send(3, self.half(slot(0, 1), 0), self.half(slot(0, 1), 0), below)
            self.send(4, self.half(slot(0, 1), 0), self.half(slot(0, 1), 0), above)
        if number == 2:
            self.arrived(3, self.half(slot(1, 1), 0), above)
            self.send(9, self.half(slot(1, 1), 0), self.half(slot(1, 1), 0), below)
            self.arrived(8, self.half(slot(-1, 1), 1), across)
            self.send(10, self.half(slot(-1, 1), 1), self.half(slot(-1, 1), 1), above)
        if number == 3:
            self.arrived(4, self.half(slot(-1, 1), 0), below)
            self.arrived(6, self.half(slot(1, 1), 1), across)
            self.arrived(5, self.half(slot(2, 0), 0), above)
            self.arrived(7, self.half(slot(2, 0), 1), below)
            self.arrived(9, self.half(slot(2, 1), 0), above)
            self.arrived(10, self.half(slot(2, 1), 1), below)
            self.finish()


class CtxSwap(Flow):
    count = 7
    groups = ("x", "z", "ctx")
    steps = ((2, 1), (2, 0), (1, 1), (-1, 1), (1, 0), (-1, 0), (0, 1))

    def phase(self, number):
        p = self.place
        if number == 0:
            for index, (dz, dx) in enumerate(self.steps):
                to = p.ctx_of(dz, dx)
                self.send(index, self.src.at[to], self.dst.at[p.c], (to, p.s))
            self.keep(self.src.at[p.c], self.dst.at[p.c])
        if number == 3:
            for index, (dz, dx) in enumerate(self.steps):
                source = p.ctx_of(-dz, dx)
                self.arrived(index, self.dst.at[source], (source, p.s))
            self.finish()


class WshGather(Flow):
    count = 3
    groups = ("y", "core")

    def phase(self, number):
        p = self.place
        partner, over = p.wsh_of(0, 1), p.wsh_of(1, 0)
        own = self.dst.at[p.s]
        if number == 0:
            self.send(1, self.src, own, (p.c, over))
            self.send(0, self.src, own, (p.c, partner))
            self.keep(self.src, own)
        if number == 2:
            self.arrived(1, self.dst.at[over], (p.c, over))
            self.send(2, self.dst.at[over], self.dst.at[over], (p.c, partner))
        if number == 3:
            self.arrived(0, self.dst.at[partner], (p.c, partner))
            self.arrived(2, self.dst.at[p.wsh_of(1, 1)], (p.c, partner))
            self.finish()


class WshSwap(Flow):
    count = 3
    groups = ("y", "core", "wsh")
    steps = ((1, 1), (1, 0), (0, 1))

    def phase(self, number):
        p = self.place
        if number == 0:
            for index, (dy, dk) in enumerate(self.steps):
                to = p.wsh_of(dy, dk)
                self.send(index, self.src.at[to], self.dst.at[p.s], (p.c, to))
            self.keep(self.src.at[p.s], self.dst.at[p.s])
        if number == 3:
            for index, (dy, dk) in enumerate(self.steps):
                source = p.wsh_of(dy, dk)
                self.arrived(index, self.dst.at[source], (p.c, source))
            self.finish()


def greet(place, groups):
    peers = set()
    if "x" in groups:
        peers.add("x")
    others = []
    if "ctx" in groups:
        for dz, dx in CtxSwap.steps:
            others.append((place.ctx_of(dz, dx), place.s))
    else:
        if "x" in groups:
            others.append((place.ctx_of(0, 1), place.s))
        if "z" in groups:
            others.append((place.ctx_of(1, 0), place.s))
            others.append((place.ctx_of(-1, 0), place.s))
    if "wsh" in groups:
        for dy, dk in WshSwap.steps:
            others.append((place.c, place.wsh_of(dy, dk)))
    else:
        if "y" in groups:
            others.append((place.c, place.wsh_of(1, 0)))
        if "core" in groups:
            others.append((place.c, place.wsh_of(0, 1)))
    barrier = pltpu.get_barrier_semaphore()
    for device in others:
        pl.semaphore_signal(barrier, inc=1, device_id=device, device_id_type=MESH_ID)
    pl.semaphore_wait(barrier, len(others))


def exchange(name, call_id, *pairs):
    kinds = [kind for kind, _ in pairs]
    arrays = [array for _, array in pairs]
    flows = len(pairs)
    groups = set()
    for kind in kinds:
        groups.update(kind.groups)

    def kernel(*refs):
        sources, targets = refs[:flows], refs[flows : 2 * flows]
        scratch = refs[2 * flows :]
        place = Place()
        greet(place, groups)
        running = []
        for index, kind in enumerate(kinds):
            sems = (scratch[3 * index], scratch[3 * index + 1])
            running.append(
                kind(place, sources[index], targets[index], sems, scratch[3 * index + 2])
            )
        for number in range(4):
            for flow in running:
                flow.phase(number)

    out_shape = []
    sem_shapes = []
    sizes = {CtxGather: FAST_CTX, WshGather: FAST_WSH}
    for kind, array in pairs:
        shape = array.shape if kind in (CtxSwap, WshSwap) else (sizes[kind],) + array.shape
        out_shape.append(jax.ShapeDtypeStruct(shape, array.dtype))
        sem_shapes.append(pltpu.SemaphoreType.DMA((kind.count,)))
        sem_shapes.append(pltpu.SemaphoreType.DMA((kind.count,)))
        sem_shapes.append(pltpu.SemaphoreType.DMA)
    return pl.pallas_call(
        kernel,
        out_shape=out_shape,
        in_specs=[pl.BlockSpec(memory_space=pltpu.VMEM)] * flows,
        out_specs=[pl.BlockSpec(memory_space=pl.ANY)] * flows,
        scratch_shapes=sem_shapes,
        compiler_params=pltpu.CompilerParams(
            collective_id=call_id, has_side_effects=True, vmem_limit_bytes=48 * 2**20
        ),
        name=name,
    )(*arrays)


def plain(name, call_id, *pairs):
    outs = []
    for kind, array in pairs:
        if kind is CtxGather:
            outs.append(lax.all_gather(array, "ctx", axis=0))
        elif kind is WshGather:
            outs.append(lax.all_gather(array, "wsh", axis=0))
        elif kind is CtxSwap:
            outs.append(lax.all_to_all(array, "ctx", 0, 0, tiled=True))
        else:
            outs.append(lax.all_to_all(array, "wsh", 0, 0, tiled=True))
    return outs


class LineGather:
    count = 12

    def __init__(self, place, src, dst, sems):
        self.p, self.src, self.dst, self.sems = place, src, dst, sems

    def x_copy(self, source_z, src, slot):
        p = self.p
        return remote(src, self.dst.at[slot], self.sems, source_z, (p.ctx_of(0, 1), p.s))

    def up_copy(self, source_z, src, slot):
        p = self.p
        to = (p.z + 1) * 2 + p.x
        return remote(src, self.dst.at[slot], self.sems, 4 + source_z, (to, p.s))

    def down_copy(self, source_z, src, slot):
        p = self.p
        to = (p.z - 1) * 2 + p.x
        return remote(src, self.dst.at[slot], self.sems, 8 + source_z, (to, p.s))

    def start(self):
        p = self.p

        @pl.when(p.z < 3)
        def _():
            self.up_copy(p.z, self.src, p.c).start()

        @pl.when(p.z > 0)
        def _():
            self.down_copy(p.z, self.src, p.c).start()

        self.x_copy(p.z, self.src, p.c).start()

    def advance(self, step):
        p = self.p
        low, high = p.z - step, p.z + step

        @pl.when(low >= 0)
        def _():
            slot = low * 2 + p.x
            self.up_copy(low, self.dst.at[slot], slot).wait_recv()

            @pl.when(p.z < 3)
            def _():
                self.up_copy(low, self.dst.at[slot], slot).start()

            self.x_copy(low, self.dst.at[slot], slot).start()

        @pl.when(high <= 3)
        def _():
            slot = high * 2 + p.x
            self.down_copy(high, self.dst.at[slot], slot).wait_recv()

            @pl.when(p.z > 0)
            def _():
                self.down_copy(high, self.dst.at[slot], slot).start()

            self.x_copy(high, self.dst.at[slot], slot).start()

    def across(self, source_z):
        slot = source_z * 2 + 1 - self.p.x
        self.x_copy(source_z, self.dst.at[slot], slot).wait_recv()

    def finish(self):
        p = self.p
        for source_z in range(4):
            slot = source_z * 2 + p.x
            self.x_copy(source_z, self.dst.at[slot], slot).wait_send()

            @pl.when((source_z <= p.z) & (p.z < 3))
            def _(source_z=source_z, slot=slot):
                self.up_copy(source_z, self.dst.at[slot], slot).wait_send()

            @pl.when((source_z >= p.z) & (p.z > 0))
            def _(source_z=source_z, slot=slot):
                self.down_copy(source_z, self.dst.at[slot], slot).wait_send()


class PairGather:
    count = 3

    def __init__(self, place, src, dst, sems):
        self.p, self.src, self.dst, self.sems = place, src, dst, sems
        self.partner = (place.c, place.wsh_of(0, 1))
        self.over = (place.c, place.wsh_of(1, 0))

    def start(self):
        p = self.p
        self.first = remote(self.src, self.dst.at[p.s], self.sems, 0, self.over)
        self.first.start()
        self.second = remote(self.src, self.dst.at[p.s], self.sems, 1, self.partner)
        self.second.start()

    def relay(self):
        block = self.dst.at[self.over[1]]
        remote(block, block, self.sems, 0, self.over).wait_recv()
        self.third = remote(block, block, self.sems, 2, self.partner)
        self.third.start()

    def arrived(self):
        block = self.dst.at[self.partner[1]]
        remote(block, block, self.sems, 1, self.partner).wait_recv()
        block = self.dst.at[self.p.wsh_of(1, 1)]
        remote(block, block, self.sems, 2, self.partner).wait_recv()

    def finish(self):
        self.first.wait_send()
        self.second.wait_send()
        self.third.wait_send()


def greet_devices(devices):
    barrier = pltpu.get_barrier_semaphore()
    for device in devices:
        pl.semaphore_signal(barrier, inc=1, device_id=device, device_id_type=MESH_ID)
    pl.semaphore_wait(barrier, len(devices))


def ctx_peers(p):
    return [((p.c + step) % 8, p.s) for step in range(1, 8)]


def wsh_peers(p):
    return [(p.c, (p.s + step) % 4) for step in range(1, 4)]


def nt(left, right):
    return lax.dot_general(
        left, right, (((1,), (1,)), ((), ())), preferred_element_type=jnp.float32
    )


def nn(left, right):
    return jnp.dot(left, right, preferred_element_type=jnp.float32)


def tn(left, right):
    return lax.dot_general(
        left, right, (((0,), (0,)), ((), ())), preferred_element_type=jnp.float32
    )


def normalized(values):
    row_mean = jnp.mean(values, axis=-1, keepdims=True)
    centered = values - row_mean
    variance = jnp.mean(centered * centered, axis=-1, keepdims=True)
    scale = lax.rsqrt(variance + norm_eps)
    return centered * scale, scale


def forward_kernel(
    tok, cot, vec, w_project, w_combine, w_expand, pos_row, pos_col,
    n1, q_out, k_out, v_out, wp, wc, we, dy, table, attended, lse, middle, two, cols,
    tok_all, vec_all, att_low, att_rows, two_mine,
    g_sems, pair_send, pair_recv, we_send, we_recv, att_send, att_recv, col_send, col_recv, loc,
):
    p = Place()
    rows, width = tok.shape
    total = n1.shape[0]
    shard = w_combine.shape[0]
    hc = q_out.shape[1]
    low = jnp.bfloat16
    own_wp = [
        pltpu.make_async_copy(
            w_project.at[:, pl.ds(pl.multiple_of(part * width + p.c * hc, hc), hc)],
            wp.at[p.s, :, pl.ds(part * hc, hc)],
            loc.at[part],
        )
        for part in range(3)
    ]
    own = [
        pltpu.make_async_copy(tok, tok_all.at[p.c], loc.at[3]),
        pltpu.make_async_copy(vec, vec_all.at[p.s], loc.at[4]),
        pltpu.make_async_copy(w_combine, wc.at[p.s], loc.at[5]),
        pltpu.make_async_copy(cot, dy.at[p.s], loc.at[6]),
        pltpu.make_async_copy(
            w_expand.at[:, pl.ds(pl.multiple_of(p.s * width, width), width)],
            we.at[p.s],
            loc.at[7],
        ),
    ]
    for copy in own_wp + own:
        copy.start()
    greet_devices(ctx_peers(p) + wsh_peers(p))
    gather = LineGather(p, tok, tok_all, (g_sems.at[0], g_sems.at[1]))
    gather.start()

    def pair(index, src, dst):
        return PairGather(p, src, dst, (pair_send.at[index], pair_recv.at[index]))

    vec_pair = pair(0, vec, vec_all)
    vec_pair.start()
    for copy in own_wp:
        copy.wait()
    wp_pair = pair(1, wp.at[p.s], wp)
    wp_pair.start()
    wc_pair = pair(2, w_combine, wc)
    wc_pair.start()
    dy_pair = pair(3, cot, dy)
    dy_pair.start()
    we_copies = []
    for index, (to_y, to_k) in enumerate(((1, 1), (1, 0), (0, 1))):
        to = p.wsh_of(to_y, to_k)
        copy = remote(
            w_expand.at[:, pl.ds(pl.multiple_of(to * width, width), width)],
            we.at[p.s],
            (we_send, we_recv),
            index,
            (p.c, to),
        )
        copy.start()
        we_copies.append(copy)

    vec_pair.relay()
    own[1].wait()
    vec_pair.arrived()
    for source in range(4):
        table[:, source * shard : (source + 1) * shard] = vec_all[source].astype(jnp.float32)
    gain, bias = table[0:1, :], table[1:2, :]

    def norm_block(slot):
        scaled, _ = normalized(tok_all[slot].astype(jnp.float32))
        n1[pl.ds(pl.multiple_of(slot * rows, rows), rows), :] = (scaled * gain + bias).astype(low)

    own[0].wait()
    gather.advance(1)
    wp_pair.relay()
    gather.advance(2)
    wc_pair.relay()
    gather.advance(3)
    step_z = 1 - 2 * (p.z // 2)

    def own_line(index, carry):
        norm_block((p.z + index * step_z + 4) % 4 * 2 + p.x)
        return carry

    lax.fori_loop(0, 4, own_line, 0)

    def other_line(index, carry):
        source_z = (p.z + index * step_z + 4) % 4
        gather.across(source_z)
        norm_block(source_z * 2 + 1 - p.x)
        return carry

    lax.fori_loop(0, 4, other_line, 0)
    wp_pair.arrived()
    head_cols = pl.ds(pl.multiple_of(p.c * hc, hc), hc)
    bias_q, bias_v = table[2:3, head_cols], table[3:4, head_cols]

    def project(index, carry):
        part = pl.ds(pl.multiple_of(index * 256, 256), 256)
        out = nn(n1[part, :], wp[...].reshape(width, 3 * hc))
        q_out[part, :] = (out[:, :hc] + bias_q).astype(low)
        k_out[part, :] = out[:, hc : 2 * hc].astype(low)
        v_out[part, :] = (out[:, 2 * hc :] + bias_v).astype(low)
        return carry

    lax.fori_loop(0, total // 256, project, 0)
    dy_pair.relay()
    wc_pair.arrived()
    dy_pair.arrived()

    scale = (width // HEADS) ** (-0.5)

    def att_send_to(dest):
        return pltpu.make_async_remote_copy(
            src_ref=att_low.at[dest],
            dst_ref=att_rows.at[:, head_cols],
            send_sem=att_send.at[dest],
            recv_sem=att_recv.at[p.c],
            device_id=(dest, p.s),
            device_id_type=MESH_ID,
        )

    def att_own():
        return pltpu.make_async_copy(att_low.at[p.c], att_rows.at[:, head_cols], loc.at[8])

    def attend(index, carry):
        part = pl.ds(pl.multiple_of(index * 256, 256), 256)
        queries = q_out[part, :]
        seen = pos_row[0:1, :] <= pos_col[part, :]
        first = lax.broadcasted_iota(jnp.int32, (256, hc), 1) < hc // 2
        outs, logs = [], []
        for head in range(2):
            mine = first if head == 0 else jnp.logical_not(first)
            scores = nt(jnp.where(mine, queries, jnp.zeros_like(queries)), k_out[...]) * scale
            scores = jnp.where(seen, scores, masked_score)
            peak = jnp.max(scores, axis=1, keepdims=True)
            grown = jnp.exp(scores - peak)
            whole = jnp.sum(grown, axis=1, keepdims=True)
            probs = (grown * (1.0 / whole)).astype(low)
            outs.append(nn(probs, v_out[...]))
            logs.append(peak + jnp.log(whole))
        mixed = jnp.where(first, outs[0], outs[1])
        attended[part, :] = mixed
        lse[part, :] = jnp.where(first, logs[0], logs[1])
        mixed_low = mixed.astype(low)
        for half in range(2):
            dest = index * 2 + half
            att_low[dest] = mixed_low[half * 128 : (half + 1) * 128]

            @pl.when(dest != p.c)
            def _(dest=dest):
                att_send_to(dest).start()

            @pl.when(dest == p.c)
            def _():
                att_own().start()

        return carry

    lax.fori_loop(0, total // 256, attend, 0)
    att_own().wait()
    for step in range(1, 8):
        source = (p.c + step) % 8
        landed = att_rows.at[:, pl.ds(pl.multiple_of(source * hc, hc), hc)]
        pltpu.make_async_remote_copy(
            src_ref=landed,
            dst_ref=landed,
            send_sem=att_send.at[source],
            recv_sem=att_recv.at[source],
            device_id=(source, p.s),
            device_id_type=MESH_ID,
        ).wait_recv()
    own[2].wait()
    mid = tok[...].astype(jnp.float32) + nn(att_rows[...], wc[...].reshape(width, width)) + table[4:5, :]
    middle[...] = mid
    scaled, _ = normalized(mid)
    two_mine[...] = (scaled * table[5:6, :] + table[6:7, :]).astype(low)
    two[p.s] = two_mine[...]
    two_pair = pair(4, two_mine, two)
    two_pair.start()
    col_copies = []
    for index, (to_y, to_k) in enumerate(((1, 1), (1, 0), (0, 1))):
        to = p.wsh_of(to_y, to_k)
        copy = remote(
            att_rows.at[:, pl.ds(pl.multiple_of(to * shard, shard), shard)],
            cols.at[p.s],
            (col_send, col_recv),
            index,
            (p.c, to),
        )
        copy.start()
        col_copies.append(copy)
    own_cols = pltpu.make_async_copy(
        att_rows.at[:, pl.ds(pl.multiple_of(p.s * shard, shard), shard)], cols.at[p.s], loc.at[9]
    )
    own_cols.start()
    two_pair.relay()
    two_pair.arrived()
    for index, (to_y, to_k) in enumerate(((1, 1), (1, 0), (0, 1))):
        source = p.wsh_of(to_y, to_k)
        remote(cols.at[source], cols.at[source], (col_send, col_recv), index, (p.c, source)).wait_recv()
        remote(we.at[source], we.at[source], (we_send, we_recv), index, (p.c, source)).wait_recv()
    own_cols.wait()
    own[3].wait()
    own[4].wait()
    for copy in we_copies + col_copies:
        copy.wait_send()
    gather.finish()
    for member in (vec_pair, wp_pair, wc_pair, dy_pair, two_pair):
        member.finish()
    for step in range(1, 8):
        att_send_to((p.c + step) % 8).wait_send()


def shape(dims, kind):
    return jax.ShapeDtypeStruct(dims, kind)


def forward_fused(tok, cot, vec, w_project, w_combine, w_expand, pos_row, pos_col):
    low, wide = jnp.bfloat16, jnp.float32
    rows, width = tok.shape
    total = rows * 8
    hc = width // 8
    shard = w_combine.shape[0]
    vmem, hbm = pl.BlockSpec(memory_space=pltpu.VMEM), pl.BlockSpec(memory_space=pl.ANY)
    dma = pltpu.SemaphoreType.DMA
    return pl.pallas_call(
        forward_kernel,
        out_shape=[
            shape((total, width), low),
            shape((total, hc), low),
            shape((total, hc), low),
            shape((total, hc), low),
            shape((4, shard, 3 * hc), low),
            shape((4, shard, width), low),
            shape((4, shard, width), low),
            shape((4, rows, width), low),
            shape((16, width), wide),
            shape((total, hc), wide),
            shape((total, hc), wide),
            shape((rows, width), wide),
            shape((4, rows, width), low),
            shape((4, rows, shard), low),
        ],
        in_specs=[vmem, vmem, vmem, hbm, vmem, hbm, vmem, vmem],
        out_specs=[vmem] * 6 + [hbm, hbm] + [vmem] * 6,
        scratch_shapes=[
            pltpu.VMEM((8, rows, width), low),
            pltpu.VMEM((4, 16, shard), low),
            pltpu.VMEM((8, rows, hc), low),
            pltpu.VMEM((rows, width), low),
            pltpu.VMEM((rows, width), low),
            dma((2, 12)),
            dma((5, 3)),
            dma((5, 3)),
            dma((3,)),
            dma((3,)),
            dma((8,)),
            dma((8,)),
            dma((3,)),
            dma((3,)),
            dma((10,)),
        ],
        compiler_params=pltpu.CompilerParams(
            collective_id=10, has_side_effects=True, vmem_limit_bytes=56 * 2**20
        ),
        name="forward",
    )(tok, cot, vec, w_project, w_combine, w_expand, pos_row, pos_col)


def adam_step(weight, gradient, first_moment, second_moment, clip_factor, step_value):
    clipped = gradient * clip_factor
    moment = beta_one * first_moment + (1.0 - beta_one) * clipped
    square = beta_two * second_moment + (1.0 - beta_two) * clipped * clipped
    moment_hat = moment / (1.0 - jnp.power(jnp.float32(beta_one), step_value))
    square_hat = square / (1.0 - jnp.power(jnp.float32(beta_two), step_value))
    update = -learn_rate * (
        moment_hat / (jnp.sqrt(square_hat) + adam_eps) + decay_rate * weight.astype(jnp.float32)
    )
    return (moment, square, update)


def body(
    tokens,
    output_cotangent,
    block_table,
    weight_project,
    weight_combine,
    weight_expand,
    weight_reduce,
    vectors,
    moment_project,
    square_project,
    moment_combine,
    square_combine,
    moment_expand,
    square_expand,
    moment_reduce,
    square_reduce,
    moment_vectors,
    square_vectors,
):
    low = jnp.bfloat16
    ctx_count, wsh_count = lax.axis_size("ctx"), lax.axis_size("wsh")
    ctx_index, wsh_index = lax.axis_index("ctx"), lax.axis_index("wsh")
    rows_dev, width = tokens.shape[1], tokens.shape[2]
    block_rows = rows_dev // 2
    total_rows = rows_dev * ctx_count
    group_rows = rows_dev * wsh_count
    head_size = width // HEADS
    score_scale = head_size ** (-0.5)
    head_cols = width // ctx_count
    local_heads = head_cols // head_size
    shard_rows = weight_project.shape[0]
    ff_width = weight_expand.shape[1]
    chunk = ff_width // wsh_count
    vec_rows = vectors.shape[0]
    fast = (ctx_count, wsh_count) == (FAST_CTX, FAST_WSH)
    swap = exchange if fast else plain

    sequence = tokens[0].astype(jnp.float32)
    cotangent_low = output_cotangent[0]
    cotangent = cotangent_low.astype(jnp.float32)

    heads = (total_rows, local_heads, head_size)
    positions = (
        block_table[:, None] * block_rows + jnp.arange(block_rows, dtype=jnp.int32)[None, :]
    ).reshape(total_rows)
    vec_pad = -vec_rows % 16
    vec_padded = jnp.pad(vectors, ((0, vec_pad), (0, 0)))
    if fast:
        (
            normed_all, queries, keys, values, project_parts, combine_parts, expand_parts,
            cot_parts, vec_table, attended, log_total, middle, two_parts, att_cols,
        ) = forward_fused(
            tokens[0], cotangent_low, vec_padded, weight_project, weight_combine, weight_expand,
            jnp.broadcast_to(positions[None, :], (8, total_rows)), positions[:, None],
        )
        vec_table = vec_table[:vec_rows]
        log_heads = log_total[:, ::head_size].T[:, :, None]
        expand_mine = expand_parts.reshape(width, chunk)
        project_mine = project_parts.reshape(width, 3 * head_cols)
        full_combine = combine_parts.reshape(width, width)
        cot_group = cot_parts.reshape(group_rows, width)
        two_group = two_parts.reshape(group_rows, width)
        visible = positions[None, None, :] <= positions[None, :, None]
        query_heads, key_heads, value_heads = (
            queries.reshape(heads),
            keys.reshape(heads),
            values.reshape(heads),
        )
        attended_heads = attended.reshape(heads)
        scores = (
            jnp.einsum("qhd,khd->hqk", query_heads, key_heads, preferred_element_type=jnp.float32)
            * score_scale
        )
        soft = jnp.where(visible, jnp.exp(scores - log_heads), 0.0)
        soft_low = soft.astype(low)
    else:
        project_cols = lax.dynamic_slice_in_dim(
            weight_project.reshape(shard_rows, 3, ctx_count, head_cols), ctx_index, 1, axis=2
        ).reshape(shard_rows, 3 * head_cols)

        (vec_parts,) = swap("vec", 0, (WshGather, vec_padded))
        vec_table = (
            vec_parts[:, :vec_rows].transpose(1, 0, 2).reshape(vec_rows, width).astype(jnp.float32)
        )
        normed_one = layer_norm(sequence, vec_table[0], vec_table[1]).astype(low)
        normed_all, project_parts, cot_parts, combine_parts, expand_parts = swap(
            "front",
            1,
            (CtxGather, normed_one),
            (WshGather, project_cols),
            (WshGather, cotangent_low),
            (WshGather, weight_combine),
            (WshSwap, weight_expand.reshape(shard_rows, wsh_count, chunk).transpose(1, 0, 2)),
        )
        normed_all = normed_all.reshape(total_rows, width)
        project_mine = project_parts.reshape(width, 3 * head_cols)
        full_combine = combine_parts.reshape(width, width)
        expand_mine = expand_parts.reshape(width, chunk)
        cot_group = cot_parts.reshape(group_rows, width)

        qkv = matmul(normed_all, project_mine)
        bias_cols = lax.dynamic_slice_in_dim(
            vec_table[:4].reshape(4, ctx_count, head_cols), ctx_index, 1, axis=1
        ).reshape(4, head_cols)
        queries = (qkv[:, :head_cols] + bias_cols[2]).astype(low)
        keys = qkv[:, head_cols : 2 * head_cols].astype(low)
        values = (qkv[:, 2 * head_cols :] + bias_cols[3]).astype(low)
        visible = positions[None, None, :] <= positions[None, :, None]
        query_heads, key_heads, value_heads = (
            queries.reshape(heads),
            keys.reshape(heads),
            values.reshape(heads),
        )
        scores = (
            jnp.einsum("qhd,khd->hqk", query_heads, key_heads, preferred_element_type=jnp.float32)
            * score_scale
        )
        scores = jnp.where(visible, scores, masked_score)
        peak = jnp.max(scores, axis=2, keepdims=True)
        grown = jnp.exp(scores - peak)
        soft = grown / jnp.sum(grown, axis=2, keepdims=True)
        soft_low = soft.astype(low)
        attended_heads = jnp.einsum(
            "hqk,khd->qhd", soft_low, value_heads, preferred_element_type=jnp.float32
        )
        attended = attended_heads.reshape(total_rows, head_cols)
        (att_parts,) = swap(
            "attended", 2, (CtxSwap, attended.astype(low).reshape(ctx_count, rows_dev, head_cols))
        )
        attended_rows = att_parts.transpose(1, 0, 2).reshape(rows_dev, width)

        middle = sequence + matmul(attended_rows, full_combine) + vec_table[4]
        normed_two = layer_norm(middle, vec_table[5], vec_table[6]).astype(low)
        two_parts, att_cols = swap(
            "normed_two",
            3,
            (WshGather, normed_two),
            (WshSwap, attended_rows.reshape(rows_dev, wsh_count, shard_rows).transpose(1, 0, 2)),
        )
        two_group = two_parts.reshape(group_rows, width)

    bias_ff = lax.dynamic_slice_in_dim(vec_table[8:].reshape(-1), wsh_index * chunk, chunk)
    hidden_pre = matmul(two_group, expand_mine) + bias_ff
    hidden, gelu_back = jax.vjp(gelu_exact, hidden_pre)
    hidden = hidden.astype(low)
    out_partial = matmul(hidden, weight_reduce)
    pre_grad = gelu_back(matmul_right_t(cot_group, weight_reduce))[0].astype(low)
    two_partial = matmul_right_t(pre_grad, expand_mine)
    part_shape = (wsh_count, rows_dev, width)
    two_terms, out_terms = swap(
        "ff_sums",
        4,
        (WshSwap, two_partial.astype(low).reshape(part_shape)),
        (WshSwap, out_partial.astype(low).reshape(part_shape)),
    )
    layer_output = middle + jnp.sum(out_terms.astype(jnp.float32), axis=0) + vec_table[7]
    normed_two_grad = jnp.sum(two_terms.astype(jnp.float32), axis=0)
    norm_two_back = jax.vjp(layer_norm, middle, vec_table[5], vec_table[6])[1](normed_two_grad)
    middle_grad = cotangent + norm_two_back[0]
    branch_grad = middle_grad.astype(low)
    attended_grad_rows = matmul_right_t(branch_grad, full_combine).astype(low)
    att_grad_parts, branch_parts = swap(
        "attended_grad",
        5,
        (CtxSwap, attended_grad_rows.reshape(rows_dev, ctx_count, head_cols).transpose(1, 0, 2)),
        (WshGather, branch_grad),
    )
    branch_group = branch_parts.reshape(group_rows, width)
    attended_grad = att_grad_parts.reshape(total_rows, head_cols)

    grad_reduce = matmul_left_t(hidden, cot_group)
    grad_expand = matmul_left_t(two_group, pre_grad)
    grad_combine = matmul_left_t(att_cols.reshape(group_rows, shard_rows), branch_group)

    grad_heads = attended_grad.reshape(heads)
    delta = jnp.sum(
        grad_heads.astype(jnp.float32) * attended_heads, axis=2
    ).transpose(1, 0)[:, :, None]
    soft_grad = jnp.einsum(
        "qhd,khd->hqk", grad_heads, value_heads, preferred_element_type=jnp.float32
    )
    score_grad = (soft * (soft_grad - delta)).astype(low)
    query_grad = (
        jnp.einsum("hqk,khd->qhd", score_grad, key_heads, preferred_element_type=jnp.float32)
        * score_scale
    )
    key_grad = (
        jnp.einsum("hqk,qhd->khd", score_grad, query_heads, preferred_element_type=jnp.float32)
        * score_scale
    )
    value_grad = jnp.einsum(
        "hqk,qhd->khd", soft_low, grad_heads, preferred_element_type=jnp.float32
    )
    flat = (total_rows, head_cols)
    qkv_grad = jnp.concatenate(
        [member.reshape(flat).astype(low) for member in (query_grad, key_grad, value_grad)], axis=1
    )
    grad_project = matmul_left_t(normed_all, qkv_grad)
    one_partial = matmul_right_t(qkv_grad, project_mine)

    cut = shard_rows // ctx_count
    cut_reduce = chunk // ctx_count
    for_ctx = jnp.concatenate(
        [
            grad_reduce.astype(low).reshape(ctx_count, cut_reduce, width),
            grad_combine.astype(low).reshape(ctx_count, cut, width),
        ],
        axis=1,
    )
    expand_ctx = (
        grad_expand.astype(low)
        .reshape(wsh_count, ctx_count, cut, chunk)
        .transpose(1, 0, 2, 3)
        .reshape(ctx_count, wsh_count * cut, chunk)
    )
    ctx_terms, expand_terms, one_terms, project_terms = swap(
        "grad_sums",
        6,
        (CtxSwap, for_ctx),
        (CtxSwap, expand_ctx),
        (CtxSwap, one_partial.astype(low).reshape(ctx_count, rows_dev, width)),
        (WshSwap, grad_project.astype(low).reshape(wsh_count, shard_rows, 3 * head_cols)),
    )
    normed_one_grad = jnp.sum(one_terms.astype(jnp.float32), axis=0)
    norm_one_back = jax.vjp(layer_norm, sequence, vec_table[0], vec_table[1])[1](normed_one_grad)
    input_gradient = (middle_grad + norm_one_back[0]).astype(low)
    ctx_piece = jnp.sum(ctx_terms.astype(jnp.float32), axis=0).astype(low)
    expand_piece = jnp.sum(expand_terms.astype(jnp.float32), axis=0).astype(low)
    project_piece = jnp.sum(project_terms.astype(jnp.float32), axis=0).astype(low)

    def spread(columns, start):
        return lax.dynamic_update_slice(
            jnp.zeros((width,), jnp.float32), columns, (start,)
        )

    ff_terms = lax.dynamic_update_slice(
        jnp.zeros((ff_width,), jnp.float32),
        jnp.sum(pre_grad.astype(jnp.float32), axis=0),
        (wsh_index * chunk,),
    ).reshape(-1, width)
    head_start = ctx_index * head_cols
    query_sum = jnp.sum(qkv_grad[:, :head_cols].astype(jnp.float32), axis=0)
    value_sum = jnp.sum(qkv_grad[:, 2 * head_cols :].astype(jnp.float32), axis=0)
    vec_terms = jnp.concatenate(
        [
            jnp.stack(
                [
                    norm_one_back[1],
                    norm_one_back[2],
                    spread(query_sum, head_start),
                    spread(value_sum, head_start),
                    jnp.sum(branch_grad.astype(jnp.float32), axis=0),
                    norm_two_back[1],
                    norm_two_back[2],
                    jnp.sum(cotangent, axis=0),
                ]
            ),
            ff_terms,
            jnp.zeros((vec_pad, width), jnp.float32),
        ],
        axis=0,
    )
    vec_cols = vectors.shape[1]
    vec_swapped, expand_rows = swap(
        "vec_sums",
        7,
        (WshSwap, vec_terms.reshape(-1, wsh_count, vec_cols).transpose(1, 0, 2)),
        (WshSwap, expand_piece.reshape(wsh_count, cut, chunk)),
    )
    vec_mine = jnp.sum(vec_swapped, axis=0)
    expand_mine_rows = expand_rows.transpose(1, 0, 2).reshape(cut, ff_width)
    square_mine = (
        jnp.sum(jnp.square(ctx_piece.astype(jnp.float32)))
        + jnp.sum(jnp.square(expand_rows.astype(jnp.float32)))
        + jnp.sum(jnp.square(project_piece.astype(jnp.float32)))
    )
    ctx_all, expand_all, project_all, vec_all, square_ctx = swap(
        "grads",
        8,
        (CtxGather, ctx_piece),
        (CtxGather, expand_mine_rows),
        (CtxGather, project_piece),
        (CtxGather, vec_mine),
        (CtxGather, jnp.full((16, 128), square_mine, jnp.float32)),
    )
    sum_reduce = ctx_all[:, :cut_reduce].reshape(chunk, width).astype(jnp.float32)
    sum_combine = ctx_all[:, cut_reduce:].reshape(shard_rows, width).astype(jnp.float32)
    sum_expand = expand_all.reshape(shard_rows, ff_width).astype(jnp.float32)
    sum_project = (
        project_all.reshape(ctx_count, shard_rows, 3, head_cols)
        .transpose(1, 2, 0, 3)
        .reshape(shard_rows, 3 * width)
        .astype(jnp.float32)
    )
    sum_vectors = jnp.sum(vec_all, axis=0)[:vec_rows]
    square_part = jnp.sum(square_ctx[:, 0, 0]) + jnp.sum(jnp.square(sum_vectors))
    (square_all,) = swap(
        "squares", 9, (WshGather, jnp.full((8, 128), square_part, jnp.float32))
    )
    norm_value = jnp.sqrt(jnp.sum(square_all[:, 0, 0]))
    params_total = 4 * width * width + 2 * width * ff_width + vec_rows * width
    clip_max = jnp.sqrt(jnp.float32(params_total))
    clip_factor = clip_max / jnp.maximum(norm_value, clip_max)
    step_value = jnp.float32(STEP)
    results = [layer_output.astype(low)[None], input_gradient[None], norm_value.reshape(1)]
    for weight, total, first, second in (
        (weight_project, sum_project, moment_project, square_project),
        (weight_combine, sum_combine, moment_combine, square_combine),
        (weight_expand, sum_expand, moment_expand, square_expand),
        (weight_reduce, sum_reduce, moment_reduce, square_reduce),
        (vectors, sum_vectors, moment_vectors, square_vectors),
    ):
        results.append(total)
        results.extend(adam_step(weight, total, first, second, clip_factor, step_value))
    return tuple(results)


def solution(mesh):
    rows, cols = P("wsh", None), P(None, "wsh")
    token = P("wsh", "ctx", None)
    return jax.shard_map(
        body,
        mesh=mesh,
        in_specs=(token, token, P(), rows, rows, rows, rows, cols) + (rows,) * 8 + (cols,) * 2,
        out_specs=(token, token, P()) + (rows,) * 16 + (cols,) * 4,
        check_vma=False,
    )
```

```python
import jax
import jax.numpy as jnp
from jax import lax
from jax.experimental import pallas as pl
from jax.experimental.pallas import tpu as pltpu
from jax.sharding import PartitionSpec as P

HEADS = 16
STEP = 4

norm_eps = 1e-05
masked_score = -1e30
beta_one = 0.9
beta_two = 0.95
learn_rate = 0.02
decay_rate = 0.1
adam_eps = 1e-08

MESH_ID = pl.DeviceIdType.MESH
FAST_CTX, FAST_WSH = 8, 4


def layer_norm(values, norm_gain, norm_bias):
    row_mean = jnp.mean(values, axis=-1, keepdims=True)
    centered = values - row_mean
    variance = jnp.mean(centered * centered, axis=-1, keepdims=True)
    return centered * lax.rsqrt(variance + norm_eps) * norm_gain + norm_bias


def gelu_exact(values):
    return jax.nn.gelu(values, approximate=False)


def matmul(left, right):
    return jnp.dot(left, right, preferred_element_type=jnp.float32)


def matmul_left_t(left, right):
    return lax.dot_general(
        left, right, (((0,), (0,)), ((), ())), preferred_element_type=jnp.float32
    )


def matmul_right_t(left, right):
    return lax.dot_general(
        left, right, (((1,), (1,)), ((), ())), preferred_element_type=jnp.float32
    )


class Place:
    def __init__(self):
        self.c = lax.axis_index("ctx")
        self.s = lax.axis_index("wsh")
        self.z, self.x = self.c // 2, self.c % 2
        self.y, self.k = self.s // 2, self.s % 2

    def ctx_of(self, dz, dx):
        return (self.z + dz + 4) % 4 * 2 + (self.x + dx) % 2

    def wsh_of(self, dy, dk):
        return (self.y + dy) % 2 * 2 + (self.k + dk) % 2


def remote(src, dst, sems, index, device):
    return pltpu.make_async_remote_copy(
        src_ref=src,
        dst_ref=dst,
        send_sem=sems[0].at[index],
        recv_sem=sems[1].at[index],
        device_id=device,
        device_id_type=MESH_ID,
    )


class Flow:
    count = 0
    local = 1

    def __init__(self, place, src, dst, sems, local_sem):
        self.place, self.src, self.dst = place, src, dst
        self.sems, self.local_sem = sems, local_sem
        self.sent = []

    def send(self, index, src, dst, device):
        copy = remote(src, dst, self.sems, index, device)
        copy.start()
        self.sent.append(copy)

    def arrived(self, index, dst, device):
        remote(dst, dst, self.sems, index, device).wait_recv()

    def keep(self, src, dst):
        self.kept = pltpu.make_async_copy(src, dst, self.local_sem)
        self.kept.start()

    def phase(self, number):
        pass

    def finish(self):
        for copy in self.sent:
            copy.wait_send()
        self.kept.wait()


class CtxGather(Flow):
    count = 11
    groups = ("x", "z")

    def half(self, slot, which):
        rows = self.dst.shape[1] // 2
        return self.dst.at[slot, pl.ds(which * rows, rows)]

    def phase(self, number):
        p = self.place
        across = (p.ctx_of(0, 1), p.s)
        above = (p.ctx_of(1, 0), p.s)
        below = (p.ctx_of(-1, 0), p.s)
        own = self.dst.at[p.c]
        slot = p.ctx_of
        if number == 0:
            self.send(0, self.src, own, across)
            self.send(1, self.src, own, below)
            self.send(2, self.src, own, above)
            self.keep(self.src, own)
        if number == 1:
            self.arrived(1, self.dst.at[slot(1, 0)], above)
            self.send(5, self.half(slot(1, 0), 0), self.half(slot(1, 0), 0), below)
            self.send(6, self.half(slot(1, 0), 1), self.half(slot(1, 0), 1), across)
            self.arrived(2, self.dst.at[slot(-1, 0)], below)
            self.send(7, self.half(slot(-1, 0), 1), self.half(slot(-1, 0), 1), above)
            self.send(8, self.half(slot(-1, 0), 1), self.half(slot(-1, 0), 1), across)
            self.arrived(0, self.dst.at[slot(0, 1)], across)
            self.send(3, self.half(slot(0, 1), 0), self.half(slot(0, 1), 0), below)
            self.send(4, self.half(slot(0, 1), 0), self.half(slot(0, 1), 0), above)
        if number == 2:
            self.arrived(3, self.half(slot(1, 1), 0), above)
            self.send(9, self.half(slot(1, 1), 0), self.half(slot(1, 1), 0), below)
            self.arrived(8, self.half(slot(-1, 1), 1), across)
            self.send(10, self.half(slot(-1, 1), 1), self.half(slot(-1, 1), 1), above)
        if number == 3:
            self.arrived(4, self.half(slot(-1, 1), 0), below)
            self.arrived(6, self.half(slot(1, 1), 1), across)
            self.arrived(5, self.half(slot(2, 0), 0), above)
            self.arrived(7, self.half(slot(2, 0), 1), below)
            self.arrived(9, self.half(slot(2, 1), 0), above)
            self.arrived(10, self.half(slot(2, 1), 1), below)
            self.finish()


class CtxSwap(Flow):
    count = 7
    groups = ("x", "z", "ctx")
    steps = ((2, 1), (2, 0), (1, 1), (-1, 1), (1, 0), (-1, 0), (0, 1))

    def phase(self, number):
        p = self.place
        if number == 0:
            for index, (dz, dx) in enumerate(self.steps):
                to = p.ctx_of(dz, dx)
                self.send(index, self.src.at[to], self.dst.at[p.c], (to, p.s))
            self.keep(self.src.at[p.c], self.dst.at[p.c])
        if number == 3:
            for index, (dz, dx) in enumerate(self.steps):
                source = p.ctx_of(-dz, dx)
                self.arrived(index, self.dst.at[source], (source, p.s))
            self.finish()


class WshGather(Flow):
    count = 3
    groups = ("y", "core")

    def phase(self, number):
        p = self.place
        partner, over = p.wsh_of(0, 1), p.wsh_of(1, 0)
        own = self.dst.at[p.s]
        if number == 0:
            self.send(1, self.src, own, (p.c, over))
            self.send(0, self.src, own, (p.c, partner))
            self.keep(self.src, own)
        if number == 2:
            self.arrived(1, self.dst.at[over], (p.c, over))
            self.send(2, self.dst.at[over], self.dst.at[over], (p.c, partner))
        if number == 3:
            self.arrived(0, self.dst.at[partner], (p.c, partner))
            self.arrived(2, self.dst.at[p.wsh_of(1, 1)], (p.c, partner))
            self.finish()


class WshSwap(Flow):
    count = 3
    groups = ("y", "core", "wsh")
    steps = ((1, 1), (1, 0), (0, 1))

    def phase(self, number):
        p = self.place
        if number == 0:
            for index, (dy, dk) in enumerate(self.steps):
                to = p.wsh_of(dy, dk)
                self.send(index, self.src.at[to], self.dst.at[p.s], (p.c, to))
            self.keep(self.src.at[p.s], self.dst.at[p.s])
        if number == 3:
            for index, (dy, dk) in enumerate(self.steps):
                source = p.wsh_of(dy, dk)
                self.arrived(index, self.dst.at[source], (p.c, source))
            self.finish()


def greet(place, groups):
    peers = set()
    if "x" in groups:
        peers.add("x")
    others = []
    if "ctx" in groups:
        for dz, dx in CtxSwap.steps:
            others.append((place.ctx_of(dz, dx), place.s))
    else:
        if "x" in groups:
            others.append((place.ctx_of(0, 1), place.s))
        if "z" in groups:
            others.append((place.ctx_of(1, 0), place.s))
            others.append((place.ctx_of(-1, 0), place.s))
    if "wsh" in groups:
        for dy, dk in WshSwap.steps:
            others.append((place.c, place.wsh_of(dy, dk)))
    else:
        if "y" in groups:
            others.append((place.c, place.wsh_of(1, 0)))
        if "core" in groups:
            others.append((place.c, place.wsh_of(0, 1)))
    barrier = pltpu.get_barrier_semaphore()
    for device in others:
        pl.semaphore_signal(barrier, inc=1, device_id=device, device_id_type=MESH_ID)
    pl.semaphore_wait(barrier, len(others))


def exchange(name, call_id, *pairs):
    kinds = [kind for kind, _ in pairs]
    arrays = [array for _, array in pairs]
    flows = len(pairs)
    groups = set()
    for kind in kinds:
        groups.update(kind.groups)

    def kernel(*refs):
        sources, targets = refs[:flows], refs[flows : 2 * flows]
        scratch = refs[2 * flows :]
        place = Place()
        greet(place, groups)
        running = []
        for index, kind in enumerate(kinds):
            sems = (scratch[3 * index], scratch[3 * index + 1])
            running.append(
                kind(place, sources[index], targets[index], sems, scratch[3 * index + 2])
            )
        for number in range(4):
            for flow in running:
                flow.phase(number)

    out_shape = []
    sem_shapes = []
    sizes = {CtxGather: FAST_CTX, WshGather: FAST_WSH}
    for kind, array in pairs:
        shape = array.shape if kind in (CtxSwap, WshSwap) else (sizes[kind],) + array.shape
        out_shape.append(jax.ShapeDtypeStruct(shape, array.dtype))
        sem_shapes.append(pltpu.SemaphoreType.DMA((kind.count,)))
        sem_shapes.append(pltpu.SemaphoreType.DMA((kind.count,)))
        sem_shapes.append(pltpu.SemaphoreType.DMA)
    return pl.pallas_call(
        kernel,
        out_shape=out_shape,
        in_specs=[pl.BlockSpec(memory_space=pltpu.VMEM)] * flows,
        out_specs=[pl.BlockSpec(memory_space=pl.ANY)] * flows,
        scratch_shapes=sem_shapes,
        compiler_params=pltpu.CompilerParams(
            collective_id=call_id, has_side_effects=True, vmem_limit_bytes=48 * 2**20
        ),
        name=name,
    )(*arrays)


def plain(name, call_id, *pairs):
    outs = []
    for kind, array in pairs:
        if kind is CtxGather:
            outs.append(lax.all_gather(array, "ctx", axis=0))
        elif kind is WshGather:
            outs.append(lax.all_gather(array, "wsh", axis=0))
        elif kind is CtxSwap:
            outs.append(lax.all_to_all(array, "ctx", 0, 0, tiled=True))
        else:
            outs.append(lax.all_to_all(array, "wsh", 0, 0, tiled=True))
    return outs


class LineGather:
    count = 12

    def __init__(self, place, src, dst, sems):
        self.p, self.src, self.dst, self.sems = place, src, dst, sems

    def x_copy(self, source_z, src, slot):
        p = self.p
        return remote(src, self.dst.at[slot], self.sems, source_z, (p.ctx_of(0, 1), p.s))

    def up_copy(self, source_z, src, slot):
        p = self.p
        to = (p.z + 1) * 2 + p.x
        return remote(src, self.dst.at[slot], self.sems, 4 + source_z, (to, p.s))

    def down_copy(self, source_z, src, slot):
        p = self.p
        to = (p.z - 1) * 2 + p.x
        return remote(src, self.dst.at[slot], self.sems, 8 + source_z, (to, p.s))

    def start(self):
        p = self.p

        @pl.when(p.z < 3)
        def _():
            self.up_copy(p.z, self.src, p.c).start()

        @pl.when(p.z > 0)
        def _():
            self.down_copy(p.z, self.src, p.c).start()

        self.x_copy(p.z, self.src, p.c).start()

    def advance(self, step):
        p = self.p
        low, high = p.z - step, p.z + step

        @pl.when(low >= 0)
        def _():
            slot = low * 2 + p.x
            self.up_copy(low, self.dst.at[slot], slot).wait_recv()

            @pl.when(p.z < 3)
            def _():
                self.up_copy(low, self.dst.at[slot], slot).start()

            self.x_copy(low, self.dst.at[slot], slot).start()

        @pl.when(high <= 3)
        def _():
            slot = high * 2 + p.x
            self.down_copy(high, self.dst.at[slot], slot).wait_recv()

            @pl.when(p.z > 0)
            def _():
                self.down_copy(high, self.dst.at[slot], slot).start()

            self.x_copy(high, self.dst.at[slot], slot).start()

    def across(self, source_z):
        slot = source_z * 2 + 1 - self.p.x
        self.x_copy(source_z, self.dst.at[slot], slot).wait_recv()

    def finish(self):
        p = self.p
        for source_z in range(4):
            slot = source_z * 2 + p.x
            self.x_copy(source_z, self.dst.at[slot], slot).wait_send()

            @pl.when((source_z <= p.z) & (p.z < 3))
            def _(source_z=source_z, slot=slot):
                self.up_copy(source_z, self.dst.at[slot], slot).wait_send()

            @pl.when((source_z >= p.z) & (p.z > 0))
            def _(source_z=source_z, slot=slot):
                self.down_copy(source_z, self.dst.at[slot], slot).wait_send()


class PairGather:
    count = 3

    def __init__(self, place, src, dst, sems):
        self.p, self.src, self.dst, self.sems = place, src, dst, sems
        self.partner = (place.c, place.wsh_of(0, 1))
        self.over = (place.c, place.wsh_of(1, 0))

    def start(self):
        p = self.p
        self.first = remote(self.src, self.dst.at[p.s], self.sems, 0, self.over)
        self.first.start()
        self.second = remote(self.src, self.dst.at[p.s], self.sems, 1, self.partner)
        self.second.start()

    def relay(self):
        block = self.dst.at[self.over[1]]
        remote(block, block, self.sems, 0, self.over).wait_recv()
        self.third = remote(block, block, self.sems, 2, self.partner)
        self.third.start()

    def arrived(self):
        block = self.dst.at[self.partner[1]]
        remote(block, block, self.sems, 1, self.partner).wait_recv()
        block = self.dst.at[self.p.wsh_of(1, 1)]
        remote(block, block, self.sems, 2, self.partner).wait_recv()

    def finish(self):
        self.first.wait_send()
        self.second.wait_send()
        self.third.wait_send()


def greet_devices(devices):
    barrier = pltpu.get_barrier_semaphore()
    for device in devices:
        pl.semaphore_signal(barrier, inc=1, device_id=device, device_id_type=MESH_ID)
    pl.semaphore_wait(barrier, len(devices))


def ctx_peers(p):
    return [((p.c + step) % 8, p.s) for step in range(1, 8)]


def wsh_peers(p):
    return [(p.c, (p.s + step) % 4) for step in range(1, 4)]


def nt(left, right):
    return lax.dot_general(
        left, right, (((1,), (1,)), ((), ())), preferred_element_type=jnp.float32
    )


def nn(left, right):
    return jnp.dot(left, right, preferred_element_type=jnp.float32)


def tn(left, right):
    return lax.dot_general(
        left, right, (((0,), (0,)), ((), ())), preferred_element_type=jnp.float32
    )


def normalized(values):
    row_mean = jnp.mean(values, axis=-1, keepdims=True)
    centered = values - row_mean
    variance = jnp.mean(centered * centered, axis=-1, keepdims=True)
    scale = lax.rsqrt(variance + norm_eps)
    return centered * scale, scale


def forward_kernel(
    tok, cot, vec, w_project, w_combine, w_expand, pos_row, pos_col,
    n1, q_out, k_out, v_out, wp, wc, we, dy, table, attended, lse, middle, two, cols,
    tok_all, vec_all, att_low, att_rows, two_mine,
    g_sems, pair_send, pair_recv, we_send, we_recv, att_send, att_recv, col_send, col_recv, loc,
):
    p = Place()
    rows, width = tok.shape
    total = n1.shape[0]
    shard = w_combine.shape[0]
    hc = q_out.shape[1]
    low = jnp.bfloat16
    own_wp = [
        pltpu.make_async_copy(
            w_project.at[:, pl.ds(pl.multiple_of(part * width + p.c * hc, hc), hc)],
            wp.at[p.s, :, pl.ds(part * hc, hc)],
            loc.at[part],
        )
        for part in range(3)
    ]
    own = [
        pltpu.make_async_copy(tok, tok_all.at[p.c], loc.at[3]),
        pltpu.make_async_copy(vec, vec_all.at[p.s], loc.at[4]),
        pltpu.make_async_copy(w_combine, wc.at[p.s], loc.at[5]),
        pltpu.make_async_copy(cot, dy.at[p.s], loc.at[6]),
        pltpu.make_async_copy(
            w_expand.at[:, pl.ds(pl.multiple_of(p.s * width, width), width)],
            we.at[p.s],
            loc.at[7],
        ),
    ]
    for copy in own_wp + own:
        copy.start()
    greet_devices(ctx_peers(p) + wsh_peers(p))
    gather = LineGather(p, tok, tok_all, (g_sems.at[0], g_sems.at[1]))
    gather.start()

    def pair(index, src, dst):
        return PairGather(p, src, dst, (pair_send.at[index], pair_recv.at[index]))

    vec_pair = pair(0, vec, vec_all)
    vec_pair.start()
    for copy in own_wp:
        copy.wait()
    wp_pair = pair(1, wp.at[p.s], wp)
    wp_pair.start()
    wc_pair = pair(2, w_combine, wc)
    wc_pair.start()
    dy_pair = pair(3, cot, dy)
    dy_pair.start()
    we_copies = []
    for index, (to_y, to_k) in enumerate(((1, 1), (1, 0), (0, 1))):
        to = p.wsh_of(to_y, to_k)
        copy = remote(
            w_expand.at[:, pl.ds(pl.multiple_of(to * width, width), width)],
            we.at[p.s],
            (we_send, we_recv),
            index,
            (p.c, to),
        )
        copy.start()
        we_copies.append(copy)

    vec_pair.relay()
    own[1].wait()
    vec_pair.arrived()
    for source in range(4):
        table[:, source * shard : (source + 1) * shard] = vec_all[source].astype(jnp.float32)
    gain, bias = table[0:1, :], table[1:2, :]

    def norm_block(slot):
        scaled, _ = normalized(tok_all[slot].astype(jnp.float32))
        n1[pl.ds(pl.multiple_of(slot * rows, rows), rows), :] = (scaled * gain + bias).astype(low)

    own[0].wait()
    gather.advance(1)
    wp_pair.relay()
    gather.advance(2)
    wc_pair.relay()
    gather.advance(3)
    step_z = 1 - 2 * (p.z // 2)

    def own_line(index, carry):
        norm_block((p.z + index * step_z + 4) % 4 * 2 + p.x)
        return carry

    lax.fori_loop(0, 4, own_line, 0)

    def other_line(index, carry):
        source_z = (p.z + index * step_z + 4) % 4
        gather.across(source_z)
        norm_block(source_z * 2 + 1 - p.x)
        return carry

    lax.fori_loop(0, 4, other_line, 0)
    wp_pair.arrived()
    head_cols = pl.ds(pl.multiple_of(p.c * hc, hc), hc)
    bias_q, bias_v = table[2:3, head_cols], table[3:4, head_cols]

    def project(index, carry):
        part = pl.ds(pl.multiple_of(index * 256, 256), 256)
        out = nn(n1[part, :], wp[...].reshape(width, 3 * hc))
        q_out[part, :] = (out[:, :hc] + bias_q).astype(low)
        k_out[part, :] = out[:, hc : 2 * hc].astype(low)
        v_out[part, :] = (out[:, 2 * hc :] + bias_v).astype(low)
        return carry

    lax.fori_loop(0, total // 256, project, 0)
    dy_pair.relay()
    wc_pair.arrived()
    dy_pair.arrived()

    scale = (width // HEADS) ** (-0.5)

    def att_send_to(dest):
        return pltpu.make_async_remote_copy(
            src_ref=att_low.at[dest],
            dst_ref=att_rows.at[:, head_cols],
            send_sem=att_send.at[dest],
            recv_sem=att_recv.at[p.c],
            device_id=(dest, p.s),
            device_id_type=MESH_ID,
        )

    def att_own():
        return pltpu.make_async_copy(att_low.at[p.c], att_rows.at[:, head_cols], loc.at[8])

    def attend(index, carry):
        part = pl.ds(pl.multiple_of(index * 256, 256), 256)
        queries = q_out[part, :]
        seen = pos_row[0:1, :] <= pos_col[part, :]
        first = lax.broadcasted_iota(jnp.int32, (256, hc), 1) < hc // 2
        outs, logs = [], []
        for head in range(2):
            mine = first if head == 0 else jnp.logical_not(first)
            scores = nt(jnp.where(mine, queries, jnp.zeros_like(queries)), k_out[...]) * scale
            scores = jnp.where(seen, scores, masked_score)
            peak = jnp.max(scores, axis=1, keepdims=True)
            grown = jnp.exp(scores - peak)
            whole = jnp.sum(grown, axis=1, keepdims=True)
            probs = (grown * (1.0 / whole)).astype(low)
            outs.append(nn(probs, v_out[...]))
            logs.append(peak + jnp.log(whole))
        mixed = jnp.where(first, outs[0], outs[1])
        attended[part, :] = mixed
        lse[part, :] = jnp.where(first, logs[0], logs[1])
        mixed_low = mixed.astype(low)
        for half in range(2):
            dest = index * 2 + half
            att_low[dest] = mixed_low[half * 128 : (half + 1) * 128]

            @pl.when(dest != p.c)
            def _(dest=dest):
                att_send_to(dest).start()

            @pl.when(dest == p.c)
            def _():
                att_own().start()

        return carry

    lax.fori_loop(0, total // 256, attend, 0)
    att_own().wait()
    for step in range(1, 8):
        source = (p.c + step) % 8
        landed = att_rows.at[:, pl.ds(pl.multiple_of(source * hc, hc), hc)]
        pltpu.make_async_remote_copy(
            src_ref=landed,
            dst_ref=landed,
            send_sem=att_send.at[source],
            recv_sem=att_recv.at[source],
            device_id=(source, p.s),
            device_id_type=MESH_ID,
        ).wait_recv()
    own[2].wait()
    mid = tok[...].astype(jnp.float32) + nn(att_rows[...], wc[...].reshape(width, width)) + table[4:5, :]
    middle[...] = mid
    scaled, _ = normalized(mid)
    two_mine[...] = (scaled * table[5:6, :] + table[6:7, :]).astype(low)
    two[p.s] = two_mine[...]
    two_pair = pair(4, two_mine, two)
    two_pair.start()
    col_copies = []
    for index, (to_y, to_k) in enumerate(((1, 1), (1, 0), (0, 1))):
        to = p.wsh_of(to_y, to_k)
        copy = remote(
            att_rows.at[:, pl.ds(pl.multiple_of(to * shard, shard), shard)],
            cols.at[p.s],
            (col_send, col_recv),
            index,
            (p.c, to),
        )
        copy.start()
        col_copies.append(copy)
    own_cols = pltpu.make_async_copy(
        att_rows.at[:, pl.ds(pl.multiple_of(p.s * shard, shard), shard)], cols.at[p.s], loc.at[9]
    )
    own_cols.start()
    two_pair.relay()
    two_pair.arrived()
    for index, (to_y, to_k) in enumerate(((1, 1), (1, 0), (0, 1))):
        source = p.wsh_of(to_y, to_k)
        remote(cols.at[source], cols.at[source], (col_send, col_recv), index, (p.c, source)).wait_recv()
        remote(we.at[source], we.at[source], (we_send, we_recv), index, (p.c, source)).wait_recv()
    own_cols.wait()
    own[3].wait()
    own[4].wait()
    for copy in we_copies + col_copies:
        copy.wait_send()
    gather.finish()
    for member in (vec_pair, wp_pair, wc_pair, dy_pair, two_pair):
        member.finish()
    for step in range(1, 8):
        att_send_to((p.c + step) % 8).wait_send()


def shape(dims, kind):
    return jax.ShapeDtypeStruct(dims, kind)


def forward_fused(tok, cot, vec, w_project, w_combine, w_expand, pos_row, pos_col):
    low, wide = jnp.bfloat16, jnp.float32
    rows, width = tok.shape
    total = rows * 8
    hc = width // 8
    shard = w_combine.shape[0]
    vmem, hbm = pl.BlockSpec(memory_space=pltpu.VMEM), pl.BlockSpec(memory_space=pl.ANY)
    dma = pltpu.SemaphoreType.DMA
    return pl.pallas_call(
        forward_kernel,
        out_shape=[
            shape((total, width), low),
            shape((total, hc), low),
            shape((total, hc), low),
            shape((total, hc), low),
            shape((4, shard, 3 * hc), low),
            shape((4, shard, width), low),
            shape((4, shard, width), low),
            shape((4, rows, width), low),
            shape((16, width), wide),
            shape((total, hc), wide),
            shape((total, hc), wide),
            shape((rows, width), wide),
            shape((4, rows, width), low),
            shape((4, rows, shard), low),
        ],
        in_specs=[vmem, vmem, vmem, hbm, vmem, hbm, vmem, vmem],
        out_specs=[vmem] * 6 + [hbm, hbm] + [vmem] * 6,
        scratch_shapes=[
            pltpu.VMEM((8, rows, width), low),
            pltpu.VMEM((4, 16, shard), low),
            pltpu.VMEM((8, rows, hc), low),
            pltpu.VMEM((rows, width), low),
            pltpu.VMEM((rows, width), low),
            dma((2, 12)),
            dma((5, 3)),
            dma((5, 3)),
            dma((3,)),
            dma((3,)),
            dma((8,)),
            dma((8,)),
            dma((3,)),
            dma((3,)),
            dma((10,)),
        ],
        compiler_params=pltpu.CompilerParams(
            collective_id=10, has_side_effects=True, vmem_limit_bytes=56 * 2**20
        ),
        name="forward",
    )(tok, cot, vec, w_project, w_combine, w_expand, pos_row, pos_col)


class LineReduce:
    count = 12

    def __init__(self, place, mine, from_x, from_low, from_high, out, acc, sems):
        self.p, self.mine, self.sems = place, mine, sems
        self.from_x, self.from_low, self.from_high = from_x, from_low, from_high
        self.out, self.acc = out, acc

    def order(self, index):
        near = self.p.z // 2
        z = self.p.z * (1 - near) + (3 - self.p.z) * near
        inner = (1 - index % 2) * (3 - index // 2) + (index % 2) * (index // 2)
        dest = (1 - z) * (3 - index) + z * inner
        return dest * (1 - near) + (3 - dest) * near

    def x_copy(self, dest):
        p = self.p
        return remote(
            self.mine.at[dest * 2 + 1 - p.x],
            self.from_x.at[dest],
            self.sems,
            dest,
            (p.ctx_of(0, 1), p.s),
        )

    def up_copy(self, dest):
        p = self.p
        to = ((p.z + 1) * 2 + p.x, p.s)
        return remote(self.out.at[dest], self.from_low.at[dest], self.sems, 4 + dest, to)

    def down_copy(self, dest):
        p = self.p
        to = ((p.z - 1) * 2 + p.x, p.s)
        return remote(self.out.at[dest], self.from_high.at[dest], self.sems, 8 + dest, to)

    def start(self):
        def body(index, carry):
            self.x_copy(self.order(index)).start()
            return carry

        lax.fori_loop(0, 4, body, 0)

    def add(self, dest, target, source, keep):
        rows = self.acc.shape[0]

        def body(index, carry):
            part = pl.ds(pl.multiple_of(index * 32, 32), 32)
            if keep:
                self.acc[part, :] = self.acc[part, :] + source[dest, part, :].astype(jnp.float32)
            else:
                slot = dest * 2 + self.p.x
                self.acc[part, :] = self.mine[slot, part, :].astype(jnp.float32) + source[
                    dest, part, :
                ].astype(jnp.float32)
            return carry

        lax.fori_loop(0, rows // 32, body, 0)

    def combine(self):
        p = self.p

        def body(index, carry):
            dest = self.order(index)
            self.x_copy(dest).wait_recv()
            self.add(dest, None, self.from_x, False)

            @pl.when((dest >= p.z) & (p.z > 0))
            def _():
                self.up_copy(dest).wait_recv()
                self.add(dest, None, self.from_low, True)

            @pl.when((dest <= p.z) & (p.z < 3))
            def _():
                self.down_copy(dest).wait_recv()
                self.add(dest, None, self.from_high, True)

            @pl.when(dest != p.z)
            def _():
                rows = self.acc.shape[0]

                def down(step, inner):
                    part = pl.ds(pl.multiple_of(step * 32, 32), 32)
                    self.out[dest, part, :] = self.acc[part, :].astype(self.out.dtype)
                    return inner

                lax.fori_loop(0, rows // 32, down, 0)

            @pl.when(dest > p.z)
            def _():
                self.up_copy(dest).start()

            @pl.when(dest < p.z)
            def _():
                self.down_copy(dest).start()

            return carry

        lax.fori_loop(0, 4, body, 0)

    def finish(self):
        p = self.p
        for dest in range(4):
            self.x_copy(dest).wait_send()

            @pl.when(dest > p.z)
            def _(dest=dest):
                self.up_copy(dest).wait_send()

            @pl.when(dest < p.z)
            def _(dest=dest):
                self.down_copy(dest).wait_send()


class QuadSwap:
    def __init__(self, place, src_of, dst, sems):
        self.p, self.src_of, self.dst, self.sems = place, src_of, dst, sems
        self.sent = []

    def start(self):
        p = self.p
        for index, (to_y, to_k) in enumerate(((1, 1), (1, 0), (0, 1))):
            to = p.wsh_of(to_y, to_k)
            copy = remote(self.src_of(to), self.dst.at[p.s], self.sems, index, (p.c, to))
            copy.start()
            self.sent.append(copy)

    def arrived(self):
        p = self.p
        for index, (to_y, to_k) in enumerate(((1, 1), (1, 0), (0, 1))):
            source = p.wsh_of(to_y, to_k)
            block = self.dst.at[source]
            remote(block, block, self.sems, index, (p.c, source)).wait_recv()

    def finish(self):
        for copy in self.sent:
            copy.wait_send()


def backward_kernel(
    att_grad, branch, att_cols, ff, n1, q, k, v, wp, attended, lse, pos_row, pos_col,
    tok, mid_grad, table, vec_in,
    in_grad, reduce_all, combine_all, expand_all, project_all, vec_sum, square_out,
    datt, branch_all, dqkv, dk, dv, gp_mine, gp_terms,
    f_x, f_low, f_high, f_out, f_acc, t_mine, t_x, t_low, t_high, t_out, t_acc,
    reduce_own, combine_own, expand_terms, expand_own, project_own,
    vec_mine, vec_terms, vec_own, vec_all, sq_own, sq_all, sq_line, sq_group,
    a_send, a_recv, pair_send, pair_recv, r_sems, quad_send, quad_recv, g_sems, loc,
):
    p = Place()
    low, wide = jnp.bfloat16, jnp.float32
    rows, width = tok.shape
    total, hc = q.shape
    shard = width // 4
    cut = shard // 8
    scale = (width // HEADS) ** (-0.5)
    greet_devices(ctx_peers(p) + wsh_peers(p))

    def a_copy(dest):
        return pltpu.make_async_remote_copy(
            src_ref=att_grad.at[:, pl.ds(pl.multiple_of(dest * hc, hc), hc)],
            dst_ref=datt.at[p.c],
            send_sem=a_send.at[dest],
            recv_sem=a_recv.at[p.c],
            device_id=(dest, p.s),
            device_id_type=MESH_ID,
        )

    for dz, dx in CtxSwap.steps:
        a_copy(p.ctx_of(dz, dx)).start()
    own_att = pltpu.make_async_copy(
        att_grad.at[:, pl.ds(pl.multiple_of(p.c * hc, hc), hc)], datt.at[p.c], loc.at[0]
    )
    own_att.start()
    own_branch = pltpu.make_async_copy(branch, branch_all.at[p.s], loc.at[1])
    own_branch.start()
    branch_pair = PairGather(p, branch, branch_all, (pair_send.at[0], pair_recv.at[0]))
    branch_pair.start()
    ff_line = LineReduce(p, ff, f_x, f_low, f_high, f_out, f_acc, (r_sems.at[0], r_sems.at[1]))
    ff_line.start()
    dk[...] = jnp.zeros_like(dk)
    dv[...] = jnp.zeros_like(dv)
    own_att.wait()
    for step in range(1, 8):
        source = (p.c + step) % 8
        pltpu.make_async_remote_copy(
            src_ref=datt.at[source],
            dst_ref=datt.at[source],
            send_sem=a_send.at[source],
            recv_sem=a_recv.at[source],
            device_id=(source, p.s),
            device_id_type=MESH_ID,
        ).wait_recv()

    def attend(index, carry):
        part = pl.ds(pl.multiple_of(index * 256, 256), 256)
        queries = q[part, :]
        grads = jnp.concatenate([datt[index * 2], datt[index * 2 + 1]], axis=0)
        seen = pos_row[0:1, :] <= pos_col[part, :]
        first = lax.broadcasted_iota(jnp.int32, (256, hc), 1) < hc // 2
        both = grads.astype(wide) * attended[part, :]
        outs = []
        for head in range(2):
            mine = first if head == 0 else jnp.logical_not(first)
            q_head = jnp.where(mine, queries, jnp.zeros_like(queries))
            g_head = jnp.where(mine, grads, jnp.zeros_like(grads))
            logs = lse[part, head * (hc // 2) : head * (hc // 2) + 1]
            scores = jnp.where(seen, nt(q_head, k[...]) * scale, masked_score)
            soft = jnp.exp(scores - logs)
            delta = jnp.sum(jnp.where(mine, both, 0.0), axis=1, keepdims=True)
            score_grad = (soft * (nt(g_head, v[...]) - delta)).astype(low)
            outs.append(nn(score_grad, k[...]))
            dk[...] += tn(score_grad, q_head)
            dv[...] += tn(soft.astype(low), g_head)
        dqkv[part, 0:hc] = (jnp.where(first, outs[0], outs[1]) * scale).astype(low)
        return carry

    lax.fori_loop(0, total // 256, attend, 0)
    dqkv[:, hc : 2 * hc] = (dk[...] * scale).astype(low)
    dqkv[:, 2 * hc :] = dv[...].astype(low)

    def one_terms(index, carry):
        part = pl.ds(pl.multiple_of(index * 256, 256), 256)
        out = nt(dqkv[part, :], wp[...].reshape(width, 3 * hc)).astype(low)
        t_mine[index * 2, 0:rows, :] = out[:rows]
        t_mine[index * 2 + 1, 0:rows, :] = out[rows:]
        return carry

    lax.fori_loop(0, total // 256, one_terms, 0)
    own_branch.wait()
    branch_pair.relay()
    branch_pair.arrived()
    grad_combine = tn(
        att_cols[...].reshape(4 * rows, shard), branch_all[...].reshape(4 * rows, width)
    ).astype(low)
    for dest in range(8):
        t_mine[dest, rows : rows + cut, :] = grad_combine[dest * cut : (dest + 1) * cut]
    tail = LineReduce(p, t_mine, t_x, t_low, t_high, t_out, t_acc, (r_sems.at[2], r_sems.at[3]))
    tail.start()
    for dest in range(4):
        gp_mine[dest] = tn(n1[:, dest * shard : (dest + 1) * shard], dqkv[...]).astype(low)
    gp_swap = QuadSwap(p, lambda to: gp_mine.at[to], gp_terms, (quad_send.at[0], quad_recv.at[0]))
    gp_swap.start()
    own_gp = pltpu.make_async_copy(gp_mine.at[p.s], gp_terms.at[p.s], loc.at[2])
    own_gp.start()

    ff_line.combine()
    reduce_own[...] = f_acc[0:rows, :].astype(low)
    for part in range(4):
        f_out[p.z, part * cut : (part + 1) * cut, :] = f_acc[
            rows + part * cut : rows + (part + 1) * cut, :
        ].astype(low)
    expand_swap = QuadSwap(
        p,
        lambda to: f_out.at[p.z, pl.ds(pl.multiple_of(to * cut, cut), cut)],
        expand_terms,
        (quad_send.at[1], quad_recv.at[1]),
    )
    expand_swap.start()
    own_expand = pltpu.make_async_copy(
        f_out.at[p.z, pl.ds(pl.multiple_of(p.s * cut, cut), cut)], expand_terms.at[p.s], loc.at[3]
    )
    own_expand.start()
    gathers = []

    def gather(index, src, dst):
        line = LineGather(p, src, dst, (g_sems.at[2 * index], g_sems.at[2 * index + 1]))
        line.start()
        own = pltpu.make_async_copy(src, dst.at[p.c], loc.at[4 + index])
        own.start()
        gathers.append((line, own))

    gather(0, reduce_own, reduce_all)
    square = jnp.sum(jnp.square(reduce_own[...].astype(wide)))
    expand_swap.arrived()
    own_expand.wait()
    for part in range(4):
        expand_own[:, part * width : (part + 1) * width] = expand_terms[part]
    gather(1, expand_own, expand_all)
    square += jnp.sum(jnp.square(expand_own[...].astype(wide)))
    gp_swap.arrived()
    own_gp.wait()
    project_own[...] = jnp.sum(gp_terms[...].astype(wide), axis=0).astype(low)
    square += jnp.sum(jnp.square(project_own[...].astype(wide)))
    gather(2, project_own, project_all)

    tail.combine()
    combine_own[...] = t_acc[rows : rows + cut, :].astype(low)
    square += jnp.sum(jnp.square(combine_own[...].astype(wide)))
    gather(3, combine_own, combine_all)
    grad = t_acc[0:rows, :]
    hat, spread = normalized(tok[...].astype(wide))
    hat_grad = grad * table[0:1, :]
    back = spread * (
        hat_grad
        - jnp.mean(hat_grad, axis=1, keepdims=True)
        - hat * jnp.mean(hat_grad * hat, axis=1, keepdims=True)
    )
    in_grad[...] = (mid_grad[...] + back).astype(low)
    vec_mine[...] = vec_in[...]
    vec_mine[0:1, :] = jnp.sum(grad * hat, axis=0, keepdims=True)
    vec_mine[1:2, :] = jnp.sum(grad, axis=0, keepdims=True)
    heads = pl.ds(pl.multiple_of(p.c * hc, hc), hc)
    vec_mine[2:3, heads] = jnp.sum(dqkv[:, 0:hc].astype(wide), axis=0, keepdims=True)
    vec_mine[3:4, heads] = jnp.sum(dqkv[:, 2 * hc :].astype(wide), axis=0, keepdims=True)
    vec_swap = QuadSwap(
        p,
        lambda to: vec_mine.at[:, pl.ds(pl.multiple_of(to * shard, shard), shard)],
        vec_terms,
        (quad_send.at[2], quad_recv.at[2]),
    )
    vec_swap.start()
    vec_terms[p.s] = vec_mine[:, pl.ds(pl.multiple_of(p.s * shard, shard), shard)]
    sq_own[...] = jnp.full(sq_own.shape, square, wide)
    vec_swap.arrived()
    vec_own[...] = jnp.sum(vec_terms[...], axis=0)
    gather(4, vec_own, vec_all)
    gather(5, sq_own, sq_all)
    for step in (1, 2, 3):
        for line, _ in gathers:
            line.advance(step)
    for source_z in range(4):
        for line, _ in gathers:
            line.across(source_z)
    for _, own in gathers:
        own.wait()
    vectors = jnp.sum(vec_all[...], axis=0)
    vec_sum[...] = vectors
    sq_line[...] = jnp.sum(sq_all[...], axis=0) + jnp.sum(jnp.square(vectors))
    sq_pair = PairGather(p, sq_line, sq_group, (pair_send.at[1], pair_recv.at[1]))
    sq_pair.start()
    sq_group[p.s] = sq_line[...]
    sq_pair.relay()
    sq_pair.arrived()
    square_out[...] = jnp.sum(sq_group[...], axis=0)
    for line, _ in gathers:
        line.finish()
    ff_line.finish()
    tail.finish()
    for member in (branch_pair, sq_pair, gp_swap, expand_swap, vec_swap):
        member.finish()
    for step in range(1, 8):
        a_copy((p.c + step) % 8).wait_send()


def backward_fused(*operands):
    low, wide = jnp.bfloat16, jnp.float32
    rows, width = operands[0].shape
    hc = width // 8
    total = rows * 8
    shard = width // 4
    cut = shard // 8
    vmem, hbm = pl.BlockSpec(memory_space=pltpu.VMEM), pl.BlockSpec(memory_space=pl.ANY)
    dma = pltpu.SemaphoreType.DMA
    mem = pltpu.VMEM
    ff_rows = operands[3].shape[1]
    tail_rows = rows + cut
    return pl.pallas_call(
        backward_kernel,
        out_shape=[
            shape((rows, width), low),
            shape((8, rows, width), low),
            shape((8, cut, width), low),
            shape((8, cut, 4 * width), low),
            shape((8, shard, 3 * hc), low),
            shape((16, shard), wide),
            shape((8, 128), wide),
        ],
        in_specs=[vmem] * len(operands),
        out_specs=[vmem, hbm, hbm, hbm, hbm, vmem, vmem],
        scratch_shapes=[
            mem((8, rows, hc), low),
            mem((4, rows, width), low),
            mem((total, 3 * hc), low),
            mem((total, hc), wide),
            mem((total, hc), wide),
            mem((4, shard, 3 * hc), low),
            mem((4, shard, 3 * hc), low),
            mem((4, ff_rows, width), low),
            mem((4, ff_rows, width), low),
            mem((4, ff_rows, width), low),
            mem((4, ff_rows, width), low),
            mem((ff_rows, width), wide),
            mem((8, tail_rows, width), low),
            mem((4, tail_rows, width), low),
            mem((4, tail_rows, width), low),
            mem((4, tail_rows, width), low),
            mem((4, tail_rows, width), low),
            mem((tail_rows, width), wide),
            mem((rows, width), low),
            mem((cut, width), low),
            mem((4, cut, width), low),
            mem((cut, 4 * width), low),
            mem((shard, 3 * hc), low),
            mem((16, width), wide),
            mem((4, 16, shard), wide),
            mem((16, shard), wide),
            mem((8, 16, shard), wide),
            mem((8, 128), wide),
            mem((8, 8, 128), wide),
            mem((8, 128), wide),
            mem((4, 8, 128), wide),
            dma((8,)),
            dma((8,)),
            dma((2, 3)),
            dma((2, 3)),
            dma((4, 12)),
            dma((3, 3)),
            dma((3, 3)),
            dma((12, 12)),
            dma((10,)),
        ],
        compiler_params=pltpu.CompilerParams(
            collective_id=11, has_side_effects=True, vmem_limit_bytes=60 * 2**20
        ),
        name="backward",
    )(*operands)


def optimizer_kernel(clip, *refs):
    factor = clip[0, 0]
    first_bias = 1.0 - beta_one**STEP
    second_bias = 1.0 - beta_two**STEP
    for index in range(4):
        weight, grad, first, second = refs[4 * index : 4 * index + 4]
        g_out, m_out, v_out, u_out = refs[16 + 4 * index : 20 + 4 * index]
        if len(grad.shape) == 3:
            pieces = [
                grad[source, :, part * 128 : (part + 1) * 128]
                for part in range(3)
                for source in range(grad.shape[0])
            ]
            total = jnp.concatenate(pieces, axis=1).astype(jnp.float32)
        else:
            total = grad[...].astype(jnp.float32)
        g_out[...] = total
        clipped = total * factor
        moment = beta_one * first[...] + (1.0 - beta_one) * clipped
        square = beta_two * second[...] + (1.0 - beta_two) * clipped * clipped
        m_out[...] = moment
        v_out[...] = square
        moment_hat = moment * (1.0 / first_bias)
        square_hat = square * (1.0 / second_bias)
        u_out[...] = -learn_rate * (
            moment_hat / (jnp.sqrt(square_hat) + adam_eps)
            + decay_rate * weight[...].astype(jnp.float32)
        )


def optimizer_fused(clip_factor, members):
    steps = members[1][0].shape[0] // 16
    operands, in_specs, out_specs, out_shape = [], [], [], []
    for weight, grad, first, second in members:
        rows, width = weight.shape
        block = rows // steps
        flat = pl.BlockSpec((block, width), lambda i: (i, 0))
        operands += [weight, grad, first, second]
        if grad.ndim == 3:
            grad_spec = pl.BlockSpec((8, block, grad.shape[2]), lambda i: (0, i, 0))
        else:
            grad_spec = flat
        in_specs += [flat, grad_spec, flat, flat]
        out_specs += [flat] * 4
        out_shape += [shape((rows, width), jnp.float32)] * 4
    return pl.pallas_call(
        optimizer_kernel,
        grid=(steps,),
        out_shape=out_shape,
        in_specs=[pl.BlockSpec(memory_space=pltpu.SMEM)] + in_specs,
        out_specs=out_specs,
        compiler_params=pltpu.CompilerParams(vmem_limit_bytes=56 * 2**20),
        name="optimizer",
    )(clip_factor.reshape(1, 1), *operands)


def adam_step(weight, gradient, first_moment, second_moment, clip_factor, step_value):
    clipped = gradient * clip_factor
    moment = beta_one * first_moment + (1.0 - beta_one) * clipped
    square = beta_two * second_moment + (1.0 - beta_two) * clipped * clipped
    moment_hat = moment / (1.0 - jnp.power(jnp.float32(beta_one), step_value))
    square_hat = square / (1.0 - jnp.power(jnp.float32(beta_two), step_value))
    update = -learn_rate * (
        moment_hat / (jnp.sqrt(square_hat) + adam_eps) + decay_rate * weight.astype(jnp.float32)
    )
    return (moment, square, update)


def body_plain(
    tokens,
    output_cotangent,
    block_table,
    weight_project,
    weight_combine,
    weight_expand,
    weight_reduce,
    vectors,
    moment_project,
    square_project,
    moment_combine,
    square_combine,
    moment_expand,
    square_expand,
    moment_reduce,
    square_reduce,
    moment_vectors,
    square_vectors,
):
    low = jnp.bfloat16
    ctx_count, wsh_count = lax.axis_size("ctx"), lax.axis_size("wsh")
    ctx_index, wsh_index = lax.axis_index("ctx"), lax.axis_index("wsh")
    rows_dev, width = tokens.shape[1], tokens.shape[2]
    block_rows = rows_dev // 2
    total_rows = rows_dev * ctx_count
    group_rows = rows_dev * wsh_count
    head_size = width // HEADS
    score_scale = head_size ** (-0.5)
    head_cols = width // ctx_count
    local_heads = head_cols // head_size
    shard_rows = weight_project.shape[0]
    ff_width = weight_expand.shape[1]
    chunk = ff_width // wsh_count
    vec_rows = vectors.shape[0]
    swap = plain

    sequence = tokens[0].astype(jnp.float32)
    cotangent_low = output_cotangent[0]
    cotangent = cotangent_low.astype(jnp.float32)

    project_cols = lax.dynamic_slice_in_dim(
        weight_project.reshape(shard_rows, 3, ctx_count, head_cols), ctx_index, 1, axis=2
    ).reshape(shard_rows, 3 * head_cols)

    vec_pad = -vec_rows % 16
    (vec_parts,) = swap("vec", 0, (WshGather, jnp.pad(vectors, ((0, vec_pad), (0, 0)))))
    vec_table = (
        vec_parts[:, :vec_rows].transpose(1, 0, 2).reshape(vec_rows, width).astype(jnp.float32)
    )
    normed_one = layer_norm(sequence, vec_table[0], vec_table[1]).astype(low)
    normed_all, project_parts, cot_parts, combine_parts, expand_parts = swap(
        "front",
        1,
        (CtxGather, normed_one),
        (WshGather, project_cols),
        (WshGather, cotangent_low),
        (WshGather, weight_combine),
        (WshSwap, weight_expand.reshape(shard_rows, wsh_count, chunk).transpose(1, 0, 2)),
    )
    normed_all = normed_all.reshape(total_rows, width)
    project_mine = project_parts.reshape(width, 3 * head_cols)
    full_combine = combine_parts.reshape(width, width)
    expand_mine = expand_parts.reshape(width, chunk)
    cot_group = cot_parts.reshape(group_rows, width)

    qkv = matmul(normed_all, project_mine)
    bias_cols = lax.dynamic_slice_in_dim(
        vec_table[:4].reshape(4, ctx_count, head_cols), ctx_index, 1, axis=1
    ).reshape(4, head_cols)
    queries = (qkv[:, :head_cols] + bias_cols[2]).astype(low)
    keys = qkv[:, head_cols : 2 * head_cols].astype(low)
    values = (qkv[:, 2 * head_cols :] + bias_cols[3]).astype(low)
    positions = (
        block_table[:, None] * block_rows + jnp.arange(block_rows, dtype=jnp.int32)[None, :]
    ).reshape(total_rows)
    visible = positions[None, None, :] <= positions[None, :, None]
    heads = (total_rows, local_heads, head_size)
    query_heads, key_heads, value_heads = (
        queries.reshape(heads),
        keys.reshape(heads),
        values.reshape(heads),
    )
    scores = (
        jnp.einsum("qhd,khd->hqk", query_heads, key_heads, preferred_element_type=jnp.float32)
        * score_scale
    )
    scores = jnp.where(visible, scores, masked_score)
    peak = jnp.max(scores, axis=2, keepdims=True)
    grown = jnp.exp(scores - peak)
    soft = grown / jnp.sum(grown, axis=2, keepdims=True)
    soft_low = soft.astype(low)
    attended_heads = jnp.einsum(
        "hqk,khd->qhd", soft_low, value_heads, preferred_element_type=jnp.float32
    )
    attended = attended_heads.reshape(total_rows, head_cols)
    (att_parts,) = swap(
        "attended", 2, (CtxSwap, attended.astype(low).reshape(ctx_count, rows_dev, head_cols))
    )
    attended_rows = att_parts.transpose(1, 0, 2).reshape(rows_dev, width)

    middle = sequence + matmul(attended_rows, full_combine) + vec_table[4]
    normed_two = layer_norm(middle, vec_table[5], vec_table[6]).astype(low)
    two_parts, att_cols = swap(
        "normed_two",
        3,
        (WshGather, normed_two),
        (WshSwap, attended_rows.reshape(rows_dev, wsh_count, shard_rows).transpose(1, 0, 2)),
    )
    two_group = two_parts.reshape(group_rows, width)

    bias_ff = lax.dynamic_slice_in_dim(vec_table[8:].reshape(-1), wsh_index * chunk, chunk)
    hidden_pre = matmul(two_group, expand_mine) + bias_ff
    hidden, gelu_back = jax.vjp(gelu_exact, hidden_pre)
    hidden = hidden.astype(low)
    out_partial = matmul(hidden, weight_reduce)
    pre_grad = gelu_back(matmul_right_t(cot_group, weight_reduce))[0].astype(low)
    two_partial = matmul_right_t(pre_grad, expand_mine)
    part_shape = (wsh_count, rows_dev, width)
    two_terms, out_terms = swap(
        "ff_sums",
        4,
        (WshSwap, two_partial.astype(low).reshape(part_shape)),
        (WshSwap, out_partial.astype(low).reshape(part_shape)),
    )
    layer_output = middle + jnp.sum(out_terms.astype(jnp.float32), axis=0) + vec_table[7]
    normed_two_grad = jnp.sum(two_terms.astype(jnp.float32), axis=0)
    norm_two_back = jax.vjp(layer_norm, middle, vec_table[5], vec_table[6])[1](normed_two_grad)
    middle_grad = cotangent + norm_two_back[0]
    branch_grad = middle_grad.astype(low)
    attended_grad_rows = matmul_right_t(branch_grad, full_combine).astype(low)
    att_grad_parts, branch_parts = swap(
        "attended_grad",
        5,
        (CtxSwap, attended_grad_rows.reshape(rows_dev, ctx_count, head_cols).transpose(1, 0, 2)),
        (WshGather, branch_grad),
    )
    branch_group = branch_parts.reshape(group_rows, width)
    attended_grad = att_grad_parts.reshape(total_rows, head_cols)

    grad_reduce = matmul_left_t(hidden, cot_group)
    grad_expand = matmul_left_t(two_group, pre_grad)
    grad_combine = matmul_left_t(att_cols.reshape(group_rows, shard_rows), branch_group)

    grad_heads = attended_grad.reshape(heads)
    delta = jnp.sum(
        grad_heads.astype(jnp.float32) * attended_heads, axis=2
    ).transpose(1, 0)[:, :, None]
    soft_grad = jnp.einsum(
        "qhd,khd->hqk", grad_heads, value_heads, preferred_element_type=jnp.float32
    )
    score_grad = (soft * (soft_grad - delta)).astype(low)
    query_grad = (
        jnp.einsum("hqk,khd->qhd", score_grad, key_heads, preferred_element_type=jnp.float32)
        * score_scale
    )
    key_grad = (
        jnp.einsum("hqk,qhd->khd", score_grad, query_heads, preferred_element_type=jnp.float32)
        * score_scale
    )
    value_grad = jnp.einsum(
        "hqk,qhd->khd", soft_low, grad_heads, preferred_element_type=jnp.float32
    )
    flat = (total_rows, head_cols)
    qkv_grad = jnp.concatenate(
        [member.reshape(flat).astype(low) for member in (query_grad, key_grad, value_grad)], axis=1
    )
    grad_project = matmul_left_t(normed_all, qkv_grad)
    one_partial = matmul_right_t(qkv_grad, project_mine)

    cut = shard_rows // ctx_count
    cut_reduce = chunk // ctx_count
    for_ctx = jnp.concatenate(
        [
            grad_reduce.astype(low).reshape(ctx_count, cut_reduce, width),
            grad_combine.astype(low).reshape(ctx_count, cut, width),
        ],
        axis=1,
    )
    expand_ctx = (
        grad_expand.astype(low)
        .reshape(wsh_count, ctx_count, cut, chunk)
        .transpose(1, 0, 2, 3)
        .reshape(ctx_count, wsh_count * cut, chunk)
    )
    ctx_terms, expand_terms, one_terms, project_terms = swap(
        "grad_sums",
        6,
        (CtxSwap, for_ctx),
        (CtxSwap, expand_ctx),
        (CtxSwap, one_partial.astype(low).reshape(ctx_count, rows_dev, width)),
        (WshSwap, grad_project.astype(low).reshape(wsh_count, shard_rows, 3 * head_cols)),
    )
    normed_one_grad = jnp.sum(one_terms.astype(jnp.float32), axis=0)
    norm_one_back = jax.vjp(layer_norm, sequence, vec_table[0], vec_table[1])[1](normed_one_grad)
    input_gradient = (middle_grad + norm_one_back[0]).astype(low)
    ctx_piece = jnp.sum(ctx_terms.astype(jnp.float32), axis=0).astype(low)
    expand_piece = jnp.sum(expand_terms.astype(jnp.float32), axis=0).astype(low)
    project_piece = jnp.sum(project_terms.astype(jnp.float32), axis=0).astype(low)

    def spread(columns, start):
        return lax.dynamic_update_slice(
            jnp.zeros((width,), jnp.float32), columns, (start,)
        )

    ff_terms = lax.dynamic_update_slice(
        jnp.zeros((ff_width,), jnp.float32),
        jnp.sum(pre_grad.astype(jnp.float32), axis=0),
        (wsh_index * chunk,),
    ).reshape(-1, width)
    head_start = ctx_index * head_cols
    query_sum = jnp.sum(qkv_grad[:, :head_cols].astype(jnp.float32), axis=0)
    value_sum = jnp.sum(qkv_grad[:, 2 * head_cols :].astype(jnp.float32), axis=0)
    vec_terms = jnp.concatenate(
        [
            jnp.stack(
                [
                    norm_one_back[1],
                    norm_one_back[2],
                    spread(query_sum, head_start),
                    spread(value_sum, head_start),
                    jnp.sum(branch_grad.astype(jnp.float32), axis=0),
                    norm_two_back[1],
                    norm_two_back[2],
                    jnp.sum(cotangent, axis=0),
                ]
            ),
            ff_terms,
            jnp.zeros((vec_pad, width), jnp.float32),
        ],
        axis=0,
    )
    vec_cols = vectors.shape[1]
    vec_swapped, expand_rows = swap(
        "vec_sums",
        7,
        (WshSwap, vec_terms.reshape(-1, wsh_count, vec_cols).transpose(1, 0, 2)),
        (WshSwap, expand_piece.reshape(wsh_count, cut, chunk)),
    )
    vec_mine = jnp.sum(vec_swapped, axis=0)
    expand_mine_rows = expand_rows.transpose(1, 0, 2).reshape(cut, ff_width)
    square_mine = (
        jnp.sum(jnp.square(ctx_piece.astype(jnp.float32)))
        + jnp.sum(jnp.square(expand_rows.astype(jnp.float32)))
        + jnp.sum(jnp.square(project_piece.astype(jnp.float32)))
    )
    ctx_all, expand_all, project_all, vec_all, square_ctx = swap(
        "grads",
        8,
        (CtxGather, ctx_piece),
        (CtxGather, expand_mine_rows),
        (CtxGather, project_piece),
        (CtxGather, vec_mine),
        (CtxGather, jnp.full((16, 128), square_mine, jnp.float32)),
    )
    sum_reduce = ctx_all[:, :cut_reduce].reshape(chunk, width).astype(jnp.float32)
    sum_combine = ctx_all[:, cut_reduce:].reshape(shard_rows, width).astype(jnp.float32)
    sum_expand = expand_all.reshape(shard_rows, ff_width).astype(jnp.float32)
    sum_project = (
        project_all.reshape(ctx_count, shard_rows, 3, head_cols)
        .transpose(1, 2, 0, 3)
        .reshape(shard_rows, 3 * width)
        .astype(jnp.float32)
    )
    sum_vectors = jnp.sum(vec_all, axis=0)[:vec_rows]
    square_part = jnp.sum(square_ctx[:, 0, 0]) + jnp.sum(jnp.square(sum_vectors))
    (square_all,) = swap(
        "squares", 9, (WshGather, jnp.full((8, 128), square_part, jnp.float32))
    )
    norm_value = jnp.sqrt(jnp.sum(square_all[:, 0, 0]))
    params_total = 4 * width * width + 2 * width * ff_width + vec_rows * width
    clip_max = jnp.sqrt(jnp.float32(params_total))
    clip_factor = clip_max / jnp.maximum(norm_value, clip_max)
    step_value = jnp.float32(STEP)
    results = [layer_output.astype(low)[None], input_gradient[None], norm_value.reshape(1)]
    for weight, total, first, second in (
        (weight_project, sum_project, moment_project, square_project),
        (weight_combine, sum_combine, moment_combine, square_combine),
        (weight_expand, sum_expand, moment_expand, square_expand),
        (weight_reduce, sum_reduce, moment_reduce, square_reduce),
        (vectors, sum_vectors, moment_vectors, square_vectors),
    ):
        results.append(total)
        results.extend(adam_step(weight, total, first, second, clip_factor, step_value))
    return tuple(results)


def body_fast(
    tokens,
    output_cotangent,
    block_table,
    weight_project,
    weight_combine,
    weight_expand,
    weight_reduce,
    vectors,
    moment_project,
    square_project,
    moment_combine,
    square_combine,
    moment_expand,
    square_expand,
    moment_reduce,
    square_reduce,
    moment_vectors,
    square_vectors,
):
    low, wide = jnp.bfloat16, jnp.float32
    wsh_index = lax.axis_index("wsh")
    rows_dev, width = tokens.shape[1], tokens.shape[2]
    block_rows = rows_dev // 2
    total_rows = rows_dev * 8
    group_rows = rows_dev * 4
    ff_width = weight_expand.shape[1]
    chunk = ff_width // 4
    vec_rows = vectors.shape[0]
    cot_low = output_cotangent[0]
    positions = (
        block_table[:, None] * block_rows + jnp.arange(block_rows, dtype=jnp.int32)[None, :]
    ).reshape(total_rows)
    pos_row = jnp.broadcast_to(positions[None, :], (8, total_rows))
    pos_col = positions[:, None]
    vec_padded = jnp.pad(vectors, ((0, -vec_rows % 16), (0, 0)))
    (
        n1, queries, keys, values, project_parts, combine_parts, expand_parts,
        cot_parts, table, attended, log_total, middle, two_parts, att_cols,
    ) = forward_fused(
        tokens[0], cot_low, vec_padded, weight_project, weight_combine, weight_expand,
        pos_row, pos_col,
    )
    expand_mine = expand_parts.reshape(width, chunk)
    full_combine = combine_parts.reshape(width, width)
    cot_group = cot_parts.reshape(group_rows, width)
    two_group = two_parts.reshape(group_rows, width)
    cotangent = cot_low.astype(wide)

    bias_ff = lax.dynamic_slice_in_dim(table[8:vec_rows].reshape(-1), wsh_index * chunk, chunk)
    hidden_pre = matmul(two_group, expand_mine) + bias_ff
    hidden, gelu_back = jax.vjp(gelu_exact, hidden_pre)
    hidden = hidden.astype(low)
    out_partial = matmul(hidden, weight_reduce)
    pre_grad = gelu_back(matmul_right_t(cot_group, weight_reduce))[0].astype(low)
    two_partial = matmul_right_t(pre_grad, expand_mine)
    part_shape = (4, rows_dev, width)
    two_terms, out_terms = exchange(
        "ff_sums",
        4,
        (WshSwap, two_partial.astype(low).reshape(part_shape)),
        (WshSwap, out_partial.astype(low).reshape(part_shape)),
    )
    layer_output = middle + jnp.sum(out_terms.astype(wide), axis=0) + table[7]
    two_grad = jnp.sum(two_terms.astype(wide), axis=0)
    norm_two_back = jax.vjp(layer_norm, middle, table[5], table[6])[1](two_grad)
    middle_grad = cotangent + norm_two_back[0]
    branch_grad = middle_grad.astype(low)
    att_grad = matmul_right_t(branch_grad, full_combine).astype(low)
    grad_reduce = matmul_left_t(hidden, cot_group).astype(low)
    grad_expand = matmul_left_t(two_group, pre_grad).astype(low)
    cut = width // 32
    ff_terms = jnp.concatenate(
        [
            grad_reduce.reshape(8, rows_dev, width),
            grad_expand.reshape(4, 8, cut, chunk).transpose(1, 0, 2, 3).reshape(8, 4 * cut, chunk),
        ],
        axis=1,
    )
    pre_sum = lax.dynamic_update_slice(
        jnp.zeros((ff_width,), wide), jnp.sum(pre_grad.astype(wide), axis=0), (wsh_index * chunk,)
    ).reshape(-1, width)
    none = jnp.zeros((4, width), wide)
    vec_in = jnp.concatenate(
        [
            none,
            jnp.stack(
                [
                    jnp.sum(branch_grad.astype(wide), axis=0),
                    norm_two_back[1],
                    norm_two_back[2],
                    jnp.sum(cotangent, axis=0),
                ]
            ),
            pre_sum,
            none,
        ],
        axis=0,
    )
    (
        input_gradient, reduce_all, combine_all, expand_all, project_all, vec_sum, squares,
    ) = backward_fused(
        att_grad, branch_grad, att_cols, ff_terms, n1, queries, keys, values, project_parts,
        attended, log_total, pos_row, pos_col, tokens[0], middle_grad, table, vec_in,
    )
    norm_value = jnp.sqrt(squares[0, 0])
    params_total = 4 * width * width + 2 * width * ff_width + vec_rows * width
    clip_max = jnp.sqrt(jnp.float32(params_total))
    clip_factor = clip_max / jnp.maximum(norm_value, clip_max)
    updated = optimizer_fused(
        clip_factor,
        (
            (weight_project, project_all, moment_project, square_project),
            (weight_combine, combine_all.reshape(-1, width), moment_combine, square_combine),
            (weight_expand, expand_all.reshape(-1, ff_width), moment_expand, square_expand),
            (weight_reduce, reduce_all.reshape(-1, width), moment_reduce, square_reduce),
        ),
    )
    vec_total = vec_sum[:vec_rows]
    vec_updated = adam_step(
        vectors, vec_total, moment_vectors, square_vectors, clip_factor, jnp.float32(STEP)
    )
    return (
        layer_output.astype(low)[None],
        input_gradient[None],
        norm_value.reshape(1),
        *updated,
        vec_total,
        *vec_updated,
    )


def solution(mesh):
    rows, cols = P("wsh", None), P(None, "wsh")
    token = P("wsh", "ctx", None)
    fast = (mesh.shape["ctx"], mesh.shape["wsh"]) == (FAST_CTX, FAST_WSH)
    return jax.shard_map(
        body_fast if fast else body_plain,
        mesh=mesh,
        in_specs=(token, token, P(), rows, rows, rows, rows, cols) + (rows,) * 8 + (cols,) * 2,
        out_specs=(token, token, P()) + (rows,) * 16 + (cols,) * 4,
        check_vma=False,
    )
```

```python
import math

import jax
import jax.numpy as jnp
from jax import lax
from jax.experimental import pallas as pl
from jax.experimental.pallas import tpu as pltpu
from jax.sharding import PartitionSpec as P

HEADS = 16
STEP = 4

norm_eps = 1e-05
masked_score = -1e30
beta_one = 0.9
beta_two = 0.95
learn_rate = 0.02
decay_rate = 0.1
adam_eps = 1e-08

MESH_ID = pl.DeviceIdType.MESH
FAST_CTX, FAST_WSH = 8, 4


def layer_norm(values, norm_gain, norm_bias):
    row_mean = jnp.mean(values, axis=-1, keepdims=True)
    centered = values - row_mean
    variance = jnp.mean(centered * centered, axis=-1, keepdims=True)
    return centered * lax.rsqrt(variance + norm_eps) * norm_gain + norm_bias


def gelu_exact(values):
    return jax.nn.gelu(values, approximate=False)


def matmul(left, right):
    return jnp.dot(left, right, preferred_element_type=jnp.float32)


def matmul_left_t(left, right):
    return lax.dot_general(
        left, right, (((0,), (0,)), ((), ())), preferred_element_type=jnp.float32
    )


def matmul_right_t(left, right):
    return lax.dot_general(
        left, right, (((1,), (1,)), ((), ())), preferred_element_type=jnp.float32
    )


class Place:
    def __init__(self):
        self.c = lax.axis_index("ctx")
        self.s = lax.axis_index("wsh")
        self.z, self.x = self.c // 2, self.c % 2
        self.y, self.k = self.s // 2, self.s % 2

    def ctx_of(self, dz, dx):
        return (self.z + dz + 4) % 4 * 2 + (self.x + dx) % 2

    def wsh_of(self, dy, dk):
        return (self.y + dy) % 2 * 2 + (self.k + dk) % 2


def remote(src, dst, sems, index, device):
    return pltpu.make_async_remote_copy(
        src_ref=src,
        dst_ref=dst,
        send_sem=sems[0].at[index],
        recv_sem=sems[1].at[index],
        device_id=device,
        device_id_type=MESH_ID,
    )


class CtxGather:
    pass


class CtxSwap:
    steps = ((2, 1), (2, 0), (1, 1), (-1, 1), (1, 0), (-1, 0), (0, 1))


class WshGather:
    pass


class WshSwap:
    pass


def plain(name, call_id, *pairs):
    outs = []
    for kind, array in pairs:
        if kind is CtxGather:
            outs.append(lax.all_gather(array, "ctx", axis=0))
        elif kind is WshGather:
            outs.append(lax.all_gather(array, "wsh", axis=0))
        elif kind is CtxSwap:
            outs.append(lax.all_to_all(array, "ctx", 0, 0, tiled=True))
        else:
            outs.append(lax.all_to_all(array, "wsh", 0, 0, tiled=True))
    return outs


def shape(dims, kind):
    return jax.ShapeDtypeStruct(dims, kind)


class LineGather:
    count = 12

    def __init__(self, place, src, dst, sems):
        self.p, self.src, self.dst, self.sems = place, src, dst, sems

    def x_copy(self, source_z, src, slot):
        p = self.p
        return remote(src, self.dst.at[slot], self.sems, source_z, (p.ctx_of(0, 1), p.s))

    def up_copy(self, source_z, src, slot):
        p = self.p
        to = (p.z + 1) * 2 + p.x
        return remote(src, self.dst.at[slot], self.sems, 4 + source_z, (to, p.s))

    def down_copy(self, source_z, src, slot):
        p = self.p
        to = (p.z - 1) * 2 + p.x
        return remote(src, self.dst.at[slot], self.sems, 8 + source_z, (to, p.s))

    def start(self):
        p = self.p

        @pl.when(p.z < 3)
        def _():
            self.up_copy(p.z, self.src, p.c).start()

        @pl.when(p.z > 0)
        def _():
            self.down_copy(p.z, self.src, p.c).start()

        self.x_copy(p.z, self.src, p.c).start()

    def advance(self, step):
        p = self.p
        low, high = p.z - step, p.z + step

        @pl.when(low >= 0)
        def _():
            slot = low * 2 + p.x
            self.up_copy(low, self.dst.at[slot], slot).wait_recv()

            @pl.when(p.z < 3)
            def _():
                self.up_copy(low, self.dst.at[slot], slot).start()

            self.x_copy(low, self.dst.at[slot], slot).start()

        @pl.when(high <= 3)
        def _():
            slot = high * 2 + p.x
            self.down_copy(high, self.dst.at[slot], slot).wait_recv()

            @pl.when(p.z > 0)
            def _():
                self.down_copy(high, self.dst.at[slot], slot).start()

            self.x_copy(high, self.dst.at[slot], slot).start()

    def across(self, source_z):
        slot = source_z * 2 + 1 - self.p.x
        self.x_copy(source_z, self.dst.at[slot], slot).wait_recv()

    def finish(self):
        p = self.p
        for source_z in range(4):
            slot = source_z * 2 + p.x
            self.x_copy(source_z, self.dst.at[slot], slot).wait_send()

            @pl.when((source_z <= p.z) & (p.z < 3))
            def _(source_z=source_z, slot=slot):
                self.up_copy(source_z, self.dst.at[slot], slot).wait_send()

            @pl.when((source_z >= p.z) & (p.z > 0))
            def _(source_z=source_z, slot=slot):
                self.down_copy(source_z, self.dst.at[slot], slot).wait_send()


class PairGather:
    count = 3

    def __init__(self, place, src, dst, sems):
        self.p, self.src, self.dst, self.sems = place, src, dst, sems
        self.partner = (place.c, place.wsh_of(0, 1))
        self.over = (place.c, place.wsh_of(1, 0))

    def start(self):
        p = self.p
        self.first = remote(self.src, self.dst.at[p.s], self.sems, 0, self.over)
        self.first.start()
        self.second = remote(self.src, self.dst.at[p.s], self.sems, 1, self.partner)
        self.second.start()

    def relay(self):
        block = self.dst.at[self.over[1]]
        remote(block, block, self.sems, 0, self.over).wait_recv()
        self.third = remote(block, block, self.sems, 2, self.partner)
        self.third.start()

    def arrived(self):
        block = self.dst.at[self.partner[1]]
        remote(block, block, self.sems, 1, self.partner).wait_recv()
        block = self.dst.at[self.p.wsh_of(1, 1)]
        remote(block, block, self.sems, 2, self.partner).wait_recv()

    def finish(self):
        self.first.wait_send()
        self.second.wait_send()
        self.third.wait_send()


def greet_devices(devices):
    barrier = pltpu.get_barrier_semaphore()
    for device in devices:
        pl.semaphore_signal(barrier, inc=1, device_id=device, device_id_type=MESH_ID)
    pl.semaphore_wait(barrier, len(devices))


def ctx_peers(p):
    return [((p.c + step) % 8, p.s) for step in range(1, 8)]


def wsh_peers(p):
    return [(p.c, (p.s + step) % 4) for step in range(1, 4)]


def nt(left, right):
    return lax.dot_general(
        left, right, (((1,), (1,)), ((), ())), preferred_element_type=jnp.float32
    )


def nn(left, right):
    return jnp.dot(left, right, preferred_element_type=jnp.float32)


def tn(left, right):
    return lax.dot_general(
        left, right, (((0,), (0,)), ((), ())), preferred_element_type=jnp.float32
    )


def normalized(values):
    row_mean = jnp.mean(values, axis=-1, keepdims=True)
    centered = values - row_mean
    variance = jnp.mean(centered * centered, axis=-1, keepdims=True)
    scale = lax.rsqrt(variance + norm_eps)
    return centered * scale, scale


class LineReduce:
    count = 12

    def __init__(self, place, mine, from_x, from_low, from_high, out, acc, sems):
        self.p, self.mine, self.sems = place, mine, sems
        self.from_x, self.from_low, self.from_high = from_x, from_low, from_high
        self.out, self.acc = out, acc

    def order(self, index):
        near = self.p.z // 2
        z = self.p.z * (1 - near) + (3 - self.p.z) * near
        inner = (1 - index % 2) * (3 - index // 2) + (index % 2) * (index // 2)
        dest = (1 - z) * (3 - index) + z * inner
        return dest * (1 - near) + (3 - dest) * near

    def x_copy(self, dest):
        p = self.p
        return remote(
            self.mine.at[dest * 2 + 1 - p.x],
            self.from_x.at[dest],
            self.sems,
            dest,
            (p.ctx_of(0, 1), p.s),
        )

    def up_copy(self, dest):
        p = self.p
        to = ((p.z + 1) * 2 + p.x, p.s)
        return remote(self.out.at[dest], self.from_low.at[dest], self.sems, 4 + dest, to)

    def down_copy(self, dest):
        p = self.p
        to = ((p.z - 1) * 2 + p.x, p.s)
        return remote(self.out.at[dest], self.from_high.at[dest], self.sems, 8 + dest, to)

    def start(self, first=0, last=4):
        def body(index, carry):
            self.x_copy(self.order(index)).start()
            return carry

        lax.fori_loop(first, last, body, 0)

    def add(self, dest, target, source, keep):
        rows = self.acc.shape[0]

        def body(index, carry):
            part = pl.ds(pl.multiple_of(index * 32, 32), 32)
            if keep:
                self.acc[part, :] = self.acc[part, :] + source[dest, part, :].astype(jnp.float32)
            else:
                slot = dest * 2 + self.p.x
                self.acc[part, :] = self.mine[slot, part, :].astype(jnp.float32) + source[
                    dest, part, :
                ].astype(jnp.float32)
            return carry

        lax.fori_loop(0, rows // 32, body, 0)

    def combine(self):
        p = self.p

        def body(index, carry):
            dest = self.order(index)
            self.x_copy(dest).wait_recv()
            self.add(dest, None, self.from_x, False)

            @pl.when((dest >= p.z) & (p.z > 0))
            def _():
                self.up_copy(dest).wait_recv()
                self.add(dest, None, self.from_low, True)

            @pl.when((dest <= p.z) & (p.z < 3))
            def _():
                self.down_copy(dest).wait_recv()
                self.add(dest, None, self.from_high, True)

            @pl.when(dest != p.z)
            def _():
                rows = self.acc.shape[0]

                def down(step, inner):
                    part = pl.ds(pl.multiple_of(step * 32, 32), 32)
                    self.out[dest, part, :] = self.acc[part, :].astype(self.out.dtype)
                    return inner

                lax.fori_loop(0, rows // 32, down, 0)

            @pl.when(dest > p.z)
            def _():
                self.up_copy(dest).start()

            @pl.when(dest < p.z)
            def _():
                self.down_copy(dest).start()

            return carry

        lax.fori_loop(0, 4, body, 0)

    def finish(self):
        p = self.p
        for dest in range(4):
            self.x_copy(dest).wait_send()

            @pl.when(dest > p.z)
            def _(dest=dest):
                self.up_copy(dest).wait_send()

            @pl.when(dest < p.z)
            def _(dest=dest):
                self.down_copy(dest).wait_send()


class QuadSwap:
    def __init__(self, place, src_of, dst, sems):
        self.p, self.src_of, self.dst, self.sems = place, src_of, dst, sems
        self.sent = []

    def start(self):
        p = self.p
        for index, (to_y, to_k) in enumerate(((1, 1), (1, 0), (0, 1))):
            to = p.wsh_of(to_y, to_k)
            copy = remote(self.src_of(to), self.dst.at[p.s], self.sems, index, (p.c, to))
            copy.start()
            self.sent.append(copy)

    def arrived(self):
        p = self.p
        for index, (to_y, to_k) in enumerate(((1, 1), (1, 0), (0, 1))):
            source = p.wsh_of(to_y, to_k)
            block = self.dst.at[source]
            remote(block, block, self.sems, index, (p.c, source)).wait_recv()

    def finish(self):
        for copy in self.sent:
            copy.wait_send()


def layer_kernel(
    tok, cot, vec, w_project, w_combine, w_expand, w_reduce, pos_row, pos_col,
    layer_output, in_grad, reduce_all, combine_all, expand_all, project_all, vec_sum, square_out,
    tok_all, vec_all_in, n1, q, k, v, wp, wc, we, wr, dy, table, attended, lse, middle, two, cols,
    att_low, att_rows, two_mine,
    hidden, d_pre, pre_sum, two_out, two_own, out_terms, layer_out, pair_in, over_in,
    mid_grad, branch, att_grad, ff,
    datt, branch_all, dqkv, dk, dv, gp_mine, gp_terms,
    f_x, f_low, f_high, f_out, f_acc, t_mine, t_x, t_low, t_high, t_out, t_acc,
    reduce_own, combine_own, expand_terms, expand_own, project_own,
    vec_mine, vec_terms, vec_own, vec_all, sq_own, sq_all, sq_line, sq_group,
    g_first, pair_send, pair_recv, we_send, we_recv, att_send, att_recv, col_send, col_recv,
    ff_send, ff_recv, a_send, a_recv, r_sems, quad_send, quad_recv, g_sems, loc,
):
    p = Place()
    rows, width = tok.shape
    total = n1.shape[0]
    wide = jnp.float32
    cut = width // 32
    shard = w_combine.shape[0]
    hc = q.shape[1]
    low = jnp.bfloat16
    own_wp = [
        pltpu.make_async_copy(
            w_project.at[:, pl.ds(pl.multiple_of(part * width + p.c * hc, hc), hc)],
            wp.at[p.s, :, pl.ds(part * hc, hc)],
            loc.at[part],
        )
        for part in range(3)
    ]
    own = [
        pltpu.make_async_copy(tok, tok_all.at[p.c], loc.at[3]),
        pltpu.make_async_copy(vec, vec_all_in.at[p.s], loc.at[4]),
        pltpu.make_async_copy(w_combine, wc.at[p.s], loc.at[5]),
        pltpu.make_async_copy(cot, dy.at[p.s], loc.at[6]),
        pltpu.make_async_copy(
            w_expand.at[:, pl.ds(pl.multiple_of(p.s * width, width), width)],
            we.at[p.s],
            loc.at[7],
        ),
    ]
    load_reduce = pltpu.make_async_copy(w_reduce, wr, loc.at[10])
    for copy in own_wp + own + [load_reduce]:
        copy.start()
    greet_devices(ctx_peers(p) + wsh_peers(p))
    gather = LineGather(p, tok, tok_all, (g_first.at[0], g_first.at[1]))
    gather.start()

    def pair(index, src, dst):
        return PairGather(p, src, dst, (pair_send.at[index], pair_recv.at[index]))

    vec_pair = pair(0, vec, vec_all_in)
    vec_pair.start()
    for copy in own_wp:
        copy.wait()
    wp_pair = pair(1, wp.at[p.s], wp)
    wp_pair.start()
    wc_pair = pair(2, w_combine, wc)
    wc_pair.start()
    dy_pair = pair(3, cot, dy)
    dy_pair.start()
    we_copies = []
    for index, (to_y, to_k) in enumerate(((1, 1), (1, 0), (0, 1))):
        to = p.wsh_of(to_y, to_k)
        copy = remote(
            w_expand.at[:, pl.ds(pl.multiple_of(to * width, width), width)],
            we.at[p.s],
            (we_send, we_recv),
            index,
            (p.c, to),
        )
        copy.start()
        we_copies.append(copy)

    vec_pair.relay()
    own[1].wait()
    vec_pair.arrived()
    for source in range(4):
        table[:, source * shard : (source + 1) * shard] = vec_all_in[source].astype(jnp.float32)
    gain, bias = table[0:1, :], table[1:2, :]

    def norm_block(slot):
        scaled, _ = normalized(tok_all[slot].astype(jnp.float32))
        n1[pl.ds(pl.multiple_of(slot * rows, rows), rows), :] = (scaled * gain + bias).astype(low)

    own[0].wait()
    gather.advance(1)
    wp_pair.relay()
    gather.advance(2)
    wc_pair.relay()
    gather.advance(3)
    step_z = 1 - 2 * (p.z // 2)

    def own_line(index, carry):
        norm_block((p.z + index * step_z + 4) % 4 * 2 + p.x)
        return carry

    lax.fori_loop(0, 4, own_line, 0)

    def other_line(index, carry):
        source_z = (p.z + index * step_z + 4) % 4
        gather.across(source_z)
        norm_block(source_z * 2 + 1 - p.x)
        return carry

    lax.fori_loop(0, 4, other_line, 0)
    wp_pair.arrived()
    head_cols = pl.ds(pl.multiple_of(p.c * hc, hc), hc)
    bias_q, bias_v = table[2:3, head_cols], table[3:4, head_cols]

    def project(index, carry):
        part = pl.ds(pl.multiple_of(index * 256, 256), 256)
        out = nn(n1[part, :], wp[...].reshape(width, 3 * hc))
        q[part, :] = (out[:, :hc] + bias_q).astype(low)
        k[part, :] = out[:, hc : 2 * hc].astype(low)
        v[part, :] = (out[:, 2 * hc :] + bias_v).astype(low)
        return carry

    lax.fori_loop(0, total // 256, project, 0)
    dy_pair.relay()
    wc_pair.arrived()
    dy_pair.arrived()

    scale = (width // HEADS) ** (-0.5)

    def att_copy(dest, source_rows):
        return remote(
            att_low.at[dest],
            att_rows.at[:, head_cols],
            (att_send, att_recv),
            0,
            (dest, p.s),
        )

    def att_send_to(dest):
        return pltpu.make_async_remote_copy(
            src_ref=att_low.at[dest],
            dst_ref=att_rows.at[:, head_cols],
            send_sem=att_send.at[dest],
            recv_sem=att_recv.at[p.c],
            device_id=(dest, p.s),
            device_id_type=MESH_ID,
        )

    def att_own():
        return pltpu.make_async_copy(att_low.at[p.c], att_rows.at[:, head_cols], loc.at[8])

    def attend(index, carry):
        part = pl.ds(pl.multiple_of(index * 256, 256), 256)
        queries = q[part, :]
        seen = pos_row[0:1, :] <= pos_col[part, :]
        first = lax.broadcasted_iota(jnp.int32, (256, hc), 1) < hc // 2
        outs, logs = [], []
        for head in range(2):
            mine = first if head == 0 else jnp.logical_not(first)
            scores = nt(jnp.where(mine, queries, jnp.zeros_like(queries)), k[...]) * scale
            scores = jnp.where(seen, scores, masked_score)
            peak = jnp.max(scores, axis=1, keepdims=True)
            grown = jnp.exp(scores - peak)
            whole = jnp.sum(grown, axis=1, keepdims=True)
            probs = (grown * (1.0 / whole)).astype(low)
            outs.append(nn(probs, v[...]))
            logs.append(peak + jnp.log(whole))
        mixed = jnp.where(first, outs[0], outs[1])
        attended[part, :] = mixed
        lse[part, :] = jnp.where(first, logs[0], logs[1])
        mixed_low = mixed.astype(low)
        for half in range(2):
            dest = index * 2 + half
            att_low[dest] = mixed_low[half * 128 : (half + 1) * 128]

            @pl.when(dest != p.c)
            def _(dest=dest):
                att_send_to(dest).start()

            @pl.when(dest == p.c)
            def _():
                att_own().start()

        return carry

    lax.fori_loop(0, total // 256, attend, 0)
    att_own().wait()
    for step in range(1, 8):
        source = (p.c + step) % 8
        landed = att_rows.at[:, pl.ds(pl.multiple_of(source * hc, hc), hc)]
        pltpu.make_async_remote_copy(
            src_ref=landed,
            dst_ref=landed,
            send_sem=att_send.at[source],
            recv_sem=att_recv.at[source],
            device_id=(source, p.s),
            device_id_type=MESH_ID,
        ).wait_recv()
    own[2].wait()
    mid = tok[...].astype(jnp.float32) + nn(att_rows[...], wc[...].reshape(width, width)) + table[4:5, :]
    middle[...] = mid
    scaled, _ = normalized(mid)
    two_mine[...] = (scaled * table[5:6, :] + table[6:7, :]).astype(low)
    two[p.s] = two_mine[...]
    two_pair = pair(4, two_mine, two)
    two_pair.start()
    col_copies = []
    for index, (to_y, to_k) in enumerate(((1, 1), (1, 0), (0, 1))):
        to = p.wsh_of(to_y, to_k)
        copy = remote(
            att_rows.at[:, pl.ds(pl.multiple_of(to * shard, shard), shard)],
            cols.at[p.s],
            (col_send, col_recv),
            index,
            (p.c, to),
        )
        copy.start()
        col_copies.append(copy)
    own_cols = pltpu.make_async_copy(
        att_rows.at[:, pl.ds(pl.multiple_of(p.s * shard, shard), shard)], cols.at[p.s], loc.at[9]
    )
    own_cols.start()
    two_pair.relay()
    for index, (to_y, to_k) in enumerate(((1, 1), (1, 0), (0, 1))):
        source = p.wsh_of(to_y, to_k)
        remote(we.at[source], we.at[source], (we_send, we_recv), index, (p.c, source)).wait_recv()
    own[3].wait()
    own[4].wait()
    load_reduce.wait()
    two_pair.arrived()

    bias_ff = table[pl.ds(8 + p.s, 1), :]
    pre_sum[...] = jnp.zeros_like(pre_sum)

    def feed(dest):
        pre = nn(two[dest], we[...].reshape(width, width)) + bias_ff
        share = 0.5 * (1.0 + lax.erf(pre * (0.5**0.5)))
        act = (pre * share).astype(low)
        hidden[dest] = act
        slope = share + pre * (jnp.exp(-0.5 * pre * pre) * (0.5 / math.pi) ** 0.5)
        grad = (nt(dy[dest], wr[...]) * slope).astype(low)
        d_pre[dest] = grad
        pre_sum[...] += jnp.sum(grad.astype(wide), axis=0, keepdims=True)
        return nt(grad, we[...].reshape(width, width))

    def pair_copy(group, index, src):
        return remote(src, pair_in.at[group, index], (ff_send.at[group], ff_recv.at[group]), index, (p.c, p.wsh_of(0, 1)))

    def over_copy(group, src):
        return remote(src, over_in.at[group], (ff_send.at[group], ff_recv.at[group]), 2, (p.c, p.wsh_of(1, 0)))

    across, beside, partner = p.wsh_of(1, 1), p.wsh_of(1, 0), p.wsh_of(0, 1)
    two_out[0] = feed(across).astype(low)
    pair_copy(0, 0, two_out.at[0]).start()
    part_beside = feed(beside)
    pair_copy(0, 0, two_out.at[0]).wait_recv()
    two_out[1] = (part_beside + pair_in[0, 0].astype(wide)).astype(low)
    over_copy(0, two_out.at[1]).start()
    two_out[2] = feed(partner).astype(low)
    pair_copy(0, 1, two_out.at[2]).start()
    two_own[...] = feed(p.s)

    for part in range(4):
        block = pl.ds(part * 256, 256)
        out = tn(
            hidden[:, :, block].reshape(4 * rows, 256), dy[...].reshape(4 * rows, width)
        ).astype(low)
        ff[2 * part, 0:rows, :] = out[:rows]
        ff[2 * part + 1, 0:rows, :] = out[rows:]
        out = tn(
            two[:, :, block].reshape(4 * rows, 256), d_pre[...].reshape(4 * rows, width)
        ).astype(low)
        for dest in range(8):
            ff[dest, rows + part * cut : rows + (part + 1) * cut, :] = out[
                dest * cut : (dest + 1) * cut
            ]
    ff_line = LineReduce(p, ff, f_x, f_low, f_high, f_out, f_acc, (r_sems.at[0], r_sems.at[1]))
    ff_line.start(0, 1)

    pair_copy(0, 1, two_out.at[2]).wait_recv()
    over_copy(0, two_out.at[1]).wait_recv()
    grad_two = two_own[...] + pair_in[0, 1].astype(wide) + over_in[0].astype(wide)
    hat_two, spread_two = normalized(middle[...])
    inner = grad_two * table[5:6, :]
    cot_wide = cot[...].astype(wide)
    mid_grad[...] = cot_wide + spread_two * (
        inner
        - jnp.mean(inner, axis=1, keepdims=True)
        - hat_two * jnp.mean(inner * hat_two, axis=1, keepdims=True)
    )
    vec_mine[...] = jnp.zeros_like(vec_mine)
    branch[...] = mid_grad[...].astype(low)
    att_grad[...] = nt(branch[...], wc[...].reshape(width, width)).astype(low)
    def a_copy(dest):
        return pltpu.make_async_remote_copy(
            src_ref=att_grad.at[:, pl.ds(pl.multiple_of(dest * hc, hc), hc)],
            dst_ref=datt.at[p.c],
            send_sem=a_send.at[dest],
            recv_sem=a_recv.at[p.c],
            device_id=(dest, p.s),
            device_id_type=MESH_ID,
        )

    for dz, dx in CtxSwap.steps:
        a_copy(p.ctx_of(dz, dx)).start()
    own_att = pltpu.make_async_copy(
        att_grad.at[:, pl.ds(pl.multiple_of(p.c * hc, hc), hc)], datt.at[p.c], loc.at[11]
    )
    own_att.start()
    own_branch = pltpu.make_async_copy(branch, branch_all.at[p.s], loc.at[12])
    own_branch.start()
    branch_pair = pair(5, branch, branch_all)
    branch_pair.start()
    ff_line.start(1, 4)
    vec_mine[4:5, :] = jnp.sum(branch[...].astype(wide), axis=0, keepdims=True)
    vec_mine[5:6, :] = jnp.sum(grad_two * hat_two, axis=0, keepdims=True)
    vec_mine[6:7, :] = jnp.sum(grad_two, axis=0, keepdims=True)
    vec_mine[7:8, :] = jnp.sum(cot_wide, axis=0, keepdims=True)
    vec_mine[pl.ds(8 + p.s, 1), :] = pre_sum[...]

    def out_part(dest):
        return nn(hidden[dest], wr[...])

    out_terms[0] = out_part(across).astype(low)
    pair_copy(1, 0, out_terms.at[0]).start()
    out_terms[2] = out_part(partner).astype(low)
    pair_copy(1, 1, out_terms.at[2]).start()
    out_beside = out_part(beside)
    pair_copy(1, 0, out_terms.at[0]).wait_recv()
    out_terms[1] = (out_beside + pair_in[1, 0].astype(wide)).astype(low)
    over_copy(1, out_terms.at[1]).start()
    layer_out[...] = out_part(p.s)
    dk[...] = jnp.zeros_like(dk)
    dv[...] = jnp.zeros_like(dv)
    own_att.wait()
    for step in range(1, 8):
        source = (p.c + step) % 8
        pltpu.make_async_remote_copy(
            src_ref=datt.at[source],
            dst_ref=datt.at[source],
            send_sem=a_send.at[source],
            recv_sem=a_recv.at[source],
            device_id=(source, p.s),
            device_id_type=MESH_ID,
        ).wait_recv()

    def attend_back(index, carry):
        part = pl.ds(pl.multiple_of(index * 256, 256), 256)
        queries = q[part, :]
        grads = jnp.concatenate([datt[index * 2], datt[index * 2 + 1]], axis=0)
        seen = pos_row[0:1, :] <= pos_col[part, :]
        first = lax.broadcasted_iota(jnp.int32, (256, hc), 1) < hc // 2
        both = grads.astype(wide) * attended[part, :]
        outs = []
        for head in range(2):
            mine = first if head == 0 else jnp.logical_not(first)
            q_head = jnp.where(mine, queries, jnp.zeros_like(queries))
            g_head = jnp.where(mine, grads, jnp.zeros_like(grads))
            logs = lse[part, head * (hc // 2) : head * (hc // 2) + 1]
            scores = jnp.where(seen, nt(q_head, k[...]) * scale, masked_score)
            soft = jnp.exp(scores - logs)
            delta = jnp.sum(jnp.where(mine, both, 0.0), axis=1, keepdims=True)
            score_grad = (soft * (nt(g_head, v[...]) - delta)).astype(low)
            outs.append(nn(score_grad, k[...]))
            dk[...] += tn(score_grad, q_head)
            dv[...] += tn(soft.astype(low), g_head)
        dqkv[part, 0:hc] = (jnp.where(first, outs[0], outs[1]) * scale).astype(low)
        return carry

    lax.fori_loop(0, total // 256, attend_back, 0)
    dqkv[:, hc : 2 * hc] = (dk[...] * scale).astype(low)
    dqkv[:, 2 * hc :] = dv[...].astype(low)

    def one_terms(index, carry):
        part = pl.ds(pl.multiple_of(index * 256, 256), 256)
        out = nt(dqkv[part, :], wp[...].reshape(width, 3 * hc)).astype(low)
        t_mine[index * 2, 0:rows, :] = out[:rows]
        t_mine[index * 2 + 1, 0:rows, :] = out[rows:]
        return carry

    lax.fori_loop(0, total // 256, one_terms, 0)
    own_branch.wait()
    branch_pair.relay()
    branch_pair.arrived()
    for index, (to_y, to_k) in enumerate(((1, 1), (1, 0), (0, 1))):
        source = p.wsh_of(to_y, to_k)
        remote(cols.at[source], cols.at[source], (col_send, col_recv), index, (p.c, source)).wait_recv()
    own_cols.wait()
    grad_combine = tn(
        cols[...].reshape(4 * rows, shard), branch_all[...].reshape(4 * rows, width)
    ).astype(low)
    for dest in range(8):
        t_mine[dest, rows : rows + cut, :] = grad_combine[dest * cut : (dest + 1) * cut]
    tail = LineReduce(p, t_mine, t_x, t_low, t_high, t_out, t_acc, (r_sems.at[2], r_sems.at[3]))
    tail.start()
    for dest in range(4):
        gp_mine[dest] = tn(n1[:, dest * shard : (dest + 1) * shard], dqkv[...]).astype(low)
    gp_swap = QuadSwap(p, lambda to: gp_mine.at[to], gp_terms, (quad_send.at[0], quad_recv.at[0]))
    gp_swap.start()
    own_gp = pltpu.make_async_copy(gp_mine.at[p.s], gp_terms.at[p.s], loc.at[13])
    own_gp.start()

    pair_copy(1, 1, out_terms.at[2]).wait_recv()
    over_copy(1, out_terms.at[1]).wait_recv()
    layer_output[...] = (
        middle[...]
        + (layer_out[...] + pair_in[1, 1].astype(wide) + over_in[1].astype(wide))
        + table[7:8, :]
    ).astype(low)

    ff_line.combine()
    reduce_own[...] = f_acc[0:rows, :].astype(low)
    for part in range(4):
        f_out[p.z, part * cut : (part + 1) * cut, :] = f_acc[
            rows + part * cut : rows + (part + 1) * cut, :
        ].astype(low)
    expand_swap = QuadSwap(
        p,
        lambda to: f_out.at[p.z, pl.ds(pl.multiple_of(to * cut, cut), cut)],
        expand_terms,
        (quad_send.at[1], quad_recv.at[1]),
    )
    expand_swap.start()
    own_expand = pltpu.make_async_copy(
        f_out.at[p.z, pl.ds(pl.multiple_of(p.s * cut, cut), cut)], expand_terms.at[p.s], loc.at[14]
    )
    own_expand.start()
    gathers = []

    def share_out(index, src, dst):
        line = LineGather(p, src, dst, (g_sems.at[2 * index], g_sems.at[2 * index + 1]))
        line.start()
        own = pltpu.make_async_copy(src, dst.at[p.c], loc.at[15 + index])
        own.start()
        gathers.append((line, own))

    share_out(0, reduce_own, reduce_all)
    square = jnp.sum(jnp.square(reduce_own[...].astype(wide)))
    expand_swap.arrived()
    own_expand.wait()
    for part in range(4):
        expand_own[:, part * width : (part + 1) * width] = expand_terms[part]
    share_out(1, expand_own, expand_all)
    square += jnp.sum(jnp.square(expand_own[...].astype(wide)))
    gp_swap.arrived()
    own_gp.wait()
    project_own[...] = jnp.sum(gp_terms[...].astype(wide), axis=0).astype(low)
    square += jnp.sum(jnp.square(project_own[...].astype(wide)))
    share_out(2, project_own, project_all)

    tail.combine()
    combine_own[...] = t_acc[rows : rows + cut, :].astype(low)
    square += jnp.sum(jnp.square(combine_own[...].astype(wide)))
    share_out(3, combine_own, combine_all)
    grad = t_acc[0:rows, :]
    hat, spread = normalized(tok[...].astype(wide))
    hat_grad = grad * table[0:1, :]
    back = spread * (
        hat_grad
        - jnp.mean(hat_grad, axis=1, keepdims=True)
        - hat * jnp.mean(hat_grad * hat, axis=1, keepdims=True)
    )
    in_grad[...] = (mid_grad[...] + back).astype(low)
    vec_mine[0:1, :] = jnp.sum(grad * hat, axis=0, keepdims=True)
    vec_mine[1:2, :] = jnp.sum(grad, axis=0, keepdims=True)
    heads = pl.ds(pl.multiple_of(p.c * hc, hc), hc)
    vec_mine[2:3, heads] = jnp.sum(dqkv[:, 0:hc].astype(wide), axis=0, keepdims=True)
    vec_mine[3:4, heads] = jnp.sum(dqkv[:, 2 * hc :].astype(wide), axis=0, keepdims=True)
    vec_swap = QuadSwap(
        p,
        lambda to: vec_mine.at[:, pl.ds(pl.multiple_of(to * shard, shard), shard)],
        vec_terms,
        (quad_send.at[2], quad_recv.at[2]),
    )
    vec_swap.start()
    vec_terms[p.s] = vec_mine[:, pl.ds(pl.multiple_of(p.s * shard, shard), shard)]
    sq_own[...] = jnp.full(sq_own.shape, square, wide)
    vec_swap.arrived()
    vec_own[...] = jnp.sum(vec_terms[...], axis=0)
    share_out(4, vec_own, vec_all)
    share_out(5, sq_own, sq_all)
    for step in (1, 2, 3):
        for line, _ in gathers:
            line.advance(step)
    for source_z in range(4):
        for line, _ in gathers:
            line.across(source_z)
    for _, own in gathers:
        own.wait()
    vectors = jnp.sum(vec_all[...], axis=0)
    vec_sum[...] = vectors
    sq_line[...] = jnp.sum(sq_all[...], axis=0) + jnp.sum(jnp.square(vectors))
    sq_pair = pair(6, sq_line, sq_group)
    sq_pair.start()
    sq_group[p.s] = sq_line[...]
    sq_pair.relay()
    sq_pair.arrived()
    square_out[...] = jnp.sum(sq_group[...], axis=0)
    for line, _ in gathers:
        line.finish()
    ff_line.finish()
    tail.finish()
    for member in (branch_pair, sq_pair, gp_swap, expand_swap, vec_swap):
        member.finish()
    for copy in we_copies + col_copies:
        copy.wait_send()
    gather.finish()
    for member in (vec_pair, wp_pair, wc_pair, dy_pair, two_pair):
        member.finish()
    for group, terms in enumerate((two_out, out_terms)):
        pair_copy(group, 0, terms.at[0]).wait_send()
        pair_copy(group, 1, terms.at[2]).wait_send()
        over_copy(group, terms.at[1]).wait_send()
    for step in range(1, 8):
        att_send_to((p.c + step) % 8).wait_send()
    for step in range(1, 8):
        a_copy((p.c + step) % 8).wait_send()


def layer_fused(tok, cot, vec, w_project, w_combine, w_expand, w_reduce, pos_row, pos_col):
    low, wide = jnp.bfloat16, jnp.float32
    rows, width = tok.shape
    total = rows * 8
    hc = width // 8
    shard = width // 4
    cut = shard // 8
    ff_rows, tail_rows = rows + 4 * cut, rows + cut
    vmem, hbm = pl.BlockSpec(memory_space=pltpu.VMEM), pl.BlockSpec(memory_space=pl.ANY)
    dma = pltpu.SemaphoreType.DMA
    mem = pltpu.VMEM
    return pl.pallas_call(
        layer_kernel,
        out_shape=[
            shape((rows, width), low),
            shape((rows, width), low),
            shape((8, rows, width), low),
            shape((8, cut, width), low),
            shape((8, cut, 4 * width), low),
            shape((8, shard, 3 * hc), low),
            shape((16, shard), wide),
            shape((8, 128), wide),
        ],
        in_specs=[vmem, vmem, vmem, hbm, vmem, hbm, hbm, vmem, vmem],
        out_specs=[vmem, vmem, hbm, hbm, hbm, hbm, vmem, vmem],
        scratch_shapes=[
            mem((8, rows, width), low),
            mem((4, 16, shard), low),
            mem((total, width), low),
            mem((total, hc), low),
            mem((total, hc), low),
            mem((total, hc), low),
            mem((4, shard, 3 * hc), low),
            mem((4, shard, width), low),
            mem((4, shard, width), low),
            mem((width, width), low),
            mem((4, rows, width), low),
            mem((16, width), wide),
            mem((total, hc), wide),
            mem((total, hc), wide),
            mem((rows, width), wide),
            mem((4, rows, width), low),
            mem((4, rows, shard), low),
            mem((8, rows, hc), low),
            mem((rows, width), low),
            mem((rows, width), low),
            mem((4, rows, width), low),
            mem((4, rows, width), low),
            mem((1, width), wide),
            mem((3, rows, width), low),
            mem((rows, width), wide),
            mem((3, rows, width), low),
            mem((rows, width), wide),
            mem((2, 2, rows, width), low),
            mem((2, rows, width), low),
            mem((rows, width), wide),
            mem((rows, width), low),
            mem((rows, width), low),
            mem((8, ff_rows, width), low),
            mem((8, rows, hc), low),
            mem((4, rows, width), low),
            mem((total, 3 * hc), low),
            mem((total, hc), wide),
            mem((total, hc), wide),
            mem((4, shard, 3 * hc), low),
            mem((4, shard, 3 * hc), low),
            mem((4, ff_rows, width), low),
            mem((4, ff_rows, width), low),
            mem((4, ff_rows, width), low),
            mem((4, ff_rows, width), low),
            mem((ff_rows, width), wide),
            mem((8, tail_rows, width), low),
            mem((4, tail_rows, width), low),
            mem((4, tail_rows, width), low),
            mem((4, tail_rows, width), low),
            mem((4, tail_rows, width), low),
            mem((tail_rows, width), wide),
            mem((rows, width), low),
            mem((cut, width), low),
            mem((4, cut, width), low),
            mem((cut, 4 * width), low),
            mem((shard, 3 * hc), low),
            mem((16, width), wide),
            mem((4, 16, shard), wide),
            mem((16, shard), wide),
            mem((8, 16, shard), wide),
            mem((8, 128), wide),
            mem((8, 8, 128), wide),
            mem((8, 128), wide),
            mem((4, 8, 128), wide),
            dma((2, 12)),
            dma((7, 3)),
            dma((7, 3)),
            dma((3,)),
            dma((3,)),
            dma((8,)),
            dma((8,)),
            dma((3,)),
            dma((3,)),
            dma((2, 3)),
            dma((2, 3)),
            dma((8,)),
            dma((8,)),
            dma((4, 12)),
            dma((3, 3)),
            dma((3, 3)),
            dma((12, 12)),
            dma((21,)),
        ],
        compiler_params=pltpu.CompilerParams(
            collective_id=10, has_side_effects=True, vmem_limit_bytes=67043328
        ),
        name="layer",
    )(tok, cot, vec, w_project, w_combine, w_expand, w_reduce, pos_row, pos_col)


def optimizer_kernel(clip, *refs):
    factor = clip[0, 0]
    first_bias = 1.0 - beta_one**STEP
    second_bias = 1.0 - beta_two**STEP
    for index in range(4):
        weight, grad, first, second = refs[4 * index : 4 * index + 4]
        g_out, m_out, v_out, u_out = refs[16 + 4 * index : 20 + 4 * index]
        if len(grad.shape) == 3:
            pieces = [
                grad[source, :, part * 128 : (part + 1) * 128]
                for part in range(3)
                for source in range(grad.shape[0])
            ]
            total = jnp.concatenate(pieces, axis=1).astype(jnp.float32)
        else:
            total = grad[...].astype(jnp.float32)
        g_out[...] = total
        clipped = total * factor
        moment = beta_one * first[...] + (1.0 - beta_one) * clipped
        square = beta_two * second[...] + (1.0 - beta_two) * clipped * clipped
        m_out[...] = moment
        v_out[...] = square
        moment_hat = moment * (1.0 / first_bias)
        square_hat = square * (1.0 / second_bias)
        u_out[...] = -learn_rate * (
            moment_hat / (jnp.sqrt(square_hat) + adam_eps)
            + decay_rate * weight[...].astype(jnp.float32)
        )


def optimizer_fused(clip_factor, members):
    steps = members[1][0].shape[0] // 16
    operands, in_specs, out_specs, out_shape = [], [], [], []
    for weight, grad, first, second in members:
        rows, width = weight.shape
        block = rows // steps
        flat = pl.BlockSpec((block, width), lambda i: (i, 0))
        operands += [weight, grad, first, second]
        if grad.ndim == 3:
            grad_spec = pl.BlockSpec((8, block, grad.shape[2]), lambda i: (0, i, 0))
        else:
            grad_spec = flat
        in_specs += [flat, grad_spec, flat, flat]
        out_specs += [flat] * 4
        out_shape += [shape((rows, width), jnp.float32)] * 4
    return pl.pallas_call(
        optimizer_kernel,
        grid=(steps,),
        out_shape=out_shape,
        in_specs=[pl.BlockSpec(memory_space=pltpu.SMEM)] + in_specs,
        out_specs=out_specs,
        compiler_params=pltpu.CompilerParams(vmem_limit_bytes=56 * 2**20),
        name="optimizer",
    )(clip_factor.reshape(1, 1), *operands)


def adam_step(weight, gradient, first_moment, second_moment, clip_factor, step_value):
    clipped = gradient * clip_factor
    moment = beta_one * first_moment + (1.0 - beta_one) * clipped
    square = beta_two * second_moment + (1.0 - beta_two) * clipped * clipped
    moment_hat = moment / (1.0 - jnp.power(jnp.float32(beta_one), step_value))
    square_hat = square / (1.0 - jnp.power(jnp.float32(beta_two), step_value))
    update = -learn_rate * (
        moment_hat / (jnp.sqrt(square_hat) + adam_eps) + decay_rate * weight.astype(jnp.float32)
    )
    return (moment, square, update)


def body_plain(
    tokens,
    output_cotangent,
    block_table,
    weight_project,
    weight_combine,
    weight_expand,
    weight_reduce,
    vectors,
    moment_project,
    square_project,
    moment_combine,
    square_combine,
    moment_expand,
    square_expand,
    moment_reduce,
    square_reduce,
    moment_vectors,
    square_vectors,
):
    low = jnp.bfloat16
    ctx_count, wsh_count = lax.axis_size("ctx"), lax.axis_size("wsh")
    ctx_index, wsh_index = lax.axis_index("ctx"), lax.axis_index("wsh")
    rows_dev, width = tokens.shape[1], tokens.shape[2]
    block_rows = rows_dev // 2
    total_rows = rows_dev * ctx_count
    group_rows = rows_dev * wsh_count
    head_size = width // HEADS
    score_scale = head_size ** (-0.5)
    head_cols = width // ctx_count
    local_heads = head_cols // head_size
    shard_rows = weight_project.shape[0]
    ff_width = weight_expand.shape[1]
    chunk = ff_width // wsh_count
    vec_rows = vectors.shape[0]
    swap = plain

    sequence = tokens[0].astype(jnp.float32)
    cotangent_low = output_cotangent[0]
    cotangent = cotangent_low.astype(jnp.float32)

    project_cols = lax.dynamic_slice_in_dim(
        weight_project.reshape(shard_rows, 3, ctx_count, head_cols), ctx_index, 1, axis=2
    ).reshape(shard_rows, 3 * head_cols)

    vec_pad = -vec_rows % 16
    (vec_parts,) = swap("vec", 0, (WshGather, jnp.pad(vectors, ((0, vec_pad), (0, 0)))))
    vec_table = (
        vec_parts[:, :vec_rows].transpose(1, 0, 2).reshape(vec_rows, width).astype(jnp.float32)
    )
    normed_one = layer_norm(sequence, vec_table[0], vec_table[1]).astype(low)
    normed_all, project_parts, cot_parts, combine_parts, expand_parts = swap(
        "front",
        1,
        (CtxGather, normed_one),
        (WshGather, project_cols),
        (WshGather, cotangent_low),
        (WshGather, weight_combine),
        (WshSwap, weight_expand.reshape(shard_rows, wsh_count, chunk).transpose(1, 0, 2)),
    )
    normed_all = normed_all.reshape(total_rows, width)
    project_mine = project_parts.reshape(width, 3 * head_cols)
    full_combine = combine_parts.reshape(width, width)
    expand_mine = expand_parts.reshape(width, chunk)
    cot_group = cot_parts.reshape(group_rows, width)

    qkv = matmul(normed_all, project_mine)
    bias_cols = lax.dynamic_slice_in_dim(
        vec_table[:4].reshape(4, ctx_count, head_cols), ctx_index, 1, axis=1
    ).reshape(4, head_cols)
    queries = (qkv[:, :head_cols] + bias_cols[2]).astype(low)
    keys = qkv[:, head_cols : 2 * head_cols].astype(low)
    values = (qkv[:, 2 * head_cols :] + bias_cols[3]).astype(low)
    positions = (
        block_table[:, None] * block_rows + jnp.arange(block_rows, dtype=jnp.int32)[None, :]
    ).reshape(total_rows)
    visible = positions[None, None, :] <= positions[None, :, None]
    heads = (total_rows, local_heads, head_size)
    query_heads, key_heads, value_heads = (
        queries.reshape(heads),
        keys.reshape(heads),
        values.reshape(heads),
    )
    scores = (
        jnp.einsum("qhd,khd->hqk", query_heads, key_heads, preferred_element_type=jnp.float32)
        * score_scale
    )
    scores = jnp.where(visible, scores, masked_score)
    peak = jnp.max(scores, axis=2, keepdims=True)
    grown = jnp.exp(scores - peak)
    soft = grown / jnp.sum(grown, axis=2, keepdims=True)
    soft_low = soft.astype(low)
    attended_heads = jnp.einsum(
        "hqk,khd->qhd", soft_low, value_heads, preferred_element_type=jnp.float32
    )
    attended = attended_heads.reshape(total_rows, head_cols)
    (att_parts,) = swap(
        "attended", 2, (CtxSwap, attended.astype(low).reshape(ctx_count, rows_dev, head_cols))
    )
    attended_rows = att_parts.transpose(1, 0, 2).reshape(rows_dev, width)

    middle = sequence + matmul(attended_rows, full_combine) + vec_table[4]
    normed_two = layer_norm(middle, vec_table[5], vec_table[6]).astype(low)
    two_parts, att_cols = swap(
        "normed_two",
        3,
        (WshGather, normed_two),
        (WshSwap, attended_rows.reshape(rows_dev, wsh_count, shard_rows).transpose(1, 0, 2)),
    )
    two_group = two_parts.reshape(group_rows, width)

    bias_ff = lax.dynamic_slice_in_dim(vec_table[8:].reshape(-1), wsh_index * chunk, chunk)
    hidden_pre = matmul(two_group, expand_mine) + bias_ff
    hidden, gelu_back = jax.vjp(gelu_exact, hidden_pre)
    hidden = hidden.astype(low)
    out_partial = matmul(hidden, weight_reduce)
    pre_grad = gelu_back(matmul_right_t(cot_group, weight_reduce))[0].astype(low)
    two_partial = matmul_right_t(pre_grad, expand_mine)
    part_shape = (wsh_count, rows_dev, width)
    two_terms, out_terms = swap(
        "ff_sums",
        4,
        (WshSwap, two_partial.astype(low).reshape(part_shape)),
        (WshSwap, out_partial.astype(low).reshape(part_shape)),
    )
    layer_output = middle + jnp.sum(out_terms.astype(jnp.float32), axis=0) + vec_table[7]
    normed_two_grad = jnp.sum(two_terms.astype(jnp.float32), axis=0)
    norm_two_back = jax.vjp(layer_norm, middle, vec_table[5], vec_table[6])[1](normed_two_grad)
    middle_grad = cotangent + norm_two_back[0]
    branch_grad = middle_grad.astype(low)
    attended_grad_rows = matmul_right_t(branch_grad, full_combine).astype(low)
    att_grad_parts, branch_parts = swap(
        "attended_grad",
        5,
        (CtxSwap, attended_grad_rows.reshape(rows_dev, ctx_count, head_cols).transpose(1, 0, 2)),
        (WshGather, branch_grad),
    )
    branch_group = branch_parts.reshape(group_rows, width)
    attended_grad = att_grad_parts.reshape(total_rows, head_cols)

    grad_reduce = matmul_left_t(hidden, cot_group)
    grad_expand = matmul_left_t(two_group, pre_grad)
    grad_combine = matmul_left_t(att_cols.reshape(group_rows, shard_rows), branch_group)

    grad_heads = attended_grad.reshape(heads)
    delta = jnp.sum(
        grad_heads.astype(jnp.float32) * attended_heads, axis=2
    ).transpose(1, 0)[:, :, None]
    soft_grad = jnp.einsum(
        "qhd,khd->hqk", grad_heads, value_heads, preferred_element_type=jnp.float32
    )
    score_grad = (soft * (soft_grad - delta)).astype(low)
    query_grad = (
        jnp.einsum("hqk,khd->qhd", score_grad, key_heads, preferred_element_type=jnp.float32)
        * score_scale
    )
    key_grad = (
        jnp.einsum("hqk,qhd->khd", score_grad, query_heads, preferred_element_type=jnp.float32)
        * score_scale
    )
    value_grad = jnp.einsum(
        "hqk,qhd->khd", soft_low, grad_heads, preferred_element_type=jnp.float32
    )
    flat = (total_rows, head_cols)
    qkv_grad = jnp.concatenate(
        [member.reshape(flat).astype(low) for member in (query_grad, key_grad, value_grad)], axis=1
    )
    grad_project = matmul_left_t(normed_all, qkv_grad)
    one_partial = matmul_right_t(qkv_grad, project_mine)

    cut = shard_rows // ctx_count
    cut_reduce = chunk // ctx_count
    for_ctx = jnp.concatenate(
        [
            grad_reduce.astype(low).reshape(ctx_count, cut_reduce, width),
            grad_combine.astype(low).reshape(ctx_count, cut, width),
        ],
        axis=1,
    )
    expand_ctx = (
        grad_expand.astype(low)
        .reshape(wsh_count, ctx_count, cut, chunk)
        .transpose(1, 0, 2, 3)
        .reshape(ctx_count, wsh_count * cut, chunk)
    )
    ctx_terms, expand_terms, one_terms, project_terms = swap(
        "grad_sums",
        6,
        (CtxSwap, for_ctx),
        (CtxSwap, expand_ctx),
        (CtxSwap, one_partial.astype(low).reshape(ctx_count, rows_dev, width)),
        (WshSwap, grad_project.astype(low).reshape(wsh_count, shard_rows, 3 * head_cols)),
    )
    normed_one_grad = jnp.sum(one_terms.astype(jnp.float32), axis=0)
    norm_one_back = jax.vjp(layer_norm, sequence, vec_table[0], vec_table[1])[1](normed_one_grad)
    input_gradient = (middle_grad + norm_one_back[0]).astype(low)
    ctx_piece = jnp.sum(ctx_terms.astype(jnp.float32), axis=0).astype(low)
    expand_piece = jnp.sum(expand_terms.astype(jnp.float32), axis=0).astype(low)
    project_piece = jnp.sum(project_terms.astype(jnp.float32), axis=0).astype(low)

    def spread(columns, start):
        return lax.dynamic_update_slice(
            jnp.zeros((width,), jnp.float32), columns, (start,)
        )

    ff_terms = lax.dynamic_update_slice(
        jnp.zeros((ff_width,), jnp.float32),
        jnp.sum(pre_grad.astype(jnp.float32), axis=0),
        (wsh_index * chunk,),
    ).reshape(-1, width)
    head_start = ctx_index * head_cols
    query_sum = jnp.sum(qkv_grad[:, :head_cols].astype(jnp.float32), axis=0)
    value_sum = jnp.sum(qkv_grad[:, 2 * head_cols :].astype(jnp.float32), axis=0)
    vec_terms = jnp.concatenate(
        [
            jnp.stack(
                [
                    norm_one_back[1],
                    norm_one_back[2],
                    spread(query_sum, head_start),
                    spread(value_sum, head_start),
                    jnp.sum(branch_grad.astype(jnp.float32), axis=0),
                    norm_two_back[1],
                    norm_two_back[2],
                    jnp.sum(cotangent, axis=0),
                ]
            ),
            ff_terms,
            jnp.zeros((vec_pad, width), jnp.float32),
        ],
        axis=0,
    )
    vec_cols = vectors.shape[1]
    vec_swapped, expand_rows = swap(
        "vec_sums",
        7,
        (WshSwap, vec_terms.reshape(-1, wsh_count, vec_cols).transpose(1, 0, 2)),
        (WshSwap, expand_piece.reshape(wsh_count, cut, chunk)),
    )
    vec_mine = jnp.sum(vec_swapped, axis=0)
    expand_mine_rows = expand_rows.transpose(1, 0, 2).reshape(cut, ff_width)
    square_mine = (
        jnp.sum(jnp.square(ctx_piece.astype(jnp.float32)))
        + jnp.sum(jnp.square(expand_rows.astype(jnp.float32)))
        + jnp.sum(jnp.square(project_piece.astype(jnp.float32)))
    )
    ctx_all, expand_all, project_all, vec_all, square_ctx = swap(
        "grads",
        8,
        (CtxGather, ctx_piece),
        (CtxGather, expand_mine_rows),
        (CtxGather, project_piece),
        (CtxGather, vec_mine),
        (CtxGather, jnp.full((16, 128), square_mine, jnp.float32)),
    )
    sum_reduce = ctx_all[:, :cut_reduce].reshape(chunk, width).astype(jnp.float32)
    sum_combine = ctx_all[:, cut_reduce:].reshape(shard_rows, width).astype(jnp.float32)
    sum_expand = expand_all.reshape(shard_rows, ff_width).astype(jnp.float32)
    sum_project = (
        project_all.reshape(ctx_count, shard_rows, 3, head_cols)
        .transpose(1, 2, 0, 3)
        .reshape(shard_rows, 3 * width)
        .astype(jnp.float32)
    )
    sum_vectors = jnp.sum(vec_all, axis=0)[:vec_rows]
    square_part = jnp.sum(square_ctx[:, 0, 0]) + jnp.sum(jnp.square(sum_vectors))
    (square_all,) = swap(
        "squares", 9, (WshGather, jnp.full((8, 128), square_part, jnp.float32))
    )
    norm_value = jnp.sqrt(jnp.sum(square_all[:, 0, 0]))
    params_total = 4 * width * width + 2 * width * ff_width + vec_rows * width
    clip_max = jnp.sqrt(jnp.float32(params_total))
    clip_factor = clip_max / jnp.maximum(norm_value, clip_max)
    step_value = jnp.float32(STEP)
    results = [layer_output.astype(low)[None], input_gradient[None], norm_value.reshape(1)]
    for weight, total, first, second in (
        (weight_project, sum_project, moment_project, square_project),
        (weight_combine, sum_combine, moment_combine, square_combine),
        (weight_expand, sum_expand, moment_expand, square_expand),
        (weight_reduce, sum_reduce, moment_reduce, square_reduce),
        (vectors, sum_vectors, moment_vectors, square_vectors),
    ):
        results.append(total)
        results.extend(adam_step(weight, total, first, second, clip_factor, step_value))
    return tuple(results)


def body_fast(
    tokens,
    output_cotangent,
    block_table,
    weight_project,
    weight_combine,
    weight_expand,
    weight_reduce,
    vectors,
    moment_project,
    square_project,
    moment_combine,
    square_combine,
    moment_expand,
    square_expand,
    moment_reduce,
    square_reduce,
    moment_vectors,
    square_vectors,
):
    rows_dev, width = tokens.shape[1], tokens.shape[2]
    block_rows = rows_dev // 2
    total_rows = rows_dev * 8
    ff_width = weight_expand.shape[1]
    vec_rows = vectors.shape[0]
    cot_low = output_cotangent[0]
    positions = (
        block_table[:, None] * block_rows + jnp.arange(block_rows, dtype=jnp.int32)[None, :]
    ).reshape(total_rows)
    pos_row = jnp.broadcast_to(positions[None, :], (8, total_rows))
    pos_col = positions[:, None]
    vec_padded = jnp.pad(vectors, ((0, -vec_rows % 16), (0, 0)))
    (
        layer_output, input_gradient, reduce_all, combine_all, expand_all, project_all, vec_sum,
        squares,
    ) = layer_fused(
        tokens[0], cot_low, vec_padded, weight_project, weight_combine, weight_expand,
        weight_reduce, pos_row, pos_col,
    )
    norm_value = jnp.sqrt(squares[0, 0])
    params_total = 4 * width * width + 2 * width * ff_width + vec_rows * width
    clip_max = jnp.sqrt(jnp.float32(params_total))
    clip_factor = clip_max / jnp.maximum(norm_value, clip_max)
    updated = optimizer_fused(
        clip_factor,
        (
            (weight_project, project_all, moment_project, square_project),
            (weight_combine, combine_all.reshape(-1, width), moment_combine, square_combine),
            (weight_expand, expand_all.reshape(-1, ff_width), moment_expand, square_expand),
            (weight_reduce, reduce_all.reshape(-1, width), moment_reduce, square_reduce),
        ),
    )
    vec_total = vec_sum[:vec_rows]
    vec_updated = adam_step(
        vectors, vec_total, moment_vectors, square_vectors, clip_factor, jnp.float32(STEP)
    )
    return (
        layer_output[None],
        input_gradient[None],
        norm_value.reshape(1),
        *updated,
        vec_total,
        *vec_updated,
    )


def solution(mesh):
    rows, cols = P("wsh", None), P(None, "wsh")
    token = P("wsh", "ctx", None)
    fast = (mesh.shape["ctx"], mesh.shape["wsh"]) == (FAST_CTX, FAST_WSH)
    return jax.shard_map(
        body_fast if fast else body_plain,
        mesh=mesh,
        in_specs=(token, token, P(), rows, rows, rows, rows, cols) + (rows,) * 8 + (cols,) * 2,
        out_specs=(token, token, P()) + (rows,) * 16 + (cols,) * 4,
        check_vma=False,
    )
```

```python
import math

import jax
import jax.numpy as jnp
from jax import lax
from jax.experimental import pallas as pl
from jax.experimental.pallas import tpu as pltpu
from jax.sharding import PartitionSpec as P

HEADS = 16
STEP = 4

norm_eps = 1e-05
masked_score = -1e30
beta_one = 0.9
beta_two = 0.95
learn_rate = 0.02
decay_rate = 0.1
adam_eps = 1e-08

MESH_ID = pl.DeviceIdType.MESH
FAST_CTX, FAST_WSH = 8, 4


def layer_norm(values, norm_gain, norm_bias):
    row_mean = jnp.mean(values, axis=-1, keepdims=True)
    centered = values - row_mean
    variance = jnp.mean(centered * centered, axis=-1, keepdims=True)
    return centered * lax.rsqrt(variance + norm_eps) * norm_gain + norm_bias


def gelu_exact(values):
    return jax.nn.gelu(values, approximate=False)


def matmul(left, right):
    return jnp.dot(left, right, preferred_element_type=jnp.float32)


def matmul_left_t(left, right):
    return lax.dot_general(
        left, right, (((0,), (0,)), ((), ())), preferred_element_type=jnp.float32
    )


def matmul_right_t(left, right):
    return lax.dot_general(
        left, right, (((1,), (1,)), ((), ())), preferred_element_type=jnp.float32
    )


class Place:
    def __init__(self):
        self.c = lax.axis_index("ctx")
        self.s = lax.axis_index("wsh")
        self.z, self.x = self.c // 2, self.c % 2
        self.y, self.k = self.s // 2, self.s % 2

    def ctx_of(self, dz, dx):
        return (self.z + dz + 4) % 4 * 2 + (self.x + dx) % 2

    def wsh_of(self, dy, dk):
        return (self.y + dy) % 2 * 2 + (self.k + dk) % 2


def remote(src, dst, sems, index, device):
    return pltpu.make_async_remote_copy(
        src_ref=src,
        dst_ref=dst,
        send_sem=sems[0].at[index],
        recv_sem=sems[1].at[index],
        device_id=device,
        device_id_type=MESH_ID,
    )


class CtxGather:
    pass


class CtxSwap:
    steps = ((2, 1), (2, 0), (1, 1), (-1, 1), (1, 0), (-1, 0), (0, 1))


class WshGather:
    pass


class WshSwap:
    pass


def plain(name, call_id, *pairs):
    outs = []
    for kind, array in pairs:
        if kind is CtxGather:
            outs.append(lax.all_gather(array, "ctx", axis=0))
        elif kind is WshGather:
            outs.append(lax.all_gather(array, "wsh", axis=0))
        elif kind is CtxSwap:
            outs.append(lax.all_to_all(array, "ctx", 0, 0, tiled=True))
        else:
            outs.append(lax.all_to_all(array, "wsh", 0, 0, tiled=True))
    return outs


def shape(dims, kind):
    return jax.ShapeDtypeStruct(dims, kind)


class LineGather:
    count = 12

    def __init__(self, place, src, dst, sems):
        self.p, self.src, self.dst, self.sems = place, src, dst, sems

    def x_copy(self, source_z, src, slot):
        p = self.p
        return remote(src, self.dst.at[slot], self.sems, source_z, (p.ctx_of(0, 1), p.s))

    def up_copy(self, source_z, src, slot):
        p = self.p
        to = (p.z + 1) * 2 + p.x
        return remote(src, self.dst.at[slot], self.sems, 4 + source_z, (to, p.s))

    def down_copy(self, source_z, src, slot):
        p = self.p
        to = (p.z - 1) * 2 + p.x
        return remote(src, self.dst.at[slot], self.sems, 8 + source_z, (to, p.s))

    def start(self):
        p = self.p

        @pl.when(p.z < 3)
        def _():
            self.up_copy(p.z, self.src, p.c).start()

        @pl.when(p.z > 0)
        def _():
            self.down_copy(p.z, self.src, p.c).start()

        self.x_copy(p.z, self.src, p.c).start()

    def advance(self, step):
        p = self.p
        low, high = p.z - step, p.z + step

        @pl.when(low >= 0)
        def _():
            slot = low * 2 + p.x
            self.up_copy(low, self.dst.at[slot], slot).wait_recv()

            @pl.when(p.z < 3)
            def _():
                self.up_copy(low, self.dst.at[slot], slot).start()

            self.x_copy(low, self.dst.at[slot], slot).start()

        @pl.when(high <= 3)
        def _():
            slot = high * 2 + p.x
            self.down_copy(high, self.dst.at[slot], slot).wait_recv()

            @pl.when(p.z > 0)
            def _():
                self.down_copy(high, self.dst.at[slot], slot).start()

            self.x_copy(high, self.dst.at[slot], slot).start()

    def across(self, source_z):
        slot = source_z * 2 + 1 - self.p.x
        self.x_copy(source_z, self.dst.at[slot], slot).wait_recv()

    def finish(self):
        p = self.p
        for source_z in range(4):
            slot = source_z * 2 + p.x
            self.x_copy(source_z, self.dst.at[slot], slot).wait_send()

            @pl.when((source_z <= p.z) & (p.z < 3))
            def _(source_z=source_z, slot=slot):
                self.up_copy(source_z, self.dst.at[slot], slot).wait_send()

            @pl.when((source_z >= p.z) & (p.z > 0))
            def _(source_z=source_z, slot=slot):
                self.down_copy(source_z, self.dst.at[slot], slot).wait_send()


class TwinGather:
    def __init__(self, place, src, dst, sems):
        self.p, self.src, self.dst, self.sems = place, src, dst, sems

    def x_copy(self, src, slot):
        p = self.p
        return remote(src, self.dst.at[slot], self.sems, 0, (p.ctx_of(0, 1), p.s))

    def up_copy(self, slot, src):
        p = self.p
        to = ((p.z + 1) * 2 + p.x, p.s)
        return remote(src, self.dst.at[slot], self.sems, 1 + slot, to)

    def down_copy(self, slot, src):
        p = self.p
        to = ((p.z - 1) * 2 + p.x, p.s)
        return remote(src, self.dst.at[slot], self.sems, 9 + slot, to)

    def both_ways(self, slot, src):
        @pl.when(self.p.z < 3)
        def _():
            self.up_copy(slot, src).start()

        @pl.when(self.p.z > 0)
        def _():
            self.down_copy(slot, src).start()

    def start(self):
        self.x_copy(self.src, self.p.c).start()
        self.both_ways(self.p.c, self.src)

    def pair(self):
        slot = self.p.ctx_of(0, 1)
        self.x_copy(self.dst.at[slot], slot).wait_recv()
        self.both_ways(slot, self.dst.at[slot])

    def advance(self, step):
        p = self.p
        for column in (p.x, 1 - p.x):
            low, high = (p.z - step) * 2 + column, (p.z + step) * 2 + column

            @pl.when(p.z >= step)
            def _(low=low):
                self.up_copy(low, self.dst.at[low]).wait_recv()

                @pl.when(p.z < 3)
                def _():
                    self.up_copy(low, self.dst.at[low]).start()

            @pl.when(p.z + step <= 3)
            def _(high=high):
                self.down_copy(high, self.dst.at[high]).wait_recv()

                @pl.when(p.z > 0)
                def _():
                    self.down_copy(high, self.dst.at[high]).start()

    def across(self, source_z):
        pass

    def finish(self):
        p = self.p
        self.x_copy(self.src, p.c).wait_send()
        for slot in range(8):
            block = self.dst.at[slot]

            @pl.when((slot // 2 <= p.z) & (p.z < 3))
            def _(slot=slot, block=block):
                self.up_copy(slot, block).wait_send()

            @pl.when((slot // 2 >= p.z) & (p.z > 0))
            def _(slot=slot, block=block):
                self.down_copy(slot, block).wait_send()


class PairGather:
    count = 3

    def __init__(self, place, src, dst, sems):
        self.p, self.src, self.dst, self.sems = place, src, dst, sems
        self.partner = (place.c, place.wsh_of(0, 1))
        self.over = (place.c, place.wsh_of(1, 0))

    def start(self):
        p = self.p
        self.first = remote(self.src, self.dst.at[p.s], self.sems, 0, self.over)
        self.first.start()
        self.second = remote(self.src, self.dst.at[p.s], self.sems, 1, self.partner)
        self.second.start()

    def relay(self):
        block = self.dst.at[self.over[1]]
        remote(block, block, self.sems, 0, self.over).wait_recv()
        self.third = remote(block, block, self.sems, 2, self.partner)
        self.third.start()

    def arrived(self):
        block = self.dst.at[self.partner[1]]
        remote(block, block, self.sems, 1, self.partner).wait_recv()
        block = self.dst.at[self.p.wsh_of(1, 1)]
        remote(block, block, self.sems, 2, self.partner).wait_recv()

    def finish(self):
        self.first.wait_send()
        self.second.wait_send()
        self.third.wait_send()


def greet_devices(devices):
    barrier = pltpu.get_barrier_semaphore()
    for device in devices:
        pl.semaphore_signal(barrier, inc=1, device_id=device, device_id_type=MESH_ID)
    pl.semaphore_wait(barrier, len(devices))


def ctx_peers(p):
    return [((p.c + step) % 8, p.s) for step in range(1, 8)]


def wsh_peers(p):
    return [(p.c, (p.s + step) % 4) for step in range(1, 4)]


def nt(left, right):
    return lax.dot_general(
        left, right, (((1,), (1,)), ((), ())), preferred_element_type=jnp.float32
    )


def nn(left, right):
    return jnp.dot(left, right, preferred_element_type=jnp.float32)


def tn(left, right):
    return lax.dot_general(
        left, right, (((0,), (0,)), ((), ())), preferred_element_type=jnp.float32
    )


def normalized(values):
    row_mean = jnp.mean(values, axis=-1, keepdims=True)
    centered = values - row_mean
    variance = jnp.mean(centered * centered, axis=-1, keepdims=True)
    scale = lax.rsqrt(variance + norm_eps)
    return centered * scale, scale


class LineReduce:
    count = 12

    def __init__(self, place, mine, from_x, from_low, from_high, out, acc, sems):
        self.p, self.mine, self.sems = place, mine, sems
        self.from_x, self.from_low, self.from_high = from_x, from_low, from_high
        self.out, self.acc = out, acc

    def order(self, index):
        near = self.p.z // 2
        z = self.p.z * (1 - near) + (3 - self.p.z) * near
        inner = (1 - index % 2) * (3 - index // 2) + (index % 2) * (index // 2)
        dest = (1 - z) * (3 - index) + z * inner
        return dest * (1 - near) + (3 - dest) * near

    def x_copy(self, dest):
        p = self.p
        return remote(
            self.mine.at[dest * 2 + 1 - p.x],
            self.from_x.at[dest],
            self.sems,
            dest,
            (p.ctx_of(0, 1), p.s),
        )

    def up_copy(self, dest):
        p = self.p
        to = ((p.z + 1) * 2 + p.x, p.s)
        return remote(self.out.at[dest], self.from_low.at[dest], self.sems, 4 + dest, to)

    def down_copy(self, dest):
        p = self.p
        to = ((p.z - 1) * 2 + p.x, p.s)
        return remote(self.out.at[dest], self.from_high.at[dest], self.sems, 8 + dest, to)

    def start(self, first=0, last=4):
        def body(index, carry):
            self.x_copy(self.order(index)).start()
            return carry

        lax.fori_loop(first, last, body, 0)

    def add(self, dest, target, source, keep):
        rows = self.acc.shape[0]

        def body(index, carry):
            part = pl.ds(pl.multiple_of(index * 32, 32), 32)
            if keep:
                self.acc[part, :] = self.acc[part, :] + source[dest, part, :].astype(jnp.float32)
            else:
                slot = dest * 2 + self.p.x
                self.acc[part, :] = self.mine[slot, part, :].astype(jnp.float32) + source[
                    dest, part, :
                ].astype(jnp.float32)
            return carry

        lax.fori_loop(0, rows // 32, body, 0)

    def combine(self):
        p = self.p

        def body(index, carry):
            dest = self.order(index)
            self.x_copy(dest).wait_recv()
            self.add(dest, None, self.from_x, False)

            @pl.when((dest >= p.z) & (p.z > 0))
            def _():
                self.up_copy(dest).wait_recv()
                self.add(dest, None, self.from_low, True)

            @pl.when((dest <= p.z) & (p.z < 3))
            def _():
                self.down_copy(dest).wait_recv()
                self.add(dest, None, self.from_high, True)

            @pl.when(dest != p.z)
            def _():
                rows = self.acc.shape[0]

                def down(step, inner):
                    part = pl.ds(pl.multiple_of(step * 32, 32), 32)
                    self.out[dest, part, :] = self.acc[part, :].astype(self.out.dtype)
                    return inner

                lax.fori_loop(0, rows // 32, down, 0)

            @pl.when(dest > p.z)
            def _():
                self.up_copy(dest).start()

            @pl.when(dest < p.z)
            def _():
                self.down_copy(dest).start()

            return carry

        lax.fori_loop(0, 4, body, 0)

    def finish(self):
        p = self.p
        for dest in range(4):
            self.x_copy(dest).wait_send()

            @pl.when(dest > p.z)
            def _(dest=dest):
                self.up_copy(dest).wait_send()

            @pl.when(dest < p.z)
            def _(dest=dest):
                self.down_copy(dest).wait_send()


class QuadSwap:
    def __init__(self, place, src_of, dst, sems):
        self.p, self.src_of, self.dst, self.sems = place, src_of, dst, sems
        self.sent = []

    def start(self):
        p = self.p
        for index, (to_y, to_k) in enumerate(((1, 1), (1, 0), (0, 1))):
            to = p.wsh_of(to_y, to_k)
            copy = remote(self.src_of(to), self.dst.at[p.s], self.sems, index, (p.c, to))
            copy.start()
            self.sent.append(copy)

    def arrived(self):
        p = self.p
        for index, (to_y, to_k) in enumerate(((1, 1), (1, 0), (0, 1))):
            source = p.wsh_of(to_y, to_k)
            block = self.dst.at[source]
            remote(block, block, self.sems, index, (p.c, source)).wait_recv()

    def finish(self):
        for copy in self.sent:
            copy.wait_send()


def layer_kernel(
    tok, cot, vec, w_project, w_combine, w_expand, w_reduce, pos_row, pos_col,
    layer_output, in_grad, reduce_all, combine_all, expand_all, project_all, vec_sum, square_out,
    tok_all, vec_all_in, n1, q, k, v, wp, wc, we, wr, dy, table, attended, lse, middle, two, cols,
    att_low, att_rows, two_mine,
    hidden, d_pre, pre_sum, two_out, two_own, out_terms, layer_out, pair_in, over_in,
    mid_grad, branch, att_grad, ff,
    datt, branch_all, dqkv, dk, dv, gp_mine, gp_terms,
    f_x, f_low, f_high, f_out, f_acc, t_mine, t_x, t_low, t_high, t_out, t_acc,
    reduce_own, combine_own, expand_terms, expand_own, project_own,
    vec_mine, vec_terms, vec_own, vec_all, sq_own, sq_all, sq_line, sq_group,
    g_first, pair_send, pair_recv, we_send, we_recv, att_send, att_recv, col_send, col_recv,
    ff_send, ff_recv, a_send, a_recv, r_sems, quad_send, quad_recv, g_sems, loc,
):
    p = Place()
    rows, width = tok.shape
    total = n1.shape[0]
    wide = jnp.float32
    cut = width // 32
    shard = w_combine.shape[0]
    hc = q.shape[1]
    low = jnp.bfloat16
    own_wp = [
        pltpu.make_async_copy(
            w_project.at[:, pl.ds(pl.multiple_of(part * width + p.c * hc, hc), hc)],
            wp.at[p.s, :, pl.ds(part * hc, hc)],
            loc.at[part],
        )
        for part in range(3)
    ]
    own = [
        pltpu.make_async_copy(tok, tok_all.at[p.c], loc.at[3]),
        pltpu.make_async_copy(vec, vec_all_in.at[p.s], loc.at[4]),
        pltpu.make_async_copy(w_combine, wc.at[p.s], loc.at[5]),
        pltpu.make_async_copy(cot, dy.at[p.s], loc.at[6]),
        pltpu.make_async_copy(
            w_expand.at[:, pl.ds(pl.multiple_of(p.s * width, width), width)],
            we.at[p.s],
            loc.at[7],
        ),
    ]
    load_reduce = pltpu.make_async_copy(w_reduce, wr, loc.at[10])
    for copy in own_wp + own + [load_reduce]:
        copy.start()
    greet_devices(ctx_peers(p) + wsh_peers(p))
    gather = LineGather(p, tok, tok_all, (g_first.at[0], g_first.at[1]))
    gather.start()

    def pair(index, src, dst):
        return PairGather(p, src, dst, (pair_send.at[index], pair_recv.at[index]))

    vec_pair = pair(0, vec, vec_all_in)
    vec_pair.start()
    for copy in own_wp:
        copy.wait()
    wp_pair = pair(1, wp.at[p.s], wp)
    wp_pair.start()
    wc_pair = pair(2, w_combine, wc)
    wc_pair.start()
    dy_pair = pair(3, cot, dy)
    dy_pair.start()
    we_copies = []
    for index, (to_y, to_k) in enumerate(((1, 1), (1, 0), (0, 1))):
        to = p.wsh_of(to_y, to_k)
        copy = remote(
            w_expand.at[:, pl.ds(pl.multiple_of(to * width, width), width)],
            we.at[p.s],
            (we_send, we_recv),
            index,
            (p.c, to),
        )
        copy.start()
        we_copies.append(copy)

    vec_pair.relay()
    own[1].wait()
    vec_pair.arrived()
    for source in range(4):
        table[:, source * shard : (source + 1) * shard] = vec_all_in[source].astype(jnp.float32)
    gain, bias = table[0:1, :], table[1:2, :]

    def norm_block(slot):
        scaled, _ = normalized(tok_all[slot].astype(jnp.float32))
        n1[pl.ds(pl.multiple_of(slot * rows, rows), rows), :] = (scaled * gain + bias).astype(low)

    own[0].wait()
    gather.advance(1)
    wp_pair.relay()
    gather.advance(2)
    wc_pair.relay()
    gather.advance(3)
    step_z = 1 - 2 * (p.z // 2)

    def own_line(index, carry):
        norm_block((p.z + index * step_z + 4) % 4 * 2 + p.x)
        return carry

    lax.fori_loop(0, 4, own_line, 0)

    def other_line(index, carry):
        source_z = (p.z + index * step_z + 4) % 4
        gather.across(source_z)
        norm_block(source_z * 2 + 1 - p.x)
        return carry

    lax.fori_loop(0, 4, other_line, 0)
    wp_pair.arrived()
    head_cols = pl.ds(pl.multiple_of(p.c * hc, hc), hc)
    bias_q, bias_v = table[2:3, head_cols], table[3:4, head_cols]

    def project(index, carry):
        part = pl.ds(pl.multiple_of(index * 256, 256), 256)
        out = nn(n1[part, :], wp[...].reshape(width, 3 * hc))
        q[part, :] = (out[:, :hc] + bias_q).astype(low)
        k[part, :] = out[:, hc : 2 * hc].astype(low)
        v[part, :] = (out[:, 2 * hc :] + bias_v).astype(low)
        return carry

    lax.fori_loop(0, total // 256, project, 0)
    dy_pair.relay()
    wc_pair.arrived()
    dy_pair.arrived()

    scale = (width // HEADS) ** (-0.5)

    def att_copy(dest, source_rows):
        return remote(
            att_low.at[dest],
            att_rows.at[:, head_cols],
            (att_send, att_recv),
            0,
            (dest, p.s),
        )

    def att_send_to(dest):
        return pltpu.make_async_remote_copy(
            src_ref=att_low.at[dest],
            dst_ref=att_rows.at[:, head_cols],
            send_sem=att_send.at[dest],
            recv_sem=att_recv.at[p.c],
            device_id=(dest, p.s),
            device_id_type=MESH_ID,
        )

    def att_own():
        return pltpu.make_async_copy(att_low.at[p.c], att_rows.at[:, head_cols], loc.at[8])

    def attend(index, carry):
        part = pl.ds(pl.multiple_of(index * 256, 256), 256)
        queries = q[part, :]
        seen = pos_row[0:1, :] <= pos_col[part, :]
        first = lax.broadcasted_iota(jnp.int32, (256, hc), 1) < hc // 2
        outs, logs = [], []
        for head in range(2):
            mine = first if head == 0 else jnp.logical_not(first)
            scores = nt(jnp.where(mine, queries, jnp.zeros_like(queries)), k[...]) * scale
            scores = jnp.where(seen, scores, masked_score)
            peak = jnp.max(scores, axis=1, keepdims=True)
            grown = jnp.exp(scores - peak)
            whole = jnp.sum(grown, axis=1, keepdims=True)
            probs = (grown * (1.0 / whole)).astype(low)
            outs.append(nn(probs, v[...]))
            logs.append(peak + jnp.log(whole))
        mixed = jnp.where(first, outs[0], outs[1])
        attended[part, :] = mixed
        lse[part, :] = jnp.where(first, logs[0], logs[1])
        mixed_low = mixed.astype(low)
        for half in range(2):
            dest = index * 2 + half
            att_low[dest] = mixed_low[half * 128 : (half + 1) * 128]

            @pl.when(dest != p.c)
            def _(dest=dest):
                att_send_to(dest).start()

            @pl.when(dest == p.c)
            def _():
                att_own().start()

        return carry

    lax.fori_loop(0, total // 256, attend, 0)
    att_own().wait()
    for step in range(1, 8):
        source = (p.c + step) % 8
        landed = att_rows.at[:, pl.ds(pl.multiple_of(source * hc, hc), hc)]
        pltpu.make_async_remote_copy(
            src_ref=landed,
            dst_ref=landed,
            send_sem=att_send.at[source],
            recv_sem=att_recv.at[source],
            device_id=(source, p.s),
            device_id_type=MESH_ID,
        ).wait_recv()
    own[2].wait()
    mid = tok[...].astype(jnp.float32) + nn(att_rows[...], wc[...].reshape(width, width)) + table[4:5, :]
    middle[...] = mid
    scaled, _ = normalized(mid)
    two_mine[...] = (scaled * table[5:6, :] + table[6:7, :]).astype(low)
    two[p.s] = two_mine[...]
    two_pair = pair(4, two_mine, two)
    two_pair.start()
    col_copies = []
    for index, (to_y, to_k) in enumerate(((1, 1), (1, 0), (0, 1))):
        to = p.wsh_of(to_y, to_k)
        copy = remote(
            att_rows.at[:, pl.ds(pl.multiple_of(to * shard, shard), shard)],
            cols.at[p.s],
            (col_send, col_recv),
            index,
            (p.c, to),
        )
        copy.start()
        col_copies.append(copy)
    own_cols = pltpu.make_async_copy(
        att_rows.at[:, pl.ds(pl.multiple_of(p.s * shard, shard), shard)], cols.at[p.s], loc.at[9]
    )
    own_cols.start()
    two_pair.relay()
    for index, (to_y, to_k) in enumerate(((1, 1), (1, 0), (0, 1))):
        source = p.wsh_of(to_y, to_k)
        remote(we.at[source], we.at[source], (we_send, we_recv), index, (p.c, source)).wait_recv()
    own[3].wait()
    own[4].wait()
    load_reduce.wait()
    two_pair.arrived()

    bias_ff = table[pl.ds(8 + p.s, 1), :]
    pre_sum[...] = jnp.zeros_like(pre_sum)

    def feed(dest):
        pre = nn(two[dest], we[...].reshape(width, width)) + bias_ff
        share = 0.5 * (1.0 + lax.erf(pre * (0.5**0.5)))
        act = (pre * share).astype(low)
        hidden[dest] = act
        slope = share + pre * (jnp.exp(-0.5 * pre * pre) * (0.5 / math.pi) ** 0.5)
        grad = (nt(dy[dest], wr[...]) * slope).astype(low)
        d_pre[dest] = grad
        pre_sum[...] += jnp.sum(grad.astype(wide), axis=0, keepdims=True)
        return nt(grad, we[...].reshape(width, width))

    def pair_copy(group, index, src):
        return remote(src, pair_in.at[group, index], (ff_send.at[group], ff_recv.at[group]), index, (p.c, p.wsh_of(0, 1)))

    def over_copy(group, src):
        return remote(src, over_in.at[group], (ff_send.at[group], ff_recv.at[group]), 2, (p.c, p.wsh_of(1, 0)))

    across, beside, partner = p.wsh_of(1, 1), p.wsh_of(1, 0), p.wsh_of(0, 1)
    two_out[0] = feed(across).astype(low)
    pair_copy(0, 0, two_out.at[0]).start()
    part_beside = feed(beside)
    pair_copy(0, 0, two_out.at[0]).wait_recv()
    two_out[1] = (part_beside + pair_in[0, 0].astype(wide)).astype(low)
    over_copy(0, two_out.at[1]).start()
    two_out[2] = feed(partner).astype(low)
    pair_copy(0, 1, two_out.at[2]).start()
    two_own[...] = feed(p.s)

    for part in range(4):
        block = pl.ds(part * 256, 256)
        out = tn(
            hidden[:, :, block].reshape(4 * rows, 256), dy[...].reshape(4 * rows, width)
        ).astype(low)
        ff[2 * part, 0:rows, :] = out[:rows]
        ff[2 * part + 1, 0:rows, :] = out[rows:]
        out = tn(
            two[:, :, block].reshape(4 * rows, 256), d_pre[...].reshape(4 * rows, width)
        ).astype(low)
        for dest in range(8):
            ff[dest, rows + part * cut : rows + (part + 1) * cut, :] = out[
                dest * cut : (dest + 1) * cut
            ]
    ff_line = LineReduce(p, ff, f_x, f_low, f_high, f_out, f_acc, (r_sems.at[0], r_sems.at[1]))
    ff_line.start(0, 1)

    pair_copy(0, 1, two_out.at[2]).wait_recv()
    over_copy(0, two_out.at[1]).wait_recv()
    grad_two = two_own[...] + pair_in[0, 1].astype(wide) + over_in[0].astype(wide)
    hat_two, spread_two = normalized(middle[...])
    inner = grad_two * table[5:6, :]
    cot_wide = cot[...].astype(wide)
    mid_grad[...] = cot_wide + spread_two * (
        inner
        - jnp.mean(inner, axis=1, keepdims=True)
        - hat_two * jnp.mean(inner * hat_two, axis=1, keepdims=True)
    )
    vec_mine[...] = jnp.zeros_like(vec_mine)
    branch[...] = mid_grad[...].astype(low)
    att_grad[...] = nt(branch[...], wc[...].reshape(width, width)).astype(low)
    def a_copy(dest):
        return pltpu.make_async_remote_copy(
            src_ref=att_grad.at[:, pl.ds(pl.multiple_of(dest * hc, hc), hc)],
            dst_ref=datt.at[p.c],
            send_sem=a_send.at[dest],
            recv_sem=a_recv.at[p.c],
            device_id=(dest, p.s),
            device_id_type=MESH_ID,
        )

    for dz, dx in CtxSwap.steps:
        a_copy(p.ctx_of(dz, dx)).start()
    own_att = pltpu.make_async_copy(
        att_grad.at[:, pl.ds(pl.multiple_of(p.c * hc, hc), hc)], datt.at[p.c], loc.at[11]
    )
    own_att.start()
    own_branch = pltpu.make_async_copy(branch, branch_all.at[p.s], loc.at[12])
    own_branch.start()
    branch_pair = pair(5, branch, branch_all)
    branch_pair.start()
    ff_line.start(1, 4)
    vec_mine[4:5, :] = jnp.sum(branch[...].astype(wide), axis=0, keepdims=True)
    vec_mine[5:6, :] = jnp.sum(grad_two * hat_two, axis=0, keepdims=True)
    vec_mine[6:7, :] = jnp.sum(grad_two, axis=0, keepdims=True)
    vec_mine[7:8, :] = jnp.sum(cot_wide, axis=0, keepdims=True)
    vec_mine[pl.ds(8 + p.s, 1), :] = pre_sum[...]

    def out_part(dest):
        return nn(hidden[dest], wr[...])

    out_terms[0] = out_part(across).astype(low)
    pair_copy(1, 0, out_terms.at[0]).start()
    out_terms[2] = out_part(partner).astype(low)
    pair_copy(1, 1, out_terms.at[2]).start()
    out_beside = out_part(beside)
    pair_copy(1, 0, out_terms.at[0]).wait_recv()
    out_terms[1] = (out_beside + pair_in[1, 0].astype(wide)).astype(low)
    over_copy(1, out_terms.at[1]).start()
    layer_out[...] = out_part(p.s)
    dk[...] = jnp.zeros_like(dk)
    dv[...] = jnp.zeros_like(dv)
    own_att.wait()
    for step in range(1, 8):
        source = (p.c + step) % 8
        pltpu.make_async_remote_copy(
            src_ref=datt.at[source],
            dst_ref=datt.at[source],
            send_sem=a_send.at[source],
            recv_sem=a_recv.at[source],
            device_id=(source, p.s),
            device_id_type=MESH_ID,
        ).wait_recv()

    def attend_back(index, carry):
        part = pl.ds(pl.multiple_of(index * 256, 256), 256)
        queries = q[part, :]
        grads = jnp.concatenate([datt[index * 2], datt[index * 2 + 1]], axis=0)
        seen = pos_row[0:1, :] <= pos_col[part, :]
        first = lax.broadcasted_iota(jnp.int32, (256, hc), 1) < hc // 2
        both = grads.astype(wide) * attended[part, :]
        outs = []
        for head in range(2):
            mine = first if head == 0 else jnp.logical_not(first)
            q_head = jnp.where(mine, queries, jnp.zeros_like(queries))
            g_head = jnp.where(mine, grads, jnp.zeros_like(grads))
            logs = lse[part, head * (hc // 2) : head * (hc // 2) + 1]
            scores = jnp.where(seen, nt(q_head, k[...]) * scale, masked_score)
            soft = jnp.exp(scores - logs)
            delta = jnp.sum(jnp.where(mine, both, 0.0), axis=1, keepdims=True)
            score_grad = (soft * (nt(g_head, v[...]) - delta)).astype(low)
            outs.append(nn(score_grad, k[...]))
            dk[...] += tn(score_grad, q_head)
            dv[...] += tn(soft.astype(low), g_head)
        dqkv[part, 0:hc] = (jnp.where(first, outs[0], outs[1]) * scale).astype(low)
        return carry

    lax.fori_loop(0, total // 256, attend_back, 0)
    dqkv[:, hc : 2 * hc] = (dk[...] * scale).astype(low)
    dqkv[:, 2 * hc :] = dv[...].astype(low)

    def one_terms(index, carry):
        part = pl.ds(pl.multiple_of(index * 256, 256), 256)
        out = nt(dqkv[part, :], wp[...].reshape(width, 3 * hc)).astype(low)
        t_mine[index * 2, 0:rows, :] = out[:rows]
        t_mine[index * 2 + 1, 0:rows, :] = out[rows:]
        return carry

    lax.fori_loop(0, total // 256, one_terms, 0)
    own_branch.wait()
    branch_pair.relay()
    branch_pair.arrived()
    for index, (to_y, to_k) in enumerate(((1, 1), (1, 0), (0, 1))):
        source = p.wsh_of(to_y, to_k)
        remote(cols.at[source], cols.at[source], (col_send, col_recv), index, (p.c, source)).wait_recv()
    own_cols.wait()
    grad_combine = tn(
        cols[...].reshape(4 * rows, shard), branch_all[...].reshape(4 * rows, width)
    ).astype(low)
    for dest in range(8):
        t_mine[dest, rows : rows + cut, :] = grad_combine[dest * cut : (dest + 1) * cut]
    tail = LineReduce(p, t_mine, t_x, t_low, t_high, t_out, t_acc, (r_sems.at[2], r_sems.at[3]))
    tail.start()
    for dest in range(4):
        gp_mine[dest] = tn(n1[:, dest * shard : (dest + 1) * shard], dqkv[...]).astype(low)
    gp_swap = QuadSwap(p, lambda to: gp_mine.at[to], gp_terms, (quad_send.at[0], quad_recv.at[0]))
    gp_swap.start()
    own_gp = pltpu.make_async_copy(gp_mine.at[p.s], gp_terms.at[p.s], loc.at[13])
    own_gp.start()

    pair_copy(1, 1, out_terms.at[2]).wait_recv()
    over_copy(1, out_terms.at[1]).wait_recv()
    layer_output[...] = (
        middle[...]
        + (layer_out[...] + pair_in[1, 1].astype(wide) + over_in[1].astype(wide))
        + table[7:8, :]
    ).astype(low)

    ff_line.combine()
    reduce_own[...] = f_acc[0:rows, :].astype(low)
    for part in range(4):
        f_out[p.z, part * cut : (part + 1) * cut, :] = f_acc[
            rows + part * cut : rows + (part + 1) * cut, :
        ].astype(low)
    expand_swap = QuadSwap(
        p,
        lambda to: f_out.at[p.z, pl.ds(pl.multiple_of(to * cut, cut), cut)],
        expand_terms,
        (quad_send.at[1], quad_recv.at[1]),
    )
    expand_swap.start()
    own_expand = pltpu.make_async_copy(
        f_out.at[p.z, pl.ds(pl.multiple_of(p.s * cut, cut), cut)], expand_terms.at[p.s], loc.at[14]
    )
    own_expand.start()
    gathers = []

    def share_out(index, src, dst, kind=LineGather):
        line = kind(p, src, dst, (g_sems.at[2 * index], g_sems.at[2 * index + 1]))
        line.start()
        own = pltpu.make_async_copy(src, dst.at[p.c], loc.at[15 + index])
        own.start()
        gathers.append((line, own))

    share_out(0, reduce_own, reduce_all)
    square = jnp.sum(jnp.square(reduce_own[...].astype(wide)))
    expand_swap.arrived()
    own_expand.wait()
    for part in range(4):
        expand_own[:, part * width : (part + 1) * width] = expand_terms[part]
    share_out(1, expand_own, expand_all)
    gathers[0][0].advance(1)
    gathers[1][0].advance(1)
    square += jnp.sum(jnp.square(expand_own[...].astype(wide)))
    gp_swap.arrived()
    own_gp.wait()
    project_own[...] = jnp.sum(gp_terms[...].astype(wide), axis=0).astype(low)
    square += jnp.sum(jnp.square(project_own[...].astype(wide)))
    share_out(2, project_own, project_all, TwinGather)

    tail.combine()
    combine_own[...] = t_acc[rows : rows + cut, :].astype(low)
    square += jnp.sum(jnp.square(combine_own[...].astype(wide)))
    share_out(3, combine_own, combine_all, TwinGather)
    grad = t_acc[0:rows, :]
    hat, spread = normalized(tok[...].astype(wide))
    hat_grad = grad * table[0:1, :]
    back = spread * (
        hat_grad
        - jnp.mean(hat_grad, axis=1, keepdims=True)
        - hat * jnp.mean(hat_grad * hat, axis=1, keepdims=True)
    )
    in_grad[...] = (mid_grad[...] + back).astype(low)
    vec_mine[0:1, :] = jnp.sum(grad * hat, axis=0, keepdims=True)
    vec_mine[1:2, :] = jnp.sum(grad, axis=0, keepdims=True)
    heads = pl.ds(pl.multiple_of(p.c * hc, hc), hc)
    vec_mine[2:3, heads] = jnp.sum(dqkv[:, 0:hc].astype(wide), axis=0, keepdims=True)
    vec_mine[3:4, heads] = jnp.sum(dqkv[:, 2 * hc :].astype(wide), axis=0, keepdims=True)
    vec_swap = QuadSwap(
        p,
        lambda to: vec_mine.at[:, pl.ds(pl.multiple_of(to * shard, shard), shard)],
        vec_terms,
        (quad_send.at[2], quad_recv.at[2]),
    )
    vec_swap.start()
    vec_terms[p.s] = vec_mine[:, pl.ds(pl.multiple_of(p.s * shard, shard), shard)]
    sq_own[...] = jnp.full(sq_own.shape, square, wide)
    gathers[2][0].pair()
    gathers[3][0].pair()
    gathers[0][0].advance(2)
    gathers[1][0].advance(2)
    vec_swap.arrived()
    vec_own[...] = jnp.sum(vec_terms[...], axis=0)
    share_out(4, vec_own, vec_all)
    share_out(5, sq_own, sq_all)
    first_two, others = gathers[:2], gathers[2:]
    for line, _ in others:
        line.advance(1)
    for line, _ in first_two:
        line.advance(3)
    for step in (2, 3):
        for line, _ in others:
            line.advance(step)
    for source_z in range(4):
        for line, _ in gathers:
            line.across(source_z)
    for _, own in gathers:
        own.wait()
    vectors = jnp.sum(vec_all[...], axis=0)
    vec_sum[...] = vectors
    sq_line[...] = jnp.sum(sq_all[...], axis=0) + jnp.sum(jnp.square(vectors))
    sq_pair = pair(6, sq_line, sq_group)
    sq_pair.start()
    sq_group[p.s] = sq_line[...]
    sq_pair.relay()
    sq_pair.arrived()
    square_out[...] = jnp.sum(sq_group[...], axis=0)
    for line, _ in gathers:
        line.finish()
    ff_line.finish()
    tail.finish()
    for member in (branch_pair, sq_pair, gp_swap, expand_swap, vec_swap):
        member.finish()
    for copy in we_copies + col_copies:
        copy.wait_send()
    gather.finish()
    for member in (vec_pair, wp_pair, wc_pair, dy_pair, two_pair):
        member.finish()
    for group, terms in enumerate((two_out, out_terms)):
        pair_copy(group, 0, terms.at[0]).wait_send()
        pair_copy(group, 1, terms.at[2]).wait_send()
        over_copy(group, terms.at[1]).wait_send()
    for step in range(1, 8):
        att_send_to((p.c + step) % 8).wait_send()
    for step in range(1, 8):
        a_copy((p.c + step) % 8).wait_send()


def layer_fused(tok, cot, vec, w_project, w_combine, w_expand, w_reduce, pos_row, pos_col):
    low, wide = jnp.bfloat16, jnp.float32
    rows, width = tok.shape
    total = rows * 8
    hc = width // 8
    shard = width // 4
    cut = shard // 8
    ff_rows, tail_rows = rows + 4 * cut, rows + cut
    vmem, hbm = pl.BlockSpec(memory_space=pltpu.VMEM), pl.BlockSpec(memory_space=pl.ANY)
    dma = pltpu.SemaphoreType.DMA
    mem = pltpu.VMEM
    return pl.pallas_call(
        layer_kernel,
        out_shape=[
            shape((rows, width), low),
            shape((rows, width), low),
            shape((8, rows, width), low),
            shape((8, cut, width), low),
            shape((8, cut, 4 * width), low),
            shape((8, shard, 3 * hc), low),
            shape((16, shard), wide),
            shape((8, 128), wide),
        ],
        in_specs=[vmem, vmem, vmem, hbm, vmem, hbm, hbm, vmem, vmem],
        out_specs=[vmem, vmem, hbm, hbm, hbm, hbm, vmem, vmem],
        scratch_shapes=[
            mem((8, rows, width), low),
            mem((4, 16, shard), low),
            mem((total, width), low),
            mem((total, hc), low),
            mem((total, hc), low),
            mem((total, hc), low),
            mem((4, shard, 3 * hc), low),
            mem((4, shard, width), low),
            mem((4, shard, width), low),
            mem((width, width), low),
            mem((4, rows, width), low),
            mem((16, width), wide),
            mem((total, hc), wide),
            mem((total, hc), wide),
            mem((rows, width), wide),
            mem((4, rows, width), low),
            mem((4, rows, shard), low),
            mem((8, rows, hc), low),
            mem((rows, width), low),
            mem((rows, width), low),
            mem((4, rows, width), low),
            mem((4, rows, width), low),
            mem((1, width), wide),
            mem((3, rows, width), low),
            mem((rows, width), wide),
            mem((3, rows, width), low),
            mem((rows, width), wide),
            mem((2, 2, rows, width), low),
            mem((2, rows, width), low),
            mem((rows, width), wide),
            mem((rows, width), low),
            mem((rows, width), low),
            mem((8, ff_rows, width), low),
            mem((8, rows, hc), low),
            mem((4, rows, width), low),
            mem((total, 3 * hc), low),
            mem((total, hc), wide),
            mem((total, hc), wide),
            mem((4, shard, 3 * hc), low),
            mem((4, shard, 3 * hc), low),
            mem((4, ff_rows, width), low),
            mem((4, ff_rows, width), low),
            mem((4, ff_rows, width), low),
            mem((4, ff_rows, width), low),
            mem((ff_rows, width), wide),
            mem((8, tail_rows, width), low),
            mem((4, tail_rows, width), low),
            mem((4, tail_rows, width), low),
            mem((4, tail_rows, width), low),
            mem((4, tail_rows, width), low),
            mem((tail_rows, width), wide),
            mem((rows, width), low),
            mem((cut, width), low),
            mem((4, cut, width), low),
            mem((cut, 4 * width), low),
            mem((shard, 3 * hc), low),
            mem((16, width), wide),
            mem((4, 16, shard), wide),
            mem((16, shard), wide),
            mem((8, 16, shard), wide),
            mem((8, 128), wide),
            mem((8, 8, 128), wide),
            mem((8, 128), wide),
            mem((4, 8, 128), wide),
            dma((2, 12)),
            dma((7, 3)),
            dma((7, 3)),
            dma((3,)),
            dma((3,)),
            dma((8,)),
            dma((8,)),
            dma((3,)),
            dma((3,)),
            dma((2, 3)),
            dma((2, 3)),
            dma((8,)),
            dma((8,)),
            dma((4, 12)),
            dma((3, 3)),
            dma((3, 3)),
            dma((12, 17)),
            dma((21,)),
        ],
        compiler_params=pltpu.CompilerParams(
            collective_id=10, has_side_effects=True, vmem_limit_bytes=67043328
        ),
        name="layer",
    )(tok, cot, vec, w_project, w_combine, w_expand, w_reduce, pos_row, pos_col)


def optimizer_kernel(clip_max, squares, vec_total, *refs):
    norm = jnp.sqrt(squares[...])
    factor = (clip_max / jnp.maximum(norm, clip_max))[0:1, 0:1]
    first_bias = 1.0 - beta_one**STEP
    second_bias = 1.0 - beta_two**STEP

    def one(weight, total, first, second, outs):
        g_out, m_out, v_out, u_out = outs
        g_out[...] = total
        clipped = total * factor
        moment = beta_one * first[...] + (1.0 - beta_one) * clipped
        square = beta_two * second[...] + (1.0 - beta_two) * clipped * clipped
        m_out[...] = moment
        v_out[...] = square
        moment_hat = moment * (1.0 / first_bias)
        square_hat = square * (1.0 / second_bias)
        u_out[...] = -learn_rate * (
            moment_hat / (jnp.sqrt(square_hat) + adam_eps)
            + decay_rate * weight[...].astype(jnp.float32)
        )

    for index in range(4):
        weight, grad, first, second = refs[4 * index : 4 * index + 4]
        if len(grad.shape) == 3:
            pieces = [
                grad[source, :, part * 128 : (part + 1) * 128]
                for part in range(3)
                for source in range(grad.shape[0])
            ]
            total = jnp.concatenate(pieces, axis=1).astype(jnp.float32)
        else:
            total = grad[...].astype(jnp.float32)
        one(weight, total, first, second, refs[19 + 4 * index : 23 + 4 * index])

    @pl.when(pl.program_id(0) == 0)
    def _():
        weight, first, second = refs[16:19]
        rows = weight.shape[0]
        one(weight, vec_total[0:rows, :], first, second, refs[35:39])
        refs[39][...] = norm


def optimizer_fused(clip_max, squares, vec_total, members, vec_members):
    steps = members[1][0].shape[0] // 32

    def whole(array):
        return pl.BlockSpec(array.shape, lambda i: (0, 0))

    operands = [squares, vec_total]
    in_specs = [whole(squares), whole(vec_total)]
    out_specs, out_shape = [], []
    for weight, grad, first, second in members:
        rows, width = weight.shape
        block = rows // steps
        flat = pl.BlockSpec((block, width), lambda i: (i, 0))
        operands += [weight, grad, first, second]
        if grad.ndim == 3:
            grad_spec = pl.BlockSpec((8, block, grad.shape[2]), lambda i: (0, i, 0))
        else:
            grad_spec = flat
        in_specs += [flat, grad_spec, flat, flat]
        out_specs += [flat] * 4
        out_shape += [shape((rows, width), jnp.float32)] * 4
    operands += vec_members
    in_specs += [whole(member) for member in vec_members]
    out_specs += [whole(vec_members[0])] * 4 + [whole(squares)]
    out_shape += [shape(vec_members[0].shape, jnp.float32)] * 4 + [
        shape(squares.shape, jnp.float32)
    ]

    def kernel(*refs):
        optimizer_kernel(clip_max, *refs)

    return pl.pallas_call(
        kernel,
        grid=(steps,),
        out_shape=out_shape,
        in_specs=in_specs,
        out_specs=out_specs,
        compiler_params=pltpu.CompilerParams(vmem_limit_bytes=60 * 2**20),
        name="optimizer",
    )(*operands)


def adam_step(weight, gradient, first_moment, second_moment, clip_factor, step_value):
    clipped = gradient * clip_factor
    moment = beta_one * first_moment + (1.0 - beta_one) * clipped
    square = beta_two * second_moment + (1.0 - beta_two) * clipped * clipped
    moment_hat = moment / (1.0 - jnp.power(jnp.float32(beta_one), step_value))
    square_hat = square / (1.0 - jnp.power(jnp.float32(beta_two), step_value))
    update = -learn_rate * (
        moment_hat / (jnp.sqrt(square_hat) + adam_eps) + decay_rate * weight.astype(jnp.float32)
    )
    return (moment, square, update)


def body_plain(
    tokens,
    output_cotangent,
    block_table,
    weight_project,
    weight_combine,
    weight_expand,
    weight_reduce,
    vectors,
    moment_project,
    square_project,
    moment_combine,
    square_combine,
    moment_expand,
    square_expand,
    moment_reduce,
    square_reduce,
    moment_vectors,
    square_vectors,
):
    low = jnp.bfloat16
    ctx_count, wsh_count = lax.axis_size("ctx"), lax.axis_size("wsh")
    ctx_index, wsh_index = lax.axis_index("ctx"), lax.axis_index("wsh")
    rows_dev, width = tokens.shape[1], tokens.shape[2]
    block_rows = rows_dev // 2
    total_rows = rows_dev * ctx_count
    group_rows = rows_dev * wsh_count
    head_size = width // HEADS
    score_scale = head_size ** (-0.5)
    head_cols = width // ctx_count
    local_heads = head_cols // head_size
    shard_rows = weight_project.shape[0]
    ff_width = weight_expand.shape[1]
    chunk = ff_width // wsh_count
    vec_rows = vectors.shape[0]
    swap = plain

    sequence = tokens[0].astype(jnp.float32)
    cotangent_low = output_cotangent[0]
    cotangent = cotangent_low.astype(jnp.float32)

    project_cols = lax.dynamic_slice_in_dim(
        weight_project.reshape(shard_rows, 3, ctx_count, head_cols), ctx_index, 1, axis=2
    ).reshape(shard_rows, 3 * head_cols)

    vec_pad = -vec_rows % 16
    (vec_parts,) = swap("vec", 0, (WshGather, jnp.pad(vectors, ((0, vec_pad), (0, 0)))))
    vec_table = (
        vec_parts[:, :vec_rows].transpose(1, 0, 2).reshape(vec_rows, width).astype(jnp.float32)
    )
    normed_one = layer_norm(sequence, vec_table[0], vec_table[1]).astype(low)
    normed_all, project_parts, cot_parts, combine_parts, expand_parts = swap(
        "front",
        1,
        (CtxGather, normed_one),
        (WshGather, project_cols),
        (WshGather, cotangent_low),
        (WshGather, weight_combine),
        (WshSwap, weight_expand.reshape(shard_rows, wsh_count, chunk).transpose(1, 0, 2)),
    )
    normed_all = normed_all.reshape(total_rows, width)
    project_mine = project_parts.reshape(width, 3 * head_cols)
    full_combine = combine_parts.reshape(width, width)
    expand_mine = expand_parts.reshape(width, chunk)
    cot_group = cot_parts.reshape(group_rows, width)

    qkv = matmul(normed_all, project_mine)
    bias_cols = lax.dynamic_slice_in_dim(
        vec_table[:4].reshape(4, ctx_count, head_cols), ctx_index, 1, axis=1
    ).reshape(4, head_cols)
    queries = (qkv[:, :head_cols] + bias_cols[2]).astype(low)
    keys = qkv[:, head_cols : 2 * head_cols].astype(low)
    values = (qkv[:, 2 * head_cols :] + bias_cols[3]).astype(low)
    positions = (
        block_table[:, None] * block_rows + jnp.arange(block_rows, dtype=jnp.int32)[None, :]
    ).reshape(total_rows)
    visible = positions[None, None, :] <= positions[None, :, None]
    heads = (total_rows, local_heads, head_size)
    query_heads, key_heads, value_heads = (
        queries.reshape(heads),
        keys.reshape(heads),
        values.reshape(heads),
    )
    scores = (
        jnp.einsum("qhd,khd->hqk", query_heads, key_heads, preferred_element_type=jnp.float32)
        * score_scale
    )
    scores = jnp.where(visible, scores, masked_score)
    peak = jnp.max(scores, axis=2, keepdims=True)
    grown = jnp.exp(scores - peak)
    soft = grown / jnp.sum(grown, axis=2, keepdims=True)
    soft_low = soft.astype(low)
    attended_heads = jnp.einsum(
        "hqk,khd->qhd", soft_low, value_heads, preferred_element_type=jnp.float32
    )
    attended = attended_heads.reshape(total_rows, head_cols)
    (att_parts,) = swap(
        "attended", 2, (CtxSwap, attended.astype(low).reshape(ctx_count, rows_dev, head_cols))
    )
    attended_rows = att_parts.transpose(1, 0, 2).reshape(rows_dev, width)

    middle = sequence + matmul(attended_rows, full_combine) + vec_table[4]
    normed_two = layer_norm(middle, vec_table[5], vec_table[6]).astype(low)
    two_parts, att_cols = swap(
        "normed_two",
        3,
        (WshGather, normed_two),
        (WshSwap, attended_rows.reshape(rows_dev, wsh_count, shard_rows).transpose(1, 0, 2)),
    )
    two_group = two_parts.reshape(group_rows, width)

    bias_ff = lax.dynamic_slice_in_dim(vec_table[8:].reshape(-1), wsh_index * chunk, chunk)
    hidden_pre = matmul(two_group, expand_mine) + bias_ff
    hidden, gelu_back = jax.vjp(gelu_exact, hidden_pre)
    hidden = hidden.astype(low)
    out_partial = matmul(hidden, weight_reduce)
    pre_grad = gelu_back(matmul_right_t(cot_group, weight_reduce))[0].astype(low)
    two_partial = matmul_right_t(pre_grad, expand_mine)
    part_shape = (wsh_count, rows_dev, width)
    two_terms, out_terms = swap(
        "ff_sums",
        4,
        (WshSwap, two_partial.astype(low).reshape(part_shape)),
        (WshSwap, out_partial.astype(low).reshape(part_shape)),
    )
    layer_output = middle + jnp.sum(out_terms.astype(jnp.float32), axis=0) + vec_table[7]
    normed_two_grad = jnp.sum(two_terms.astype(jnp.float32), axis=0)
    norm_two_back = jax.vjp(layer_norm, middle, vec_table[5], vec_table[6])[1](normed_two_grad)
    middle_grad = cotangent + norm_two_back[0]
    branch_grad = middle_grad.astype(low)
    attended_grad_rows = matmul_right_t(branch_grad, full_combine).astype(low)
    att_grad_parts, branch_parts = swap(
        "attended_grad",
        5,
        (CtxSwap, attended_grad_rows.reshape(rows_dev, ctx_count, head_cols).transpose(1, 0, 2)),
        (WshGather, branch_grad),
    )
    branch_group = branch_parts.reshape(group_rows, width)
    attended_grad = att_grad_parts.reshape(total_rows, head_cols)

    grad_reduce = matmul_left_t(hidden, cot_group)
    grad_expand = matmul_left_t(two_group, pre_grad)
    grad_combine = matmul_left_t(att_cols.reshape(group_rows, shard_rows), branch_group)

    grad_heads = attended_grad.reshape(heads)
    delta = jnp.sum(
        grad_heads.astype(jnp.float32) * attended_heads, axis=2
    ).transpose(1, 0)[:, :, None]
    soft_grad = jnp.einsum(
        "qhd,khd->hqk", grad_heads, value_heads, preferred_element_type=jnp.float32
    )
    score_grad = (soft * (soft_grad - delta)).astype(low)
    query_grad = (
        jnp.einsum("hqk,khd->qhd", score_grad, key_heads, preferred_element_type=jnp.float32)
        * score_scale
    )
    key_grad = (
        jnp.einsum("hqk,qhd->khd", score_grad, query_heads, preferred_element_type=jnp.float32)
        * score_scale
    )
    value_grad = jnp.einsum(
        "hqk,qhd->khd", soft_low, grad_heads, preferred_element_type=jnp.float32
    )
    flat = (total_rows, head_cols)
    qkv_grad = jnp.concatenate(
        [member.reshape(flat).astype(low) for member in (query_grad, key_grad, value_grad)], axis=1
    )
    grad_project = matmul_left_t(normed_all, qkv_grad)
    one_partial = matmul_right_t(qkv_grad, project_mine)

    cut = shard_rows // ctx_count
    cut_reduce = chunk // ctx_count
    for_ctx = jnp.concatenate(
        [
            grad_reduce.astype(low).reshape(ctx_count, cut_reduce, width),
            grad_combine.astype(low).reshape(ctx_count, cut, width),
        ],
        axis=1,
    )
    expand_ctx = (
        grad_expand.astype(low)
        .reshape(wsh_count, ctx_count, cut, chunk)
        .transpose(1, 0, 2, 3)
        .reshape(ctx_count, wsh_count * cut, chunk)
    )
    ctx_terms, expand_terms, one_terms, project_terms = swap(
        "grad_sums",
        6,
        (CtxSwap, for_ctx),
        (CtxSwap, expand_ctx),
        (CtxSwap, one_partial.astype(low).reshape(ctx_count, rows_dev, width)),
        (WshSwap, grad_project.astype(low).reshape(wsh_count, shard_rows, 3 * head_cols)),
    )
    normed_one_grad = jnp.sum(one_terms.astype(jnp.float32), axis=0)
    norm_one_back = jax.vjp(layer_norm, sequence, vec_table[0], vec_table[1])[1](normed_one_grad)
    input_gradient = (middle_grad + norm_one_back[0]).astype(low)
    ctx_piece = jnp.sum(ctx_terms.astype(jnp.float32), axis=0).astype(low)
    expand_piece = jnp.sum(expand_terms.astype(jnp.float32), axis=0).astype(low)
    project_piece = jnp.sum(project_terms.astype(jnp.float32), axis=0).astype(low)

    def spread(columns, start):
        return lax.dynamic_update_slice(
            jnp.zeros((width,), jnp.float32), columns, (start,)
        )

    ff_terms = lax.dynamic_update_slice(
        jnp.zeros((ff_width,), jnp.float32),
        jnp.sum(pre_grad.astype(jnp.float32), axis=0),
        (wsh_index * chunk,),
    ).reshape(-1, width)
    head_start = ctx_index * head_cols
    query_sum = jnp.sum(qkv_grad[:, :head_cols].astype(jnp.float32), axis=0)
    value_sum = jnp.sum(qkv_grad[:, 2 * head_cols :].astype(jnp.float32), axis=0)
    vec_terms = jnp.concatenate(
        [
            jnp.stack(
                [
                    norm_one_back[1],
                    norm_one_back[2],
                    spread(query_sum, head_start),
                    spread(value_sum, head_start),
                    jnp.sum(branch_grad.astype(jnp.float32), axis=0),
                    norm_two_back[1],
                    norm_two_back[2],
                    jnp.sum(cotangent, axis=0),
                ]
            ),
            ff_terms,
            jnp.zeros((vec_pad, width), jnp.float32),
        ],
        axis=0,
    )
    vec_cols = vectors.shape[1]
    vec_swapped, expand_rows = swap(
        "vec_sums",
        7,
        (WshSwap, vec_terms.reshape(-1, wsh_count, vec_cols).transpose(1, 0, 2)),
        (WshSwap, expand_piece.reshape(wsh_count, cut, chunk)),
    )
    vec_mine = jnp.sum(vec_swapped, axis=0)
    expand_mine_rows = expand_rows.transpose(1, 0, 2).reshape(cut, ff_width)
    square_mine = (
        jnp.sum(jnp.square(ctx_piece.astype(jnp.float32)))
        + jnp.sum(jnp.square(expand_rows.astype(jnp.float32)))
        + jnp.sum(jnp.square(project_piece.astype(jnp.float32)))
    )
    ctx_all, expand_all, project_all, vec_all, square_ctx = swap(
        "grads",
        8,
        (CtxGather, ctx_piece),
        (CtxGather, expand_mine_rows),
        (CtxGather, project_piece),
        (CtxGather, vec_mine),
        (CtxGather, jnp.full((16, 128), square_mine, jnp.float32)),
    )
    sum_reduce = ctx_all[:, :cut_reduce].reshape(chunk, width).astype(jnp.float32)
    sum_combine = ctx_all[:, cut_reduce:].reshape(shard_rows, width).astype(jnp.float32)
    sum_expand = expand_all.reshape(shard_rows, ff_width).astype(jnp.float32)
    sum_project = (
        project_all.reshape(ctx_count, shard_rows, 3, head_cols)
        .transpose(1, 2, 0, 3)
        .reshape(shard_rows, 3 * width)
        .astype(jnp.float32)
    )
    sum_vectors = jnp.sum(vec_all, axis=0)[:vec_rows]
    square_part = jnp.sum(square_ctx[:, 0, 0]) + jnp.sum(jnp.square(sum_vectors))
    (square_all,) = swap(
        "squares", 9, (WshGather, jnp.full((8, 128), square_part, jnp.float32))
    )
    norm_value = jnp.sqrt(jnp.sum(square_all[:, 0, 0]))
    params_total = 4 * width * width + 2 * width * ff_width + vec_rows * width
    clip_max = jnp.sqrt(jnp.float32(params_total))
    clip_factor = clip_max / jnp.maximum(norm_value, clip_max)
    step_value = jnp.float32(STEP)
    results = [layer_output.astype(low)[None], input_gradient[None], norm_value.reshape(1)]
    for weight, total, first, second in (
        (weight_project, sum_project, moment_project, square_project),
        (weight_combine, sum_combine, moment_combine, square_combine),
        (weight_expand, sum_expand, moment_expand, square_expand),
        (weight_reduce, sum_reduce, moment_reduce, square_reduce),
        (vectors, sum_vectors, moment_vectors, square_vectors),
    ):
        results.append(total)
        results.extend(adam_step(weight, total, first, second, clip_factor, step_value))
    return tuple(results)


def body_fast(
    tokens,
    output_cotangent,
    block_table,
    weight_project,
    weight_combine,
    weight_expand,
    weight_reduce,
    vectors,
    moment_project,
    square_project,
    moment_combine,
    square_combine,
    moment_expand,
    square_expand,
    moment_reduce,
    square_reduce,
    moment_vectors,
    square_vectors,
):
    rows_dev, width = tokens.shape[1], tokens.shape[2]
    block_rows = rows_dev // 2
    total_rows = rows_dev * 8
    ff_width = weight_expand.shape[1]
    vec_rows = vectors.shape[0]
    cot_low = output_cotangent[0]
    positions = (
        block_table[:, None] * block_rows + jnp.arange(block_rows, dtype=jnp.int32)[None, :]
    ).reshape(total_rows)
    pos_row = jnp.broadcast_to(positions[None, :], (8, total_rows))
    pos_col = positions[:, None]
    vec_padded = jnp.pad(vectors, ((0, -vec_rows % 16), (0, 0)))
    (
        layer_output, input_gradient, reduce_all, combine_all, expand_all, project_all, vec_sum,
        squares,
    ) = layer_fused(
        tokens[0], cot_low, vec_padded, weight_project, weight_combine, weight_expand,
        weight_reduce, pos_row, pos_col,
    )
    params_total = 4 * width * width + 2 * width * ff_width + vec_rows * width
    updated = optimizer_fused(
        float(params_total) ** 0.5,
        squares,
        vec_sum,
        (
            (weight_project, project_all, moment_project, square_project),
            (weight_combine, combine_all.reshape(-1, width), moment_combine, square_combine),
            (weight_expand, expand_all.reshape(-1, ff_width), moment_expand, square_expand),
            (weight_reduce, reduce_all.reshape(-1, width), moment_reduce, square_reduce),
        ),
        [vectors, moment_vectors, square_vectors],
    )
    *updated, norm_tile = updated
    return (layer_output[None], input_gradient[None], norm_tile[0, :1], *updated)


def solution(mesh):
    rows, cols = P("wsh", None), P(None, "wsh")
    token = P("wsh", "ctx", None)
    fast = (mesh.shape["ctx"], mesh.shape["wsh"]) == (FAST_CTX, FAST_WSH)
    return jax.shard_map(
        body_fast if fast else body_plain,
        mesh=mesh,
        in_specs=(token, token, P(), rows, rows, rows, rows, cols) + (rows,) * 8 + (cols,) * 2,
        out_specs=(token, token, P()) + (rows,) * 16 + (cols,) * 4,
        check_vma=False,
    )
```
